256 devices in a mesh: gx: 4 (over z_lo), gy: 8 (over z_hi, x), gz: 8 (over y, core).
Axes of the slice: x: 4, y: 4, z: 8 (z_hi: 2, z_lo: 4; z = z_hi * 4 + z_lo), core: 2. Of those that a mesh axis runs over, the one named last changes fastest.
Arguments:
- volume: bfloat16 [32, 8, 128, 1024], P(None, 'gx', 'gy', 'gz'), may hold values from -6 to 6
- w_first: bfloat16 [3, 3, 3, 32, 32], replicated, may hold values from -0.21875 to 0.21875
- w_second: bfloat16 [3, 3, 3, 32, 32], replicated, may hold values from -0.21875 to 0.21875
- v_first: bfloat16 [3, 3, 3, 32, 32], replicated, may hold values from -0.21875 to 0.21875
- v_second: bfloat16 [3, 3, 3, 32, 32], replicated, may hold values from -0.21875 to 0.21875
Outputs:
- jv: bfloat16 [32, 8, 128, 1024], P(None, 'gx', 'gy', 'gz')
- gv_first: float32 [3, 3, 3, 32, 32], replicated
- gv_second: float32 [3, 3, 3, 32, 32], replicated
The draws below stay inside these ranges and needn't reach their ends.
All inputs are finite; a program needn't handle non-finite values.
Results may differ from the reference program's by a relative error of at most 0.005.
Values may be sent and summed in bfloat16 or wider, within the bound.
No kernel may reach another device: no remote copies, remote signals or barrier semaphores. Data moves between devices by JAX's collectives and lax.ppermute only.
A program may use at most 64 MiB of HBM per device.

```python
import jax
import jax.numpy as jnp
from jax import lax

CHANNELS = 32
NX = 8
NY = 128
NZ = 1024
CELLS = 1048576
FILT = 864


def shard_levels(key, extent, split, least, high):
    factor_of, own = 1.0, jax.random.fold_in(key, 6)
    for dim, parts in split:
        heights = jnp.exp(jax.random.uniform(jax.random.fold_in(own, dim), (parts,), jnp.float32, least / len(split), high / len(split)))
        factor_of = factor_of * jnp.repeat(heights, extent[dim] // parts).reshape([-1 if axis == dim else 1 for axis in range(len(extent))])
    return factor_of


def bell_draw(key, dims, deviation, bound, shards=(), held_as=jnp.bfloat16):
    gain = shard_levels(key, dims, shards, -0.22, 0.18) if shards else 1.0
    drawn = jax.random.normal(key, dims, jnp.float32) * deviation * gain
    return jnp.minimum(jnp.maximum(drawn, -bound), bound).astype(held_as)


def setup_inputs(seed: int = 0) -> dict:
    key_of = jax.random.split(jax.random.key(seed), 6)
    return {
        "volume": bell_draw(key_of[0], (CHANNELS, NX, NY, NZ), 1.0, 6.0, ((1, 4), (2, 8), (3, 8))),
        "w_first": bell_draw(key_of[1], (3, 3, 3, CHANNELS, CHANNELS), FILT ** -0.5, 0.21875),
        "w_second": bell_draw(key_of[2], (3, 3, 3, CHANNELS, CHANNELS), FILT ** -0.5, 0.21875),
        "v_first": bell_draw(key_of[3], (3, 3, 3, CHANNELS, CHANNELS), FILT ** -0.5, 0.21875),
        "v_second": bell_draw(key_of[4], (3, 3, 3, CHANNELS, CHANNELS), FILT ** -0.5, 0.21875),
    }


def gelu_pair(pre):
    inner = 0.7978845608 * (pre + 0.044715 * pre * pre * pre)
    hyper = jnp.tanh(inner)
    hidden = 0.5 * pre * (1.0 + hyper)
    slope = 0.5 * (1.0 + hyper) + 0.5 * pre * (1.0 - hyper * hyper) * 0.7978845608 * (1.0 + 0.134145 * pre * pre)
    return hidden, slope


def convolve(field, weight):
    result = lax.conv_general_dilated(field.astype(jnp.float32)[None], weight.astype(jnp.float32), (1, 1, 1), "SAME", dimension_numbers=("NCDHW", "DHWIO", "NCDHW"), precision=lax.Precision.HIGHEST)
    return result[0]


def correlate(field, target):
    padded = jnp.pad(field.astype(jnp.float32), ((0, 0), (1, 1), (1, 1), (1, 1)))
    target32 = target.astype(jnp.float32)
    sizes = field.shape
    planes = []
    for shift_x in range(3):
        rows_y = []
        for shift_y in range(3):
            rows_z = []
            for shift_z in range(3):
                window = padded[:, shift_x:shift_x + sizes[1], shift_y:shift_y + sizes[2], shift_z:shift_z + sizes[3]]
                rows_z.append(jnp.einsum("cxyz,oxyz->co", window, target32, precision=lax.Precision.HIGHEST))
            rows_y.append(jnp.stack(rows_z))
        planes.append(jnp.stack(rows_y))
    return jnp.stack(planes)


def reference(volume, w_first, w_second, v_first, v_second):
    pre = convolve(volume, w_first)
    hidden_f, slope = gelu_pair(pre)
    hidden = hidden_f.astype(jnp.bfloat16)
    tangent = (slope * convolve(volume, v_first)).astype(jnp.bfloat16)
    jv = (convolve(tangent, w_second) + convolve(hidden, v_second)).astype(jnp.bfloat16)
    flipped = jnp.transpose(jnp.flip(w_second, (0, 1, 2)), (0, 1, 2, 4, 3))
    back = (slope * convolve(jv, flipped)).astype(jnp.bfloat16)
    count_all = jnp.float32(CELLS)
    factor = jnp.float32(FILT) ** 0.5
    gv_second = factor * (correlate(hidden, jv) / count_all + 0.1 * v_second.astype(jnp.float32))
    gv_first = factor * (correlate(volume, back) / count_all + 0.1 * v_first.astype(jnp.float32))
    return jv, gv_first, gv_second
```

```python
import math

import jax
import jax.numpy as jnp
from jax import lax
from jax.experimental import pallas as pl
from jax.experimental.pallas import tpu as pltpu
from jax.sharding import PartitionSpec as P

PITCH = 136
LA = 1408
LH = 1152
LJ = 896
LB = 640
F32 = jnp.float32
BF16 = jnp.bfloat16
AXES = ("gx", "gy", "gz")


def lanes_of(shape):
    return lax.broadcasted_iota(jnp.int32, shape, len(shape) - 1)


def assemble(planes, main_ref, up_ref, down_ref, field_ref, strip_ref):
    lane = lanes_of((32, 128))

    def plane(x, carry):
        rolled = []
        for row in range(10):
            if row < 3:
                tile = up_ref[x, row]
            elif row < 7:
                tile = main_ref[x, row - 3]
            else:
                tile = down_ref[x, row - 7]
            rolled.append(pltpu.roll(tile.astype(F32), 8 * row + 3, 1))
        strip = jnp.zeros((32, 128), F32)
        for row in range(10):
            strip = jnp.where((lane >= 8 * row) & (lane < 8 * row + 6), rolled[row], strip)
        strip_ref[x] = strip.astype(BF16)
        for tile in range(11):
            value = jnp.zeros((32, 128), F32)
            if tile < 10:
                value = jnp.where(lane >= 8 * tile + 3, rolled[tile], value)
            if tile > 0:
                value = jnp.where(lane < 8 * tile - 5, rolled[tile - 1], value)
            field_ref[x, :, 128 * tile : 128 * tile + 128] = value.astype(BF16)
        return carry

    lax.fori_loop(0, planes, plane, 0)


def gelu_pair(pre):
    inner = 0.7978845608 * (pre + 0.044715 * pre * pre * pre)
    hyper = jnp.tanh(inner)
    hidden = 0.5 * pre * (1.0 + hyper)
    slope = 0.5 * (1.0 + hyper) + 0.5 * pre * (1.0 - hyper * hyper) * 0.7978845608 * (
        1.0 + 0.134145 * pre * pre
    )
    return hidden, slope


def back_by(value, shift):
    if shift == 0:
        return value
    return pltpu.roll(value, value.shape[1] - shift, 1)


def fold(product):
    return product[0:32] + back_by(product[32:64], 1) + back_by(product[64:96], 2)


def spread(ref, x, value, width):
    for shift in range(3):
        ref[pl.ds(pl.multiple_of((x + 1) * 96 + 32 * shift, 32), 32), :] = back_by(
            value, PITCH * shift
        )[:, :width].astype(BF16)


def layers(
    planes,
    field_ref,
    left_ref,
    right_ref,
    weight_ref,
    mask_ref,
    jv_ref,
    sums_ref,
    p_vol,
    p_hid,
    p_tan,
    p_jv,
    slopes,
):
    for ref, width in ((p_vol, LH), (p_hid, LJ), (p_tan, LJ), (p_jv, LB)):
        blank = jnp.zeros((96, width), BF16)
        ref[0:96, :] = blank
        ref[96 * (planes + 1) : 96 * (planes + 2), :] = blank
    sums_ref[...] = jnp.zeros_like(sums_ref)
    lane = lanes_of((32, 128))

    def window(x):
        return pl.ds(pl.multiple_of(x * 96, 32), 288)

    def fill(x, carry):
        left = left_ref[x].astype(F32)
        right = right_ref[x].astype(F32)
        tiles = []
        for tile in range(11):
            value = field_ref[x, :, 128 * tile : 128 * tile + 128].astype(F32)
            if tile < 10:
                value = jnp.where((lane >= 8 * tile) & (lane < 8 * tile + 3), left, value)
            if tile > 0:
                value = jnp.where((lane >= 8 * tile - 5) & (lane < 8 * tile - 2), right, value)
            tiles.append(value)
        spread(p_vol, x, jnp.concatenate(tiles, axis=1), LH)
        return carry

    lax.fori_loop(0, planes, fill, 0)

    def first(x, carry):
        product = jnp.dot(weight_ref[0:192, :], p_vol[window(x), :], preferred_element_type=F32)
        inside = mask_ref[0:1, :LH] > 0.0
        hidden, slope = gelu_pair(fold(product[0:96]))
        tangent = slope * fold(product[96:192])
        slopes[x] = back_by(slope, 2 * PITCH + 2)[:, :LB]
        spread(p_hid, x, jnp.where(inside, hidden, 0.0), LJ)
        spread(p_tan, x, jnp.where(inside, tangent, 0.0), LJ)
        return carry

    lax.fori_loop(0, planes, first, 0)

    def second(x, carry):
        near = p_hid[window(x), :]
        product = jnp.dot(weight_ref[192:288, :], p_tan[window(x), :], preferred_element_type=F32)
        product = product + jnp.dot(weight_ref[288:384, :], near, preferred_element_type=F32)
        jv = fold(product).astype(BF16).astype(F32)
        jv = jnp.where(mask_ref[1:2, :LJ] > 0.0, jv, 0.0)
        spread(p_jv, x, jv, LB)
        for row in range(4):
            pair = jv[:, 128 * (row + 1) : 128 * (row + 3)]
            jv_ref[x, row] = back_by(pair, 8 * row + 9)[:, :128].astype(BF16)
        own = jnp.where(mask_ref[2:3, :LJ] > 0.0, jv, 0.0)
        moved = jnp.concatenate([own, pltpu.roll(own, 1, 1), pltpu.roll(own, 2, 1)], axis=0)
        sums_ref[0] += lax.dot_general(
            near[:, 128:768],
            moved[:, 128:768].astype(BF16),
            (((1,), (1,)), ((), ())),
            preferred_element_type=F32,
        )
        return carry

    lax.fori_loop(0, planes, second, 0)

    def third(x, carry):
        product = jnp.dot(weight_ref[384:480, :], p_jv[window(x), :], preferred_element_type=F32)
        back = slopes[x] * fold(product)
        back = jnp.where(mask_ref[3:4, :LB] > 0.0, back, 0.0).astype(BF16).astype(F32)
        moved = jnp.concatenate([pltpu.roll(back, 18 + k, 1) for k in range(3)], axis=0)
        sums_ref[1] += lax.dot_general(
            p_vol[window(x), 256:896],
            moved.astype(BF16),
            (((1,), (1,)), ((), ())),
            preferred_element_type=F32,
        )
        return carry

    lax.fori_loop(0, planes, third, 0)


def cell_masks(row0, col0, height, width):
    q = jnp.arange(LH, dtype=jnp.int32)
    row, col = q // PITCH, q % PITCH

    def inside(rows, cols, margin):
        y = row0 + row - margin
        z = col0 + col - margin
        return (row < rows) & (col < cols) & (y >= 0) & (y < height) & (z >= 0) & (z < width)

    own_jv = (row >= 1) & (row < 5) & (col >= 1) & (col < 129)
    own_back = (row < 4) & (col < 128)
    none = jnp.zeros_like(own_jv)
    rows = [inside(8, 132, 2), inside(6, 130, 1), own_jv, own_back, none, none, none, none]
    return jnp.stack(rows).astype(F32)


def filters(w_first, v_first, w_second, v_second):
    flipped = jnp.transpose(jnp.flip(w_second, (0, 1, 2)), (0, 1, 2, 4, 3))
    stacked = jnp.stack([w_first, v_first, w_second, v_second, flipped])
    return jnp.transpose(stacked, (0, 3, 5, 1, 2, 4)).reshape(480, 288)


def total(sums):
    count = lax.axis_size(AXES)
    parts = sums.reshape(count, -1)
    mine = jnp.sum(lax.all_to_all(parts, AXES, 0, 0), axis=0).astype(BF16)
    every = jnp.broadcast_to(mine[None], (count, mine.shape[0]))
    return lax.all_to_all(every, AXES, 0, 0).astype(F32).reshape(sums.shape)


def body(volume, w_first, w_second, v_first, v_second):
    channels, depth, height, width = volume.shape
    n_gx, n_gy, n_gz = lax.axis_size("gx"), lax.axis_size("gy"), lax.axis_size("gz")
    planes = depth * n_gx
    rows = height // n_gx
    count_all = float(planes * height * n_gy * width * n_gz)
    factor = math.sqrt(27.0 * channels)

    split = jnp.transpose(volume.reshape(channels, depth, n_gx, rows, width), (2, 1, 3, 0, 4))
    main = lax.all_to_all(split, "gx", 0, 0).reshape(planes, rows, channels, width)

    def device(block):
        return (block % n_gx) * n_gy + block // n_gx

    blocks = n_gx * n_gy
    onward = [(device(i), device(i + 1)) for i in range(blocks - 1)]
    backward = [(b, a) for a, b in onward]
    up = lax.ppermute(main[:, 1:], ("gx", "gy"), onward)
    down = lax.ppermute(main[:, :3], ("gx", "gy"), backward)

    vmem = pl.BlockSpec(memory_space=pltpu.VMEM)
    field, strip = pl.pallas_call(
        lambda *refs: assemble(planes, *refs),
        out_shape=(
            jax.ShapeDtypeStruct((planes, channels, LA), BF16),
            jax.ShapeDtypeStruct((planes, channels, 128), BF16),
        ),
        in_specs=[vmem] * 3,
        out_specs=(vmem, vmem),
        name="assemble",
    )(main, up, down)

    ends = [(i, i + 1) for i in range(n_gz - 1)]
    left = lax.ppermute(strip, "gz", ends)
    right = lax.ppermute(strip, "gz", [(b, a) for a, b in ends])

    row0 = (lax.axis_index("gy") * n_gx + lax.axis_index("gx")) * rows
    col0 = lax.axis_index("gz") * width
    masks = cell_masks(row0, col0, height * n_gy, width * n_gz)
    weights = filters(w_first, v_first, w_second, v_second)

    jv, sums = pl.pallas_call(
        lambda *refs: layers(planes, *refs),
        out_shape=(
            jax.ShapeDtypeStruct((planes, rows, channels, width), BF16),
            jax.ShapeDtypeStruct((2, 288, 96), F32),
        ),
        in_specs=[vmem] * 5,
        out_specs=(vmem, vmem),
        scratch_shapes=[
            pltpu.VMEM((96 * (planes + 2), LH), BF16),
            pltpu.VMEM((96 * (planes + 2), LJ), BF16),
            pltpu.VMEM((96 * (planes + 2), LJ), BF16),
            pltpu.VMEM((96 * (planes + 2), LB), BF16),
            pltpu.VMEM((planes, channels, LB), F32),
        ],
        name="layers",
    )(field, left, right, weights, masks)

    home = lax.all_to_all(jv.reshape(n_gx, depth, rows, channels, width), "gx", 0, 0)
    out = jnp.transpose(home, (3, 1, 0, 2, 4)).reshape(channels, depth, height, width)

    summed = total(sums).reshape(2, 3, 3, channels, 3, channels)
    summed_second, summed_first = jnp.transpose(summed, (0, 1, 2, 4, 3, 5))
    gv_first = factor * (summed_first / count_all + 0.1 * v_first.astype(F32))
    gv_second = factor * (summed_second / count_all + 0.1 * v_second.astype(F32))
    return (out, gv_first, gv_second)


def solution(mesh):
    in_specs = (P(None, "gx", "gy", "gz"), P(), P(), P(), P())
    out_specs = (P(None, "gx", "gy", "gz"), P(), P())
    return jax.shard_map(body, mesh=mesh, in_specs=in_specs, out_specs=out_specs, check_vma=False)
```

```python
import math

import jax
import jax.numpy as jnp
from jax import lax
from jax.experimental import pallas as pl
from jax.experimental.pallas import tpu as pltpu
from jax.sharding import PartitionSpec as P

PITCH = 136
LA = 1408
LH = 1152
LJ = 896
LB = 640
F32 = jnp.float32
BF16 = jnp.bfloat16
AXES = ("gx", "gy", "gz")


def lanes_of(shape):
    return lax.broadcasted_iota(jnp.int32, shape, len(shape) - 1)


def assemble(planes, main_ref, up_ref, down_ref, field_ref, strip_ref):
    lane = lanes_of((32, 128))

    def plane(x, carry):
        rolled = []
        for row in range(10):
            if row < 3:
                tile = up_ref[x, row]
            elif row < 7:
                tile = main_ref[x, row - 3]
            else:
                tile = down_ref[x, row - 7]
            rolled.append(pltpu.roll(tile.astype(F32), 8 * row + 3, 1))
        strip = jnp.zeros((32, 128), F32)
        for row in range(10):
            strip = jnp.where((lane >= 8 * row) & (lane < 8 * row + 6), rolled[row], strip)
        strip_ref[x] = strip.astype(BF16)
        for tile in range(11):
            value = jnp.zeros((32, 128), F32)
            if tile < 10:
                value = jnp.where(lane >= 8 * tile + 3, rolled[tile], value)
            if tile > 0:
                value = jnp.where(lane < 8 * tile - 5, rolled[tile - 1], value)
            field_ref[x, :, 128 * tile : 128 * tile + 128] = value.astype(BF16)
        return carry

    lax.fori_loop(0, planes, plane, 0)


def gelu_pair(pre):
    inner = 0.7978845608 * (pre + 0.044715 * pre * pre * pre)
    hyper = jnp.tanh(inner)
    hidden = 0.5 * pre * (1.0 + hyper)
    slope = 0.5 * (1.0 + hyper) + 0.5 * pre * (1.0 - hyper * hyper) * 0.7978845608 * (
        1.0 + 0.134145 * pre * pre
    )
    return hidden, slope


def back_by(value, shift):
    if shift == 0:
        return value
    return pltpu.roll(value, value.shape[1] - shift, 1)


def fold(product):
    return product[0:32] + back_by(product[32:64], 1) + back_by(product[64:96], 2)


def spread(ref, x, value, width):
    for shift in range(3):
        ref[pl.ds(pl.multiple_of((x + 1) * 96 + 32 * shift, 32), 32), :] = back_by(
            value, PITCH * shift
        )[:, :width].astype(BF16)


def window(x):
    return pl.ds(pl.multiple_of(x * 96, 32), 288)


def correlate(rows, moved):
    return lax.dot_general(
        rows, moved.astype(BF16), (((1,), (1,)), ((), ())), preferred_element_type=F32
    )


def outward(
    planes,
    field_ref,
    left_ref,
    right_ref,
    weight_ref,
    mask_ref,
    jv_ref,
    sums_ref,
    p_vol,
    p_jv,
    slopes,
    p_hid,
    p_tan,
):
    for ref, width in ((p_vol, LH), (p_hid, LJ), (p_tan, LJ), (p_jv, LB)):
        blank = jnp.zeros((96, width), BF16)
        ref[0:96, :] = blank
        ref[96 * (planes + 1) : 96 * (planes + 2), :] = blank
    sums_ref[...] = jnp.zeros_like(sums_ref)
    lane = lanes_of((32, 128))

    def fill(x, carry):
        left = left_ref[x].astype(F32)
        right = right_ref[x].astype(F32)
        tiles = []
        for tile in range(11):
            value = field_ref[x, :, 128 * tile : 128 * tile + 128].astype(F32)
            if tile < 10:
                value = jnp.where((lane >= 8 * tile) & (lane < 8 * tile + 3), left, value)
            if tile > 0:
                value = jnp.where((lane >= 8 * tile - 5) & (lane < 8 * tile - 2), right, value)
            tiles.append(value)
        spread(p_vol, x, jnp.concatenate(tiles, axis=1), LH)
        return carry

    lax.fori_loop(0, planes, fill, 0)

    def first(x, carry):
        product = jnp.dot(weight_ref[0:192, :], p_vol[window(x), :], preferred_element_type=F32)
        inside = mask_ref[0:1, :LH] > 0.0
        hidden, slope = gelu_pair(fold(product[0:96]))
        tangent = slope * fold(product[96:192])
        slopes[x] = back_by(slope, 2 * PITCH + 2)[:, :LB]
        spread(p_hid, x, jnp.where(inside, hidden, 0.0), LJ)
        spread(p_tan, x, jnp.where(inside, tangent, 0.0), LJ)
        return carry

    lax.fori_loop(0, planes, first, 0)

    def second(x, carry):
        near = p_hid[window(x), :]
        product = jnp.dot(weight_ref[192:288, :], p_tan[window(x), :], preferred_element_type=F32)
        product = product + jnp.dot(weight_ref[288:384, :], near, preferred_element_type=F32)
        jv = fold(product).astype(BF16).astype(F32)
        jv = jnp.where(mask_ref[1:2, :LJ] > 0.0, jv, 0.0)
        spread(p_jv, x, jv, LB)
        for row in range(4):
            pair = jv[:, 128 * (row + 1) : 128 * (row + 3)]
            jv_ref[x, row] = back_by(pair, 8 * row + 9)[:, :128].astype(BF16)
        own = jnp.where(mask_ref[2:3, :LJ] > 0.0, jv, 0.0)
        moved = jnp.concatenate(
            [own, pltpu.roll(own, 1, 1), pltpu.roll(own, 2, 1), jnp.zeros_like(own)], axis=0
        )
        sums_ref[...] += correlate(near[:, 128:768], moved[:, 128:768])
        return carry

    lax.fori_loop(0, planes, second, 0)


def inward(planes, weight_ref, mask_ref, second_ref, p_vol, p_jv, slopes, packed_ref, sums):
    sums[...] = jnp.zeros_like(sums)

    def third(x, carry):
        product = jnp.dot(weight_ref[384:480, :], p_jv[window(x), :], preferred_element_type=F32)
        back = slopes[x] * fold(product)
        back = jnp.where(mask_ref[3:4, :LB] > 0.0, back, 0.0).astype(BF16).astype(F32)
        moved = jnp.concatenate(
            [
                pltpu.roll(back, 19, 1),
                pltpu.roll(back, 20, 1),
                jnp.zeros_like(back),
                pltpu.roll(back, 18, 1),
            ],
            axis=0,
        )
        sums[...] += correlate(p_vol[window(x), 256:896], moved)
        return carry

    lax.fori_loop(0, planes, third, 0)
    packed_ref[0:288, :] = jnp.where(lanes_of((288, 128)) < 96, second_ref[...], sums[...])
    packed_ref[288:432, :] = jnp.where(
        lanes_of((144, 128)) < 64, sums[0:144, :], pltpu.roll(sums[144:288, :], 64, 1)
    )
    packed_ref[432:512, :] = jnp.zeros((80, 128), F32)


def combine(parts_ref, out_ref):
    total = jnp.sum(parts_ref[...].reshape(64, 8, 128), axis=0)
    total = total + pltpu.roll(total, 4, 0)
    total = total + pltpu.roll(total, 2, 0)
    out_ref[...] = jnp.broadcast_to(total[None], (64, 8, 128)).reshape(512, 128).astype(BF16)


def finish(factor, count_all, packed_ref, v_first_ref, v_second_ref, first_ref, second_ref):
    def damped(summed, direction):
        return factor * (summed / count_all + 0.1 * direction.astype(F32))

    high = packed_ref[288:432, :].astype(F32)
    high = jnp.concatenate([high, pltpu.roll(high, 64, 1)], axis=0)
    for k in range(9):
        low = packed_ref[32 * k : 32 * k + 32, :].astype(F32)
        far = high[32 * k : 32 * k + 32]
        for offset in range(3):
            at = 3 * k + offset
            second_ref[at] = damped(low[:, 32 * offset : 32 * offset + 32], v_second_ref[at])
        first_ref[3 * k] = damped(low[:, 96:128], v_first_ref[3 * k])
        first_ref[3 * k + 1] = damped(far[:, 0:32], v_first_ref[3 * k + 1])
        first_ref[3 * k + 2] = damped(far[:, 32:64], v_first_ref[3 * k + 2])


def cell_masks(row0, col0, height, width):
    q = jnp.arange(LH, dtype=jnp.int32)
    row, col = q // PITCH, q % PITCH

    def inside(rows, cols, margin):
        y = row0 + row - margin
        z = col0 + col - margin
        return (row < rows) & (col < cols) & (y >= 0) & (y < height) & (z >= 0) & (z < width)

    own_jv = (row >= 1) & (row < 5) & (col >= 1) & (col < 129)
    own_back = (row < 4) & (col < 128)
    none = jnp.zeros_like(own_jv)
    rows = [inside(8, 132, 2), inside(6, 130, 1), own_jv, own_back, none, none, none, none]
    return jnp.stack(rows).astype(F32)


def filters(w_first, v_first, w_second, v_second):
    flipped = jnp.transpose(jnp.flip(w_second, (0, 1, 2)), (0, 1, 2, 4, 3))
    stacked = jnp.stack([w_first, v_first, w_second, v_second, flipped])
    return jnp.transpose(stacked, (0, 3, 5, 1, 2, 4)).reshape(480, 288)


def body(volume, w_first, w_second, v_first, v_second):
    channels, depth, height, width = volume.shape
    n_gx, n_gy, n_gz = lax.axis_size("gx"), lax.axis_size("gy"), lax.axis_size("gz")
    planes = depth * n_gx
    rows = height // n_gx
    count_all = float(planes * height * n_gy * width * n_gz)
    factor = math.sqrt(27.0 * channels)

    split = jnp.transpose(volume.reshape(channels, depth, n_gx, rows, width), (2, 1, 3, 0, 4))
    main = lax.all_to_all(split, "gx", 0, 0).reshape(planes, rows, channels, width)

    def device(block):
        return (block % n_gx) * n_gy + block // n_gx

    blocks = n_gx * n_gy
    onward = [(device(i), device(i + 1)) for i in range(blocks - 1)]
    backward = [(b, a) for a, b in onward]
    row0 = (lax.axis_index("gy") * n_gx + lax.axis_index("gx")) * rows
    col0 = lax.axis_index("gz") * width
    masks = cell_masks(row0, col0, height * n_gy, width * n_gz)
    weights = filters(w_first, v_first, w_second, v_second)
    main, masks, weights = lax.optimization_barrier((main, masks, weights))

    up = lax.ppermute(main[:, 1:], ("gx", "gy"), onward)
    down = lax.ppermute(main[:, :3], ("gx", "gy"), backward)

    vmem = pl.BlockSpec(memory_space=pltpu.VMEM)

    def call(kernel, operands, outputs, scratch, name, limit):
        return pl.pallas_call(
            kernel,
            out_shape=tuple(jax.ShapeDtypeStruct(shape, dtype) for shape, dtype in outputs),
            in_specs=[vmem] * len(operands),
            out_specs=(vmem,) * len(outputs),
            scratch_shapes=[pltpu.VMEM(shape, dtype) for shape, dtype in scratch],
            compiler_params=pltpu.CompilerParams(vmem_limit_bytes=limit << 20),
            name=name,
        )(*operands)

    field, strip = call(
        lambda *refs: assemble(planes, *refs),
        (main, up, down),
        [((planes, channels, LA), BF16), ((planes, channels, 128), BF16)],
        [],
        "assemble",
        8,
    )

    ends = [(i, i + 1) for i in range(n_gz - 1)]
    left = lax.ppermute(strip, "gz", ends)
    right = lax.ppermute(strip, "gz", [(b, a) for a, b in ends])

    stack = 96 * (planes + 2)
    jv, second, p_vol, p_jv, slopes = call(
        lambda *refs: outward(planes, *refs),
        (field, left, right, weights, masks),
        [
            ((planes, rows, channels, width), BF16),
            ((288, 128), F32),
            ((stack, LH), BF16),
            ((stack, LB), BF16),
            ((planes, channels, LB), F32),
        ],
        [((stack, LJ), BF16), ((stack, LJ), BF16)],
        "outward",
        24,
    )

    home = lax.all_to_all(jv.reshape(n_gx, depth, rows, channels, width), "gx", 0, 0)
    out = jnp.transpose(home, (3, 1, 0, 2, 4)).reshape(channels, depth, height, width)

    (packed,) = call(
        lambda *refs: inward(planes, *refs),
        (weights, masks, second, p_vol, p_jv, slopes),
        [((512, 128), F32)],
        [((288, 128), F32)],
        "inward",
        24,
    )

    count = lax.axis_size(AXES)
    parts = lax.all_to_all(packed.reshape(count, 2, 128), AXES, 0, 0).reshape(512, 128)
    (every,) = call(combine, (parts,), [((512, 128), BF16)], [], "combine", 4)
    every = lax.all_to_all(every.reshape(count, 2, 128), AXES, 0, 0).reshape(512, 128)
    gv_first, gv_second = call(
        lambda *refs: finish(factor, count_all, *refs),
        (every, v_first.reshape(27, channels, channels), v_second.reshape(27, channels, channels)),
        [((27, channels, channels), F32)] * 2,
        [],
        "finish",
        8,
    )
    return (out, gv_first.reshape(v_first.shape), gv_second.reshape(v_first.shape))


def solution(mesh):
    in_specs = (P(None, "gx", "gy", "gz"), P(), P(), P(), P())
    out_specs = (P(None, "gx", "gy", "gz"), P(), P())
    return jax.shard_map(body, mesh=mesh, in_specs=in_specs, out_specs=out_specs, check_vma=False)
```

```python
import math

import jax
import jax.numpy as jnp
from jax import lax
from jax.experimental import pallas as pl
from jax.experimental.pallas import tpu as pltpu
from jax.sharding import PartitionSpec as P

PITCH = 136
LA = 1408
LH = 1152
LJ = 896
LB = 640
LV = 1024
F32 = jnp.float32
BF16 = jnp.bfloat16
AXES = ("gx", "gy", "gz")


def lanes_of(shape):
    return lax.broadcasted_iota(jnp.int32, shape, len(shape) - 1)


def assemble(planes, main_ref, up_ref, down_ref, field_ref, strip_ref):
    lane = lanes_of((32, 128))

    def plane(x, carry):
        rolled = []
        for row in range(10):
            if row < 3:
                tile = up_ref[x, row]
            elif row < 7:
                tile = main_ref[x, row - 3]
            else:
                tile = down_ref[x, row - 7]
            rolled.append(pltpu.roll(tile.astype(F32), 8 * row + 3, 1))
        strip = jnp.zeros((32, 128), F32)
        for row in range(10):
            strip = jnp.where((lane >= 8 * row) & (lane < 8 * row + 6), rolled[row], strip)
        strip_ref[x] = strip.astype(BF16)
        for tile in range(11):
            value = jnp.zeros((32, 128), F32)
            if tile < 10:
                value = jnp.where(lane >= 8 * tile + 3, rolled[tile], value)
            if tile > 0:
                value = jnp.where(lane < 8 * tile - 5, rolled[tile - 1], value)
            field_ref[x, :, 128 * tile : 128 * tile + 128] = value.astype(BF16)
        return carry

    lax.fori_loop(0, planes, plane, 0)


def gelu_pair(pre):
    inner = 0.7978845608 * (pre + 0.044715 * pre * pre * pre)
    hyper = jnp.tanh(inner)
    hidden = 0.5 * pre * (1.0 + hyper)
    slope = 0.5 * (1.0 + hyper) + 0.5 * pre * (1.0 - hyper * hyper) * 0.7978845608 * (
        1.0 + 0.134145 * pre * pre
    )
    return hidden, slope


def back_by(value, shift):
    if shift == 0:
        return value
    return pltpu.roll(value, value.shape[1] - shift, 1)


def fold(product):
    return product[0:32] + back_by(product[32:64], 1) + back_by(product[64:96], 2)


def spread(ref, x, value, width):
    for shift in range(3):
        ref[pl.ds(pl.multiple_of((x + 1) * 96 + 32 * shift, 32), 32), :] = back_by(
            value, PITCH * shift
        )[:, :width].astype(BF16)


def blank_ends(ref, planes):
    blank = jnp.zeros((96, ref.shape[1]), BF16)
    ref[0:96, :] = blank
    ref[96 * (planes + 1) : 96 * (planes + 2), :] = blank


def window(x):
    return pl.ds(pl.multiple_of(x * 96, 32), 288)


def correlate(rows, moved):
    return lax.dot_general(
        rows, moved.astype(BF16), (((1,), (1,)), ((), ())), preferred_element_type=F32
    )


def outward(
    planes,
    field_ref,
    left_ref,
    right_ref,
    weight_ref,
    mask_ref,
    jv_ref,
    volume_all,
    hidden_all,
    jv_all,
    slopes,
    p_vol,
    p_hid,
    p_tan,
):
    for ref in (p_vol, p_hid, p_tan):
        blank_ends(ref, planes)
    lane = lanes_of((32, 128))

    def fill(x, carry):
        left = left_ref[x].astype(F32)
        right = right_ref[x].astype(F32)
        tiles = []
        for tile in range(11):
            value = field_ref[x, :, 128 * tile : 128 * tile + 128].astype(F32)
            if tile < 10:
                value = jnp.where((lane >= 8 * tile) & (lane < 8 * tile + 3), left, value)
            if tile > 0:
                value = jnp.where((lane >= 8 * tile - 5) & (lane < 8 * tile - 2), right, value)
            tiles.append(value)
        value = jnp.concatenate(tiles, axis=1)
        spread(p_vol, x, value, LH)
        volume_all[x] = value[:, 256 : 256 + LV].astype(BF16)
        return carry

    lax.fori_loop(0, planes, fill, 0)

    def first(x, carry):
        product = jnp.dot(weight_ref[0:192, :], p_vol[window(x), :], preferred_element_type=F32)
        inside = mask_ref[0:1, :LH] > 0.0
        hidden, slope = gelu_pair(fold(product[0:96]))
        tangent = slope * fold(product[96:192])
        slopes[x] = back_by(slope, 2 * PITCH + 2)[:, :LB]
        hidden = jnp.where(inside, hidden, 0.0)
        hidden_all[x] = hidden[:, 128:].astype(BF16)
        spread(p_hid, x, hidden, LJ)
        spread(p_tan, x, jnp.where(inside, tangent, 0.0), LJ)
        return carry

    lax.fori_loop(0, planes, first, 0)

    def second(x, carry):
        near = p_hid[window(x), :]
        product = jnp.dot(weight_ref[192:288, :], p_tan[window(x), :], preferred_element_type=F32)
        product = product + jnp.dot(weight_ref[288:384, :], near, preferred_element_type=F32)
        jv = fold(product).astype(BF16).astype(F32)
        jv = jnp.where(mask_ref[1:2, :LJ] > 0.0, jv, 0.0)
        jv_all[x] = jv.astype(BF16)
        for row in range(4):
            pair = jv[:, 128 * (row + 1) : 128 * (row + 3)]
            jv_ref[x, row] = back_by(pair, 8 * row + 9)[:, :128].astype(BF16)
        return carry

    lax.fori_loop(0, planes, second, 0)


def inward(
    planes,
    weight_ref,
    mask_ref,
    volume_all,
    hidden_all,
    jv_all,
    slopes,
    packed_ref,
    sums_first,
    sums_second,
    p_vol,
    p_hid,
    p_jv,
):
    for ref in (p_vol, p_hid, p_jv):
        blank_ends(ref, planes)
    sums_first[...] = jnp.zeros_like(sums_first)
    sums_second[...] = jnp.zeros_like(sums_second)

    def fill(x, carry):
        spread(p_vol, x, volume_all[x].astype(F32), LB)
        spread(p_hid, x, hidden_all[x].astype(F32), LB)
        spread(p_jv, x, jv_all[x].astype(F32), LB)
        return carry

    lax.fori_loop(0, planes, fill, 0)

    def sums(x, carry):
        own = jnp.where(mask_ref[2:3, :LJ] > 0.0, jv_all[x].astype(F32), 0.0)[:, 128:768]
        moved = [own, pltpu.roll(own, 1, 1), pltpu.roll(own, 2, 1), jnp.zeros_like(own)]
        sums_second[...] += correlate(p_hid[window(x), :], jnp.concatenate(moved, axis=0))

        product = jnp.dot(weight_ref[384:480, :], p_jv[window(x), :], preferred_element_type=F32)
        back = slopes[x] * fold(product)
        back = jnp.where(mask_ref[3:4, :LB] > 0.0, back, 0.0).astype(BF16).astype(F32)
        moved = [
            pltpu.roll(back, 19, 1),
            pltpu.roll(back, 20, 1),
            jnp.zeros_like(back),
            pltpu.roll(back, 18, 1),
        ]
        sums_first[...] += correlate(p_vol[window(x), :], jnp.concatenate(moved, axis=0))
        return carry

    lax.fori_loop(0, planes, sums, 0)
    packed_ref[0:288, :] = jnp.where(
        lanes_of((288, 128)) < 96, sums_second[...], sums_first[...]
    )
    packed_ref[288:432, :] = jnp.where(
        lanes_of((144, 128)) < 64, sums_first[0:144, :], pltpu.roll(sums_first[144:288, :], 64, 1)
    )
    packed_ref[432:512, :] = jnp.zeros((80, 128), F32)


def combine(parts_ref, out_ref):
    total = jnp.sum(parts_ref[...].reshape(64, 8, 128), axis=0)
    total = total + pltpu.roll(total, 4, 0)
    total = total + pltpu.roll(total, 2, 0)
    out_ref[...] = jnp.broadcast_to(total[None], (64, 8, 128)).reshape(512, 128).astype(BF16)


def finish(factor, count_all, packed_ref, v_first_ref, v_second_ref, first_ref, second_ref):
    def damped(summed, direction):
        return factor * (summed / count_all + 0.1 * direction.astype(F32))

    high = packed_ref[288:432, :].astype(F32)
    high = jnp.concatenate([high, pltpu.roll(high, 64, 1)], axis=0)
    for k in range(9):
        low = packed_ref[32 * k : 32 * k + 32, :].astype(F32)
        far = high[32 * k : 32 * k + 32]
        for offset in range(3):
            at = 3 * k + offset
            second_ref[at] = damped(low[:, 32 * offset : 32 * offset + 32], v_second_ref[at])
        first_ref[3 * k] = damped(low[:, 96:128], v_first_ref[3 * k])
        first_ref[3 * k + 1] = damped(far[:, 0:32], v_first_ref[3 * k + 1])
        first_ref[3 * k + 2] = damped(far[:, 32:64], v_first_ref[3 * k + 2])


def cell_masks(row0, col0, height, width):
    q = jnp.arange(LH, dtype=jnp.int32)
    row, col = q // PITCH, q % PITCH

    def inside(rows, cols, margin):
        y = row0 + row - margin
        z = col0 + col - margin
        return (row < rows) & (col < cols) & (y >= 0) & (y < height) & (z >= 0) & (z < width)

    own_jv = (row >= 1) & (row < 5) & (col >= 1) & (col < 129)
    own_back = (row < 4) & (col < 128)
    none = jnp.zeros_like(own_jv)
    rows = [inside(8, 132, 2), inside(6, 130, 1), own_jv, own_back, none, none, none, none]
    return jnp.stack(rows).astype(F32)


def filters(w_first, v_first, w_second, v_second):
    flipped = jnp.transpose(jnp.flip(w_second, (0, 1, 2)), (0, 1, 2, 4, 3))
    stacked = jnp.stack([w_first, v_first, w_second, v_second, flipped])
    return jnp.transpose(stacked, (0, 3, 5, 1, 2, 4)).reshape(480, 288)


def body(volume, w_first, w_second, v_first, v_second):
    channels, depth, height, width = volume.shape
    n_gx, n_gy, n_gz = lax.axis_size("gx"), lax.axis_size("gy"), lax.axis_size("gz")
    planes = depth * n_gx
    rows = height // n_gx
    count_all = float(planes * height * n_gy * width * n_gz)
    factor = math.sqrt(27.0 * channels)

    split = jnp.transpose(volume.reshape(channels, depth, n_gx, rows, width), (2, 1, 3, 0, 4))
    main = lax.all_to_all(split, "gx", 0, 0).reshape(planes, rows, channels, width)

    def device(block):
        return (block % n_gx) * n_gy + block // n_gx

    blocks = n_gx * n_gy
    onward = [(device(i), device(i + 1)) for i in range(blocks - 1)]
    backward = [(b, a) for a, b in onward]
    row0 = (lax.axis_index("gy") * n_gx + lax.axis_index("gx")) * rows
    col0 = lax.axis_index("gz") * width
    masks = cell_masks(row0, col0, height * n_gy, width * n_gz)
    weights = filters(w_first, v_first, w_second, v_second)
    main, masks, weights = lax.optimization_barrier((main, masks, weights))

    up = lax.ppermute(main[:, 1:], ("gx", "gy"), onward)
    down = lax.ppermute(main[:, :3], ("gx", "gy"), backward)

    vmem = pl.BlockSpec(memory_space=pltpu.VMEM)

    def call(kernel, operands, outputs, scratch, name, limit, flops):
        return pl.pallas_call(
            kernel,
            out_shape=tuple(jax.ShapeDtypeStruct(shape, dtype) for shape, dtype in outputs),
            in_specs=[vmem] * len(operands),
            out_specs=(vmem,) * len(outputs),
            scratch_shapes=[pltpu.VMEM(shape, dtype) for shape, dtype in scratch],
            compiler_params=pltpu.CompilerParams(vmem_limit_bytes=limit << 20),
            cost_estimate=pl.CostEstimate(flops=flops, bytes_accessed=1 << 20, transcendentals=0),
            name=name,
        )(*operands)

    field, strip = call(
        lambda *refs: assemble(planes, *refs),
        (main, up, down),
        [((planes, channels, LA), BF16), ((planes, channels, 128), BF16)],
        [],
        "assemble",
        8,
        10**8,
    )

    ends = [(i, i + 1) for i in range(n_gz - 1)]
    left = lax.ppermute(strip, "gz", ends)
    right = lax.ppermute(strip, "gz", [(b, a) for a, b in ends])

    stack = 96 * (planes + 2)
    jv, volume_all, hidden_all, jv_all, slopes = call(
        lambda *refs: outward(planes, *refs),
        (field, left, right, weights, masks),
        [
            ((planes, rows, channels, width), BF16),
            ((planes, channels, LV), BF16),
            ((planes, channels, LV), BF16),
            ((planes, channels, LJ), BF16),
            ((planes, channels, LB), F32),
        ],
        [((stack, LH), BF16), ((stack, LJ), BF16), ((stack, LJ), BF16)],
        "outward",
        24,
        6 * 10**9,
    )

    home = lax.all_to_all(jv.reshape(n_gx, depth, rows, channels, width), "gx", 0, 0)

    (packed,) = call(
        lambda *refs: inward(planes, *refs),
        (weights, masks, volume_all, hidden_all, jv_all, slopes),
        [((512, 128), F32)],
        [((288, 128), F32)] * 2 + [((stack, LB), BF16)] * 3,
        "inward",
        24,
        3 * 10**9,
    )

    packed, home = lax.optimization_barrier((packed, home))

    out = jnp.transpose(home, (3, 1, 0, 2, 4)).reshape(channels, depth, height, width)

    count = lax.axis_size(AXES)
    parts = lax.all_to_all(packed.reshape(count, 2, 128), AXES, 0, 0).reshape(512, 128)
    (every,) = call(combine, (parts,), [((512, 128), BF16)], [], "combine", 4, 10**8)
    every = lax.all_to_all(every.reshape(count, 2, 128), AXES, 0, 0).reshape(512, 128)
    gv_first, gv_second = call(
        lambda *refs: finish(factor, count_all, *refs),
        (every, v_first.reshape(27, channels, channels), v_second.reshape(27, channels, channels)),
        [((27, channels, channels), F32)] * 2,
        [],
        "finish",
        8,
        10**8,
    )
    return (out, gv_first.reshape(v_first.shape), gv_second.reshape(v_first.shape))


def solution(mesh):
    in_specs = (P(None, "gx", "gy", "gz"), P(), P(), P(), P())
    out_specs = (P(None, "gx", "gy", "gz"), P(), P())
    return jax.shard_map(body, mesh=mesh, in_specs=in_specs, out_specs=out_specs, check_vma=False)
```

```python
import math

import jax
import jax.numpy as jnp
from jax import lax
from jax.experimental import pallas as pl
from jax.experimental.pallas import tpu as pltpu
from jax.sharding import PartitionSpec as P

F32 = jnp.float32
BF16 = jnp.bfloat16
AXES = ("gx", "gy", "gz")
GROUP = ("gx", "gy")
PLANES = 8
OWN = 4
MEMBERS = 32


def lanes_of(shape):
    return lax.broadcasted_iota(jnp.int32, shape, len(shape) - 1)


def exchange(tiles, bits):
    tiles = list(tiles)
    lane = lanes_of(tiles[0].shape)
    for place, bit in enumerate(bits):
        step = 1 << bit
        clear = (lane & step) == 0
        for low in range(len(tiles)):
            if low & (1 << place):
                continue
            high = low | (1 << place)
            a, b = tiles[low], tiles[high]
            tiles[low] = jnp.where(clear, a, pltpu.roll(b, step, 1))
            tiles[high] = jnp.where(clear, pltpu.roll(a, 128 - step, 1), b)
    return tiles


def permutation(inverse):
    source = lax.broadcasted_iota(jnp.int32, (128, 128), 0)
    target = lax.broadcasted_iota(jnp.int32, (128, 128), 1)
    if inverse:
        source, target = target, source
    hit = source == 4 * (target & 31) + (target >> 5)
    return jnp.where(hit, 1.0, 0.0).astype(BF16)


def pack(cells_ref, out_ref, sorted_ref):
    moved = jnp.dot(cells_ref[...].reshape(1024, 128), permutation(False), preferred_element_type=F32)
    sorted_ref[...] = moved.reshape(32, 32, 128)
    for part in range(2):
        at = slice(16 * part, 16 * part + 16)
        tiles = exchange([sorted_ref[i, at] for i in range(32)], (0, 1, 2, 3, 4))
        for member in range(MEMBERS):
            out_ref[member, at] = tiles[member].astype(BF16)


def arrange(parts_ref, own_ref):
    for g in range(4):
        tiles = exchange([parts_ref[8 * g + j].astype(F32) for j in range(8)], (4, 5, 6))
        for i in range(8):
            plane = 2 * g + i % 2
            own_ref[i // 2, 32 * plane : 32 * plane + 32] = tiles[i].astype(BF16)


def unpack(parts_ref, out_ref, mixed_ref):
    for part in range(2):
        at = slice(16 * part, 16 * part + 16)
        tiles = exchange([parts_ref[i, at].astype(F32) for i in range(MEMBERS)], (0, 1, 2, 3, 4))
        for i in range(32):
            mixed_ref[i, at] = tiles[i].astype(BF16)
    moved = jnp.dot(mixed_ref[...].reshape(1024, 128), permutation(True), preferred_element_type=F32)
    out_ref[...] = moved.astype(BF16).reshape(2, 16, 32, 128)


def gelu_pair(pre):
    inner = 0.7978845608 * (pre + 0.044715 * pre * pre * pre)
    hyper = jnp.tanh(inner)
    hidden = 0.5 * pre * (1.0 + hyper)
    slope = 0.5 * (1.0 + hyper) + 0.5 * pre * (1.0 - hyper * hyper) * 0.7978845608 * (
        1.0 + 0.134145 * pre * pre
    )
    return hidden, slope


def before(value):
    return jnp.where(lanes_of(value.shape) > 0, pltpu.roll(value, 1, 1), 0.0)


def after(value):
    return jnp.where(lanes_of(value.shape) < 127, pltpu.roll(value, 127, 1), 0.0)


def fold(product):
    return before(product[0:32]) + product[32:64] + after(product[64:96])


def near(ref, z, x):
    return jnp.concatenate(
        [
            jnp.concatenate([ref[z + at + offset, 32 * x : 32 * x + 96] for offset in range(3)], axis=0)
            for at in range(2)
        ],
        axis=1,
    )


def tile_of(x):
    return slice(32 * x + 32, 32 * x + 64)


def correlate(ref, z, targets):
    rows = jnp.concatenate([near(ref, z, x) for x in range(PLANES)], axis=1)
    return lax.dot_general(
        rows,
        jnp.concatenate(targets, axis=1),
        (((1,), (1,)), ((), ())),
        preferred_element_type=F32,
    )


def layers(
    own_ref,
    left_ref,
    right_ref,
    weight_ref,
    mask_ref,
    out_ref,
    p_vol,
    p_hid,
    p_tan,
    p_jv,
    slopes,
    sums_first,
    sums_second,
    packed,
):
    blank = jnp.zeros((32, 128), BF16)
    for ref, count in ((p_vol, 10), (p_hid, 8), (p_tan, 8), (p_jv, 6)):
        for z in range(count):
            ref[z, 0:32] = blank
            ref[z, 288:320] = blank
    for z in range(3):
        p_vol[z, 32:288] = left_ref[z]
        p_vol[7 + z, 32:288] = right_ref[z]
    for z in range(OWN):
        p_vol[3 + z, 32:288] = own_ref[z]
    sums_first[...] = jnp.zeros_like(sums_first)
    sums_second[...] = jnp.zeros_like(sums_second)

    def first(step, carry):
        z = 2 * step
        for x in range(PLANES):
            product = jnp.dot(weight_ref[0:192, :], near(p_vol, z, x), preferred_element_type=F32)
            for at in range(2):
                part = product[:, 128 * at : 128 * at + 128]
                inside = mask_ref[z + at] > 0.0
                hidden, slope = gelu_pair(fold(part[0:96]))
                tangent = slope * fold(part[96:192])
                p_hid[z + at, tile_of(x)] = jnp.where(inside, hidden, 0.0).astype(BF16)
                p_tan[z + at, tile_of(x)] = jnp.where(inside, tangent, 0.0).astype(BF16)
                slopes[z + at, x] = slope
        return carry

    lax.fori_loop(0, 4, first, 0)

    def second(step, carry):
        z = 2 * step
        for x in range(PLANES):
            product = jnp.dot(weight_ref[192:288, :], near(p_tan, z, x), preferred_element_type=F32)
            product = product + jnp.dot(
                weight_ref[288:384, :], near(p_hid, z, x), preferred_element_type=F32
            )
            for at in range(2):
                jv = fold(product[:, 128 * at : 128 * at + 128])
                jv = jnp.where(mask_ref[8 + z + at] > 0.0, jv, 0.0)
                p_jv[z + at, tile_of(x)] = jv.astype(BF16)
        return carry

    lax.fori_loop(0, 3, second, 0)

    def spread(tiles):
        both = [
            jnp.concatenate(
                [after(tile), tile, before(tile), jnp.zeros_like(tile)], axis=0
            )
            for tile in tiles
        ]
        return jnp.concatenate(both, axis=1).astype(BF16)

    def third(step, carry):
        z = 2 * step
        targets = [
            spread([p_jv[z + at + 1, tile_of(x)].astype(F32) for at in range(2)])
            for x in range(PLANES)
        ]
        sums_second[...] += correlate(p_hid.at[pl.ds(1, 6)], z, targets)
        targets = []
        for x in range(PLANES):
            product = jnp.dot(weight_ref[384:480, :], near(p_jv, z, x), preferred_element_type=F32)
            tiles = []
            for at in range(2):
                back = slopes[z + at + 2, x] * fold(product[:, 128 * at : 128 * at + 128])
                tiles.append(back.astype(BF16).astype(F32))
            targets.append(spread(tiles))
        sums_first[...] += correlate(p_vol.at[pl.ds(2, 6)], z, targets)
        return carry

    lax.fori_loop(0, 2, third, 0)

    for g in range(4):
        tiles = [p_jv[1 + i // 2, tile_of(2 * g + i % 2)].astype(F32) for i in range(8)]
        tiles = exchange(tiles, (4, 5, 6))
        for j in range(8):
            out_ref[8 * g + j, 0:32] = tiles[j].astype(BF16)

    low = jnp.where(
        lanes_of((288, 128)) < 96, sums_second[...], pltpu.roll(sums_first[...], 96, 1)
    )
    rest = pltpu.roll(sums_first[...], 96, 1)
    packed[0:288] = low
    packed[288:432] = jnp.where(
        lanes_of((144, 128)) < 64, rest[0:144], pltpu.roll(rest[144:288], 64, 1)
    )
    packed[432:512] = jnp.zeros((80, 128), F32)
    for member in range(MEMBERS):
        rows = packed[16 * member : 16 * member + 16]
        high = rows.astype(BF16)
        out_ref[member, 32:48] = high
        out_ref[member, 48:64] = (rows - high.astype(F32)).astype(BF16)


def gather_sums(parts_ref, out_ref):
    total = jnp.sum(
        parts_ref[:, 32:48].astype(F32) + parts_ref[:, 48:64].astype(F32), axis=0
    )
    for member in range(8):
        out_ref[member] = total


def combine(parts_ref, out_ref):
    total = jnp.sum(parts_ref[...], axis=0).astype(BF16)
    for member in range(MEMBERS):
        out_ref[member] = total


def finish(factor, count_all, packed_ref, v_first_ref, v_second_ref, first_ref, second_ref):
    def damped(summed, direction):
        return factor * (summed / count_all + 0.1 * direction.astype(F32))

    rest = packed_ref[288:432, :].astype(F32)
    rest = jnp.concatenate([rest, pltpu.roll(rest, 64, 1)], axis=0)
    for block in range(9):
        low = packed_ref[32 * block : 32 * block + 32, :].astype(F32)
        far = rest[32 * block : 32 * block + 32]
        at = [9 * (block % 3) + 3 * row + block // 3 for row in range(3)]
        for row in range(3):
            second_ref[at[row]] = damped(low[:, 32 * row : 32 * row + 32], v_second_ref[at[row]])
        first_ref[at[0]] = damped(low[:, 96:128], v_first_ref[at[0]])
        first_ref[at[1]] = damped(far[:, 0:32], v_first_ref[at[1]])
        first_ref[at[2]] = damped(far[:, 32:64], v_first_ref[at[2]])


def cell_masks(column, width):
    at = jnp.concatenate([jnp.arange(8) - 2, jnp.arange(8) - 1]).astype(jnp.int32) + column
    inside = (at >= 0) & (at < width)
    return jnp.broadcast_to(inside[:, None, None], (16, 32, 128)).astype(F32)


def filters(w_first, v_first, w_second, v_second):
    flipped = jnp.transpose(jnp.flip(w_second, (0, 1, 2)), (0, 1, 2, 4, 3))
    stacked = jnp.stack([w_first, v_first, w_second, v_second, flipped])
    return jnp.transpose(stacked, (0, 2, 5, 3, 1, 4)).reshape(480, 288)


def call(kernel, operands, outputs, scratch, name, limit, flops):
    vmem = pl.BlockSpec(memory_space=pltpu.VMEM)
    return pl.pallas_call(
        kernel,
        out_shape=tuple(jax.ShapeDtypeStruct(shape, dtype) for shape, dtype in outputs),
        in_specs=[vmem] * len(operands),
        out_specs=(vmem,) * len(outputs),
        scratch_shapes=[pltpu.VMEM(shape, dtype) for shape, dtype in scratch],
        compiler_params=pltpu.CompilerParams(vmem_limit_bytes=limit << 20),
        cost_estimate=pl.CostEstimate(flops=flops, bytes_accessed=1 << 20, transcendentals=0),
        name=name,
    )(*operands)


def body(volume, w_first, w_second, v_first, v_second):
    channels, depth, height, width = volume.shape
    n_gx, n_gy, n_gz = (lax.axis_size(axis) for axis in AXES)
    members = n_gx * n_gy
    count_all = float(depth * n_gx * height * n_gy * width * n_gz)
    factor = math.sqrt(27.0 * channels)
    small = (channels, 128)

    cells = jnp.transpose(volume, (1, 2, 0, 3))
    (sent,) = call(pack, (cells,), [((members,) + small, BF16)], [((32,) + small, F32)], "pack", 8, 10**8)
    parts = lax.all_to_all(sent, GROUP, 0, 0)

    block = lax.axis_index("gz") * members + lax.axis_index("gx") * n_gy + lax.axis_index("gy")
    masks = cell_masks(OWN * block, width * n_gz)
    weights = filters(w_first, v_first, w_second, v_second)
    parts, masks, weights = lax.optimization_barrier((parts, masks, weights))

    (own,) = call(arrange, (parts,), [((OWN, 256, 128), BF16)], [], "arrange", 8, 10**8)

    def device(at):
        return (at % members) * n_gz + at // members

    onward = [(device(i), device(i + 1)) for i in range(members * n_gz - 1)]
    left = lax.ppermute(own[1:], AXES, onward)
    right = lax.ppermute(own[:3], AXES, [(b, a) for a, b in onward])

    (leaving,) = call(
        layers,
        (own, left, right, weights, masks),
        [((members, 64, 128), BF16)],
        [
            ((10, 320, 128), BF16),
            ((8, 320, 128), BF16),
            ((8, 320, 128), BF16),
            ((6, 320, 128), BF16),
            ((8, PLANES) + small, F32),
            ((288, 128), F32),
            ((288, 128), F32),
            ((512, 128), F32),
        ],
        "layers",
        24,
        8 * 10**9,
    )

    parts = lax.all_to_all(leaving, GROUP, 0, 0)
    (sums,) = call(gather_sums, (parts,), [((n_gz, 16, 128), F32)], [], "gather_sums", 8, 10**8)
    sums = lax.all_to_all(sums, "gz", 0, 0)
    (every,) = call(combine, (sums,), [((members, 16, 128), BF16)], [], "combine", 8, 10**8)
    every = lax.all_to_all(every, GROUP, 0, 0).reshape(512, 128)
    (home,) = call(
        unpack,
        (parts,),
        [((depth, height) + small, BF16)],
        [((32,) + small, BF16)],
        "unpack",
        8,
        10**9,
    )
    out = jnp.transpose(home, (2, 0, 1, 3))
    gv_first, gv_second = call(
        lambda *refs: finish(factor, count_all, *refs),
        (every, v_first.reshape(27, channels, channels), v_second.reshape(27, channels, channels)),
        [((27, channels, channels), F32)] * 2,
        [],
        "finish",
        8,
        10**8,
    )
    return (out, gv_first.reshape(v_first.shape), gv_second.reshape(v_first.shape))


def solution(mesh):
    in_specs = (P(None, "gx", "gy", "gz"), P(), P(), P(), P())
    out_specs = (P(None, "gx", "gy", "gz"), P(), P())
    return jax.shard_map(body, mesh=mesh, in_specs=in_specs, out_specs=out_specs, check_vma=False)
```

```python
import math

import jax
import jax.numpy as jnp
from jax import lax
from jax.experimental import pallas as pl
from jax.experimental.pallas import tpu as pltpu
from jax.sharding import PartitionSpec as P

F32 = jnp.float32
BF16 = jnp.bfloat16
AXES = ("gx", "gy", "gz")
GROUP = ("gx", "gy")
PLANES = 8
OWN = 4
MEMBERS = 32


def closed_line():
    def member(z, x):
        return (z % 4) * 8 + (z // 4) * 4 + x

    line = []
    for z in range(8):
        line += [member(z, x) for x in ((1, 2, 3) if z % 2 == 0 else (3, 2, 1))]
    return tuple(line + [member(z, 0) for z in reversed(range(8))])


LINE = closed_line()


def lanes_of(shape):
    return lax.broadcasted_iota(jnp.int32, shape, len(shape) - 1)


def exchange(tiles, bits):
    tiles = list(tiles)
    lane = lanes_of(tiles[0].shape)
    for place, bit in enumerate(bits):
        step = 1 << bit
        clear = (lane & step) == 0
        for low in range(len(tiles)):
            if low & (1 << place):
                continue
            high = low | (1 << place)
            a, b = tiles[low], tiles[high]
            tiles[low] = jnp.where(clear, a, pltpu.roll(b, step, 1))
            tiles[high] = jnp.where(clear, pltpu.roll(a, 128 - step, 1), b)
    return tiles


def permutation(inverse):
    source = lax.broadcasted_iota(jnp.int32, (128, 128), 0)
    target = lax.broadcasted_iota(jnp.int32, (128, 128), 1)
    if inverse:
        source, target = target, source
    hit = source == 4 * (target & 31) + (target >> 5)
    return jnp.where(hit, 1.0, 0.0).astype(BF16)


def pack(cells_ref, out_ref, sorted_ref):
    sorted_ref[...] = jnp.dot(
        cells_ref[...].reshape(1024, 128), permutation(False), preferred_element_type=F32
    )
    for part in range(2):
        at = slice(16 * part, 16 * part + 16)
        tiles = [sorted_ref[pl.ds(512 * part + i, 16, stride=32)] for i in range(32)]
        tiles = exchange(tiles, (0, 1, 2, 3, 4))
        for i in range(MEMBERS):
            out_ref[LINE[i], at] = tiles[i].astype(BF16)


def arrange(parts_ref, own_ref):
    for g in range(4):
        tiles = exchange([parts_ref[8 * g + j].astype(F32) for j in range(8)], (4, 5, 6))
        for i in range(8):
            plane = 2 * g + i % 2
            own_ref[i // 2, 32 * plane : 32 * plane + 32] = tiles[i].astype(BF16)


def unpack(parts_ref, out_ref, mixed_ref):
    for part in range(2):
        at = slice(16 * part, 16 * part + 16)
        tiles = [parts_ref[LINE[i], at].astype(F32) for i in range(MEMBERS)]
        tiles = exchange(tiles, (0, 1, 2, 3, 4))
        for i in range(32):
            mixed_ref[pl.ds(512 * part + i, 16, stride=32)] = tiles[i]
    moved = jnp.dot(mixed_ref[...].astype(BF16), permutation(True), preferred_element_type=F32)
    out_ref[...] = moved.astype(BF16).reshape(32, 2, 16, 128)


def gelu_pair(pre):
    inner = 0.7978845608 * (pre + 0.044715 * pre * pre * pre)
    hyper = jnp.tanh(inner)
    hidden = 0.5 * pre * (1.0 + hyper)
    slope = 0.5 * (1.0 + hyper) + 0.5 * pre * (1.0 - hyper * hyper) * 0.7978845608 * (
        1.0 + 0.134145 * pre * pre
    )
    return hidden, slope


def before(value):
    return jnp.where(lanes_of(value.shape) > 0, pltpu.roll(value, 1, 1), 0.0)


def after(value):
    return jnp.where(lanes_of(value.shape) < 127, pltpu.roll(value, 127, 1), 0.0)


def fold(product):
    return before(product[0:32]) + product[32:64] + after(product[64:96])


def near(ref, z, x):
    return jnp.concatenate(
        [
            jnp.concatenate([ref[z + at + offset, 32 * x : 32 * x + 96] for offset in range(3)], axis=0)
            for at in range(2)
        ],
        axis=1,
    )


def tile_of(x):
    return slice(32 * x + 32, 32 * x + 64)


def correlate(ref, z, targets):
    rows = jnp.concatenate([near(ref, z, x) for x in range(PLANES)], axis=1)
    return lax.dot_general(
        rows,
        jnp.concatenate(targets, axis=1),
        (((1,), (1,)), ((), ())),
        preferred_element_type=F32,
    )


def layers(
    own_ref,
    left_ref,
    right_ref,
    weight_ref,
    mask_ref,
    out_ref,
    p_vol,
    p_hid,
    p_tan,
    p_jv,
    slopes,
    sums_first,
    sums_second,
    packed,
):
    blank = jnp.zeros((32, 128), BF16)
    for ref, count in ((p_vol, 10), (p_hid, 8), (p_tan, 8), (p_jv, 6)):
        for z in range(count):
            ref[z, 0:32] = blank
            ref[z, 288:320] = blank
    for z in range(3):
        p_vol[z, 32:288] = left_ref[z]
        p_vol[7 + z, 32:288] = right_ref[z]
    for z in range(OWN):
        p_vol[3 + z, 32:288] = own_ref[z]
    sums_first[...] = jnp.zeros_like(sums_first)
    sums_second[...] = jnp.zeros_like(sums_second)

    def first(step, carry):
        z = 2 * step
        for x in range(PLANES):
            product = jnp.dot(weight_ref[0:192, :], near(p_vol, z, x), preferred_element_type=F32)
            for at in range(2):
                part = product[:, 128 * at : 128 * at + 128]
                inside = mask_ref[z + at] > 0.0
                hidden, slope = gelu_pair(fold(part[0:96]))
                tangent = slope * fold(part[96:192])
                p_hid[z + at, tile_of(x)] = jnp.where(inside, hidden, 0.0).astype(BF16)
                p_tan[z + at, tile_of(x)] = jnp.where(inside, tangent, 0.0).astype(BF16)
                slopes[z + at, x] = slope
        return carry

    lax.fori_loop(0, 4, first, 0)

    def second(step, carry):
        z = 2 * step
        for x in range(PLANES):
            product = jnp.dot(weight_ref[192:288, :], near(p_tan, z, x), preferred_element_type=F32)
            product = product + jnp.dot(
                weight_ref[288:384, :], near(p_hid, z, x), preferred_element_type=F32
            )
            for at in range(2):
                jv = fold(product[:, 128 * at : 128 * at + 128])
                jv = jnp.where(mask_ref[8 + z + at] > 0.0, jv, 0.0)
                p_jv[z + at, tile_of(x)] = jv.astype(BF16)
        return carry

    lax.fori_loop(0, 3, second, 0)

    def spread(tiles):
        both = [
            jnp.concatenate(
                [after(tile), tile, before(tile), jnp.zeros_like(tile)], axis=0
            )
            for tile in tiles
        ]
        return jnp.concatenate(both, axis=1).astype(BF16)

    def third(step, carry):
        z = 2 * step
        targets = [
            spread([p_jv[z + at + 1, tile_of(x)].astype(F32) for at in range(2)])
            for x in range(PLANES)
        ]
        sums_second[...] += correlate(p_hid.at[pl.ds(1, 6)], z, targets)
        targets = []
        for x in range(PLANES):
            product = jnp.dot(weight_ref[384:480, :], near(p_jv, z, x), preferred_element_type=F32)
            tiles = []
            for at in range(2):
                back = slopes[z + at + 2, x] * fold(product[:, 128 * at : 128 * at + 128])
                tiles.append(back.astype(BF16).astype(F32))
            targets.append(spread(tiles))
        sums_first[...] += correlate(p_vol.at[pl.ds(2, 6)], z, targets)
        return carry

    lax.fori_loop(0, 2, third, 0)

    for g in range(4):
        tiles = [p_jv[1 + i // 2, tile_of(2 * g + i % 2)].astype(F32) for i in range(8)]
        tiles = exchange(tiles, (4, 5, 6))
        for j in range(8):
            out_ref[8 * g + j, 0:32] = tiles[j].astype(BF16)

    low = jnp.where(
        lanes_of((288, 128)) < 96, sums_second[...], pltpu.roll(sums_first[...], 96, 1)
    )
    rest = pltpu.roll(sums_first[...], 96, 1)
    packed[0:288] = low
    packed[288:432] = jnp.where(
        lanes_of((144, 128)) < 64, rest[0:144], pltpu.roll(rest[144:288], 64, 1)
    )
    packed[432:512] = jnp.zeros((80, 128), F32)
    for member in range(MEMBERS):
        rows = packed[16 * member : 16 * member + 16]
        high = rows.astype(BF16)
        out_ref[member, 32:48] = high
        out_ref[member, 48:64] = (rows - high.astype(F32)).astype(BF16)


def gather_sums(parts_ref, out_ref):
    total = jnp.sum(
        parts_ref[:, 32:48].astype(F32) + parts_ref[:, 48:64].astype(F32), axis=0
    )
    for member in range(8):
        out_ref[member] = total


def combine(parts_ref, out_ref):
    total = jnp.sum(parts_ref[...], axis=0).astype(BF16)
    for member in range(MEMBERS):
        out_ref[member] = total


def finish(scale, packed_ref, d_first_ref, d_second_ref, first_ref, second_ref):
    def damped(summed, damping):
        return scale * summed + damping

    rest = packed_ref[288:432, :].astype(F32)
    rest = jnp.concatenate([rest, pltpu.roll(rest, 64, 1)], axis=0)
    for block in range(9):
        low = packed_ref[32 * block : 32 * block + 32, :].astype(F32)
        far = rest[32 * block : 32 * block + 32]
        at = [9 * (block % 3) + 3 * row + block // 3 for row in range(3)]
        for row in range(3):
            second_ref[at[row]] = damped(low[:, 32 * row : 32 * row + 32], d_second_ref[at[row]])
        first_ref[at[0]] = damped(low[:, 96:128], d_first_ref[at[0]])
        first_ref[at[1]] = damped(far[:, 0:32], d_first_ref[at[1]])
        first_ref[at[2]] = damped(far[:, 32:64], d_first_ref[at[2]])


def cell_masks(column, width):
    at = jnp.concatenate([jnp.arange(8) - 2, jnp.arange(8) - 1]).astype(jnp.int32) + column
    inside = (at >= 0) & (at < width)
    return jnp.broadcast_to(inside[:, None, None], (16, 32, 128)).astype(F32)


def filters(w_first, v_first, w_second, v_second):
    flipped = jnp.transpose(jnp.flip(w_second, (0, 1, 2)), (0, 1, 2, 4, 3))
    stacked = jnp.stack([w_first, v_first, w_second, v_second, flipped])
    return jnp.transpose(stacked, (0, 2, 5, 3, 1, 4)).reshape(480, 288)


def call(kernel, operands, outputs, scratch, name, limit, flops):
    vmem = pl.BlockSpec(memory_space=pltpu.VMEM)
    return pl.pallas_call(
        kernel,
        out_shape=tuple(jax.ShapeDtypeStruct(shape, dtype) for shape, dtype in outputs),
        in_specs=[vmem] * len(operands),
        out_specs=(vmem,) * len(outputs),
        scratch_shapes=[pltpu.VMEM(shape, dtype) for shape, dtype in scratch],
        compiler_params=pltpu.CompilerParams(vmem_limit_bytes=limit << 20),
        cost_estimate=pl.CostEstimate(flops=flops, bytes_accessed=1 << 20, transcendentals=0),
        name=name,
    )(*operands)


def body(volume, w_first, w_second, v_first, v_second):
    channels, depth, height, width = volume.shape
    n_gx, n_gy, n_gz = (lax.axis_size(axis) for axis in AXES)
    members = n_gx * n_gy
    count_all = float(depth * n_gx * height * n_gy * width * n_gz)
    factor = math.sqrt(27.0 * channels)
    small = (channels, 128)

    (sent,) = call(pack, (volume,), [((members,) + small, BF16)], [((1024, 128), F32)], "pack", 8, 10**8)
    parts = lax.all_to_all(sent, GROUP, 0, 0)

    member = lax.axis_index("gx") * n_gy + lax.axis_index("gy")
    place = jnp.sum(jnp.where(jnp.array(LINE) == member, jnp.arange(members), 0)).astype(jnp.int32)
    masks = cell_masks(OWN * (lax.axis_index("gz") * members + place), width * n_gz)
    weights = filters(w_first, v_first, w_second, v_second)
    damping = tuple(
        factor * 0.1 * v.astype(F32).reshape(27, channels, channels) for v in (v_first, v_second)
    )
    parts, masks, weights, damping = lax.optimization_barrier((parts, masks, weights, damping))

    (own,) = call(arrange, (parts,), [((OWN, 256, 128), BF16)], [], "arrange", 8, 10**8)

    def device(at):
        return LINE[at % members] * n_gz + at // members

    onward = [(device(i), device(i + 1)) for i in range(members * n_gz - 1)]
    left = lax.ppermute(own[1:], AXES, onward)
    right = lax.ppermute(own[:3], AXES, [(b, a) for a, b in onward])

    (leaving,) = call(
        layers,
        (own, left, right, weights, masks),
        [((members, 64, 128), BF16)],
        [
            ((10, 320, 128), BF16),
            ((8, 320, 128), BF16),
            ((8, 320, 128), BF16),
            ((6, 320, 128), BF16),
            ((8, PLANES) + small, F32),
            ((288, 128), F32),
            ((288, 128), F32),
            ((512, 128), F32),
        ],
        "layers",
        24,
        8 * 10**9,
    )

    parts = lax.all_to_all(leaving, GROUP, 0, 0)
    (sums,) = call(gather_sums, (parts,), [((n_gz, 16, 128), F32)], [], "gather_sums", 8, 10**8)
    sums = lax.all_to_all(sums, "gz", 0, 0)
    (every,) = call(combine, (sums,), [((members, 16, 128), BF16)], [], "combine", 8, 10**8)
    every = lax.all_to_all(every, GROUP, 0, 0).reshape(512, 128)
    (out,) = call(
        unpack,
        (parts,),
        [(volume.shape, BF16)],
        [((1024, 128), F32)],
        "unpack",
        8,
        10**9,
    )
    gv_first, gv_second = call(
        lambda *refs: finish(factor / count_all, *refs),
        (every,) + damping,
        [((27, channels, channels), F32)] * 2,
        [],
        "finish",
        8,
        10**8,
    )
    return (out, gv_first.reshape(v_first.shape), gv_second.reshape(v_first.shape))


def solution(mesh):
    in_specs = (P(None, "gx", "gy", "gz"), P(), P(), P(), P())
    out_specs = (P(None, "gx", "gy", "gz"), P(), P())
    return jax.shard_map(body, mesh=mesh, in_specs=in_specs, out_specs=out_specs, check_vma=False)
```

```python
import math

import jax
import jax.numpy as jnp
from jax import lax
from jax.experimental import pallas as pl
from jax.experimental.pallas import tpu as pltpu
from jax.sharding import PartitionSpec as P

F32 = jnp.float32
BF16 = jnp.bfloat16
AXES = ("gx", "gy", "gz")
GROUP = ("gx", "gy")
PLANES = 8
OWN = 4
MEMBERS = 32


def closed_line():
    def member(z, x):
        return (z % 4) * 8 + (z // 4) * 4 + x

    line = []
    for z in range(8):
        line += [member(z, x) for x in ((1, 2, 3) if z % 2 == 0 else (3, 2, 1))]
    return tuple(line + [member(z, 0) for z in reversed(range(8))])


LINE = closed_line()


def lanes_of(shape):
    return lax.broadcasted_iota(jnp.int32, shape, len(shape) - 1)


def exchange(tiles, bits):
    tiles = list(tiles)
    lane = lanes_of(tiles[0].shape)
    for place, bit in enumerate(bits):
        step = 1 << bit
        clear = (lane & step) == 0
        for low in range(len(tiles)):
            if low & (1 << place):
                continue
            high = low | (1 << place)
            a, b = tiles[low], tiles[high]
            tiles[low] = jnp.where(clear, a, pltpu.roll(b, step, 1))
            tiles[high] = jnp.where(clear, pltpu.roll(a, 128 - step, 1), b)
    return tiles


def permutation(inverse):
    source = lax.broadcasted_iota(jnp.int32, (128, 128), 0)
    target = lax.broadcasted_iota(jnp.int32, (128, 128), 1)
    if inverse:
        source, target = target, source
    hit = source == 4 * (target & 31) + (target >> 5)
    return jnp.where(hit, 1.0, 0.0).astype(BF16)


def pack(cells_ref, out_ref, sorted_ref):
    sorted_ref[...] = jnp.dot(
        cells_ref[...].reshape(1024, 128), permutation(False), preferred_element_type=F32
    )
    for part in range(2):
        at = slice(16 * part, 16 * part + 16)
        tiles = [sorted_ref[pl.ds(512 * part + i, 16, stride=32)] for i in range(32)]
        tiles = exchange(tiles, (0, 1, 2, 3, 4))
        for i in range(MEMBERS):
            out_ref[LINE[i], at] = tiles[i].astype(BF16)


def arrange(parts_ref, odd_ref, own_ref, first_ref, second_ref):
    for g in range(4):
        tiles = exchange([parts_ref[8 * g + j].astype(F32) for j in range(8)], (4, 5, 6))
        for i in range(8):
            plane = 2 * g + i % 2
            own_ref[i // 2, 32 * plane : 32 * plane + 32] = tiles[i].astype(BF16)
    odd = odd_ref[0] > 0

    @pl.when(odd)
    def _():
        first_ref[...] = own_ref[0:3]
        second_ref[...] = own_ref[1:4]

    @pl.when(jnp.logical_not(odd))
    def _():
        first_ref[...] = own_ref[1:4]
        second_ref[...] = own_ref[0:3]


def unpack(parts_ref, out_ref, mixed_ref):
    for part in range(2):
        at = slice(16 * part, 16 * part + 16)
        tiles = [parts_ref[LINE[i], at].astype(F32) for i in range(MEMBERS)]
        tiles = exchange(tiles, (0, 1, 2, 3, 4))
        for i in range(32):
            mixed_ref[pl.ds(512 * part + i, 16, stride=32)] = tiles[i]
    moved = jnp.dot(mixed_ref[...].astype(BF16), permutation(True), preferred_element_type=F32)
    out_ref[...] = moved.astype(BF16).reshape(32, 2, 16, 128)


def gelu_pair(pre):
    inner = 0.7978845608 * (pre + 0.044715 * pre * pre * pre)
    hyper = jnp.tanh(inner)
    hidden = 0.5 * pre * (1.0 + hyper)
    slope = 0.5 * (1.0 + hyper) + 0.5 * pre * (1.0 - hyper * hyper) * 0.7978845608 * (
        1.0 + 0.134145 * pre * pre
    )
    return hidden, slope


def before(value):
    return jnp.where(lanes_of(value.shape) > 0, pltpu.roll(value, 1, 1), 0.0)


def after(value):
    return jnp.where(lanes_of(value.shape) < 127, pltpu.roll(value, 127, 1), 0.0)


def fold(product):
    return before(product[0:32]) + product[32:64] + after(product[64:96])


def near(refs, z, x):
    def block(ref, at):
        rows = ref[at, max(32 * x - 32, 0) : min(32 * x + 64, 256)]
        blank = jnp.zeros((32, 128), BF16)
        if x == 0:
            return [blank, rows]
        if x == PLANES - 1:
            return [rows, blank]
        return [rows]

    columns = []
    for at in range(2):
        rows = sum((block(ref, z + at + offset) for ref in refs for offset in range(3)), [])
        columns.append(jnp.concatenate(rows, axis=0))
    return jnp.concatenate(columns, axis=1)


def tile_of(x):
    return slice(32 * x, 32 * x + 32)


def correlate(ref, z, targets):
    rows = jnp.concatenate([near((ref,), z, x) for x in range(PLANES)], axis=1)
    return lax.dot_general(
        rows,
        jnp.concatenate(targets, axis=1),
        (((1,), (1,)), ((), ())),
        preferred_element_type=F32,
    )


def layers(
    width,
    own_ref,
    first_ref,
    second_ref,
    odd_ref,
    weight_ref,
    joint_ref,
    column_ref,
    out_ref,
    p_vol,
    p_hid,
    p_tan,
    p_jv,
    slopes,
    packed,
):
    odd = odd_ref[0] > 0

    @pl.when(odd)
    def _():
        p_vol[0:3] = first_ref[...]
        p_vol[7:10] = second_ref[...]

    @pl.when(jnp.logical_not(odd))
    def _():
        p_vol[0:3] = second_ref[...]
        p_vol[7:10] = first_ref[...]

    p_vol[3:7] = own_ref[...]

    def inside(column):
        at = column_ref[0] + column
        return (at >= 0) & (at < width)

    for z in range(0, 8, 2):
        for x in range(PLANES):
            product = jnp.dot(weight_ref[0:192, :], near((p_vol,), z, x), preferred_element_type=F32)
            for at in range(2):
                part = product[:, 128 * at : 128 * at + 128]
                here = inside(z + at - 2)
                hidden, slope = gelu_pair(fold(part[0:96]))
                tangent = slope * fold(part[96:192])
                p_hid[z + at, tile_of(x)] = jnp.where(here, hidden, 0.0).astype(BF16)
                p_tan[z + at, tile_of(x)] = jnp.where(here, tangent, 0.0).astype(BF16)
                if 2 <= z + at < 6:
                    slopes[z + at - 2, x] = slope

    for z in range(0, 6, 2):
        for x in range(PLANES):
            product = jnp.dot(joint_ref[...], near((p_tan, p_hid), z, x), preferred_element_type=F32)
            for at in range(2):
                jv = fold(product[:, 128 * at : 128 * at + 128])
                jv = jnp.where(inside(z + at - 1), jv, 0.0)
                p_jv[z + at, tile_of(x)] = jv.astype(BF16)

    def spread(tiles):
        both = [
            jnp.concatenate([after(tile), tile, before(tile), jnp.zeros_like(tile)], axis=0)
            for tile in tiles
        ]
        return jnp.concatenate(both, axis=1).astype(BF16)

    sums_first = sums_second = 0.0
    for z in range(0, OWN, 2):
        targets = [
            spread([p_jv[z + at + 1, tile_of(x)].astype(F32) for at in range(2)])
            for x in range(PLANES)
        ]
        sums_second = sums_second + correlate(p_hid, z + 1, targets)
        targets = []
        for x in range(PLANES):
            product = jnp.dot(weight_ref[192:288, :], near((p_jv,), z, x), preferred_element_type=F32)
            tiles = []
            for at in range(2):
                back = slopes[z + at, x] * fold(product[:, 128 * at : 128 * at + 128])
                tiles.append(back.astype(BF16).astype(F32))
            targets.append(spread(tiles))
        sums_first = sums_first + correlate(p_vol, z + 2, targets)

    for g in range(4):
        tiles = [p_jv[1 + i // 2, tile_of(2 * g + i % 2)].astype(F32) for i in range(8)]
        tiles = exchange(tiles, (4, 5, 6))
        for j in range(8):
            out_ref[8 * g + j, 0:32] = tiles[j].astype(BF16)

    rest = pltpu.roll(sums_first, 96, 1)
    packed[0:288] = jnp.where(lanes_of((288, 128)) < 96, sums_second, rest)
    packed[288:432] = jnp.where(
        lanes_of((144, 128)) < 64, rest[0:144], pltpu.roll(rest[144:288], 64, 1)
    )
    packed[432:512] = jnp.zeros((80, 128), F32)
    for member in range(MEMBERS):
        rows = packed[16 * member : 16 * member + 16]
        high = rows.astype(BF16)
        out_ref[member, 32:48] = high
        out_ref[member, 48:64] = (rows - high.astype(F32)).astype(BF16)


def gather_sums(parts_ref, out_ref):
    total = jnp.sum(
        parts_ref[:, 32:48].astype(F32) + parts_ref[:, 48:64].astype(F32), axis=0
    )
    for member in range(8):
        out_ref[member] = total


def combine(parts_ref, out_ref):
    total = jnp.sum(parts_ref[...], axis=0).astype(BF16)
    for member in range(MEMBERS):
        out_ref[member] = total


def finish(scale, packed_ref, d_first_ref, d_second_ref, first_ref, second_ref):
    def damped(summed, damping):
        return scale * summed + damping

    rest = packed_ref[288:432, :].astype(F32)
    rest = jnp.concatenate([rest, pltpu.roll(rest, 64, 1)], axis=0)
    for block in range(9):
        low = packed_ref[32 * block : 32 * block + 32, :].astype(F32)
        far = rest[32 * block : 32 * block + 32]
        at = [9 * (block % 3) + 3 * row + block // 3 for row in range(3)]
        for row in range(3):
            second_ref[at[row]] = damped(low[:, 32 * row : 32 * row + 32], d_second_ref[at[row]])
        first_ref[at[0]] = damped(low[:, 96:128], d_first_ref[at[0]])
        first_ref[at[1]] = damped(far[:, 0:32], d_first_ref[at[1]])
        first_ref[at[2]] = damped(far[:, 32:64], d_first_ref[at[2]])


def filters(w_first_ref, v_first_ref, w_second_ref, v_second_ref, rows_ref, joint_ref):
    def tall(ref):
        return jnp.concatenate(
            [
                jnp.concatenate(
                    [ref[9 * (k % 3) + 3 * row + k // 3].astype(F32) for k in range(9)], axis=0
                )
                for row in range(3)
            ],
            axis=1,
        )

    def turned(refs):
        return jnp.concatenate([tall(ref) for ref in refs], axis=0).T.astype(BF16)

    rows_ref[0:96] = turned([w_first_ref])
    rows_ref[96:192] = turned([v_first_ref])
    joint_ref[...] = turned([w_second_ref, v_second_ref])
    for row in range(3):
        blocks = [
            w_second_ref[26 - (9 * (k % 3) + 3 * row + k // 3)].astype(F32) for k in range(9)
        ]
        rows_ref[192 + 32 * row : 224 + 32 * row] = jnp.concatenate(blocks, axis=1).astype(BF16)


def call(kernel, operands, outputs, scratch, name, limit, flops):
    vmem = pl.BlockSpec(memory_space=pltpu.VMEM)
    smem = pl.BlockSpec(memory_space=pltpu.SMEM)
    return pl.pallas_call(
        kernel,
        out_shape=tuple(jax.ShapeDtypeStruct(shape, dtype) for shape, dtype in outputs),
        in_specs=[smem if x.dtype == jnp.int32 else vmem for x in operands],
        out_specs=(vmem,) * len(outputs),
        scratch_shapes=[pltpu.VMEM(shape, dtype) for shape, dtype in scratch],
        compiler_params=pltpu.CompilerParams(vmem_limit_bytes=limit << 20),
        cost_estimate=pl.CostEstimate(flops=flops, bytes_accessed=1 << 20, transcendentals=0),
        name=name,
    )(*operands)


def body(volume, w_first, w_second, v_first, v_second):
    channels, depth, height, width = volume.shape
    n_gx, n_gy, n_gz = (lax.axis_size(axis) for axis in AXES)
    members = n_gx * n_gy
    count_all = float(depth * n_gx * height * n_gy * width * n_gz)
    factor = math.sqrt(27.0 * channels)
    small = (channels, 128)

    (sent,) = call(pack, (volume,), [((members,) + small, BF16)], [((1024, 128), F32)], "pack", 8, 10**8)
    parts = lax.all_to_all(sent, GROUP, 0, 0)

    z = (lax.axis_index("gy") // 4) * 4 + lax.axis_index("gx")
    x = lax.axis_index("gy") & 3
    place = jnp.where(x == 0, 31 - z, 3 * z + jnp.where((z & 1) == 0, x - 1, 3 - x))
    odd = (place & 1).reshape(1)
    column = (OWN * (lax.axis_index("gz") * members + place)).reshape(1)
    blocks = [w.reshape(27, channels, channels) for w in (w_first, v_first, w_second, v_second)]
    weights = call(
        filters, blocks, [((288, 288), BF16), ((96, 576), BF16)], [], "filters", 8, 2 * 10**8
    )
    damping = tuple(
        factor * 0.1 * v.astype(F32).reshape(27, channels, channels) for v in (v_first, v_second)
    )
    parts, odd, column, weights, damping = lax.optimization_barrier(
        (parts, odd, column, weights, damping)
    )

    halo = ((OWN - 1, 256, 128), BF16)
    own, first, second = call(
        arrange, (parts, odd), [((OWN, 256, 128), BF16), halo, halo], [], "arrange", 8, 10**8
    )

    def swapped(start):
        def device(at):
            return LINE[at % members] * n_gz + at // members

        pairs = [(device(i), device(i + 1)) for i in range(start, members * n_gz - 1, 2)]
        return pairs + [(b, a) for a, b in pairs]

    first = lax.ppermute(first, AXES, swapped(0))
    second = lax.ppermute(second, AXES, swapped(1))

    (leaving,) = call(
        lambda *refs: layers(width * n_gz, *refs),
        (own, first, second, odd, *weights, column),
        [((members, 64, 128), BF16)],
        [
            ((10, 256, 128), BF16),
            ((8, 256, 128), BF16),
            ((8, 256, 128), BF16),
            ((6, 256, 128), BF16),
            ((OWN, PLANES) + small, F32),
            ((512, 128), F32),
        ],
        "layers",
        24,
        8 * 10**9,
    )

    parts = lax.all_to_all(leaving, GROUP, 0, 0)
    (sums,) = call(gather_sums, (parts,), [((n_gz, 16, 128), F32)], [], "gather_sums", 8, 10**8)
    sums = lax.all_to_all(sums, "gz", 0, 0)
    (every,) = call(combine, (sums,), [((members, 16, 128), BF16)], [], "combine", 8, 10**8)
    every = lax.all_to_all(every, GROUP, 0, 0).reshape(512, 128)
    (out,) = call(
        unpack,
        (parts,),
        [(volume.shape, BF16)],
        [((1024, 128), F32)],
        "unpack",
        8,
        10**9,
    )
    gv_first, gv_second = call(
        lambda *refs: finish(factor / count_all, *refs),
        (every,) + damping,
        [((27, channels, channels), F32)] * 2,
        [],
        "finish",
        8,
        10**8,
    )
    return (out, gv_first.reshape(v_first.shape), gv_second.reshape(v_first.shape))


def solution(mesh):
    in_specs = (P(None, "gx", "gy", "gz"), P(), P(), P(), P())
    out_specs = (P(None, "gx", "gy", "gz"), P(), P())
    return jax.shard_map(body, mesh=mesh, in_specs=in_specs, out_specs=out_specs, check_vma=False)
```

```python
import math

import jax
import jax.numpy as jnp
from jax import lax
from jax.experimental import pallas as pl
from jax.experimental.pallas import tpu as pltpu
from jax.sharding import PartitionSpec as P

F32 = jnp.float32
BF16 = jnp.bfloat16
AXES = ("gx", "gy", "gz")
GROUP = ("gx", "gy")
PLANES = 8
OWN = 4
MEMBERS = 32


def closed_line():
    def member(z, x):
        return (z % 4) * 8 + (z // 4) * 4 + x

    line = []
    for z in range(8):
        line += [member(z, x) for x in ((1, 2, 3) if z % 2 == 0 else (3, 2, 1))]
    return tuple(line + [member(z, 0) for z in reversed(range(8))])


LINE = closed_line()


def lanes_of(shape):
    return lax.broadcasted_iota(jnp.int32, shape, len(shape) - 1)


def exchange(tiles, bits):
    tiles = list(tiles)
    lane = lanes_of(tiles[0].shape)
    for place, bit in enumerate(bits):
        step = 1 << bit
        clear = (lane & step) == 0
        for low in range(len(tiles)):
            if low & (1 << place):
                continue
            high = low | (1 << place)
            a, b = tiles[low], tiles[high]
            tiles[low] = jnp.where(clear, a, pltpu.roll(b, step, 1))
            tiles[high] = jnp.where(clear, pltpu.roll(a, 128 - step, 1), b)
    return tiles


def permutation(inverse):
    source = lax.broadcasted_iota(jnp.int32, (128, 128), 0)
    target = lax.broadcasted_iota(jnp.int32, (128, 128), 1)
    if inverse:
        source, target = target, source
    hit = source == 4 * (target & 31) + (target >> 5)
    return jnp.where(hit, 1.0, 0.0).astype(BF16)


def pack(cells_ref, out_ref, sorted_ref):
    sorted_ref[...] = jnp.dot(
        cells_ref[...].reshape(256, 128), permutation(False), preferred_element_type=F32
    )
    tiles = exchange([sorted_ref[pl.ds(i, 8, stride=32)] for i in range(32)], (0, 1, 2, 3, 4))
    for i in range(MEMBERS):
        out_ref[LINE[i]] = tiles[i].astype(BF16)


def arrange(parts_ref, odd_ref, own_ref, first_ref, second_ref):
    for g in range(4):
        tiles = exchange([parts_ref[8 * g + j].astype(F32) for j in range(8)], (4, 5, 6))
        for i in range(8):
            plane = 2 * g + i % 2
            own_ref[i // 2, 32 * plane : 32 * plane + 32] = tiles[i].astype(BF16)
    odd = odd_ref[0] > 0

    @pl.when(odd)
    def _():
        first_ref[...] = own_ref[0:3]
        second_ref[...] = own_ref[1:4]

    @pl.when(jnp.logical_not(odd))
    def _():
        first_ref[...] = own_ref[1:4]
        second_ref[...] = own_ref[0:3]


def unpack(parts_ref, out_ref, mixed_ref):
    for part in range(2):
        at = slice(16 * part, 16 * part + 16)
        tiles = [parts_ref[LINE[i], at].astype(F32) for i in range(MEMBERS)]
        tiles = exchange(tiles, (0, 1, 2, 3, 4))
        for i in range(32):
            mixed_ref[pl.ds(512 * part + i, 16, stride=32)] = tiles[i]
    moved = jnp.dot(mixed_ref[...].astype(BF16), permutation(True), preferred_element_type=F32)
    out_ref[...] = moved.astype(BF16).reshape(32, 2, 16, 128)


def gelu_pair(pre):
    inner = 0.7978845608 * (pre + 0.044715 * pre * pre * pre)
    hyper = jnp.tanh(inner)
    hidden = 0.5 * pre * (1.0 + hyper)
    slope = 0.5 * (1.0 + hyper) + 0.5 * pre * (1.0 - hyper * hyper) * 0.7978845608 * (
        1.0 + 0.134145 * pre * pre
    )
    return hidden, slope


def before(value):
    return jnp.where(lanes_of(value.shape) > 0, pltpu.roll(value, 1, 1), 0.0)


def after(value):
    return jnp.where(lanes_of(value.shape) < 127, pltpu.roll(value, 127, 1), 0.0)


def fold(product):
    return before(product[0:32]) + product[32:64] + after(product[64:96])


def near(refs, z, x):
    def block(ref, at):
        rows = ref[at, max(32 * x - 32, 0) : min(32 * x + 64, 256)]
        blank = jnp.zeros((32, 128), BF16)
        if x == 0:
            return [blank, rows]
        if x == PLANES - 1:
            return [rows, blank]
        return [rows]

    columns = []
    for at in range(2):
        rows = sum((block(ref, z + at + offset) for ref in refs for offset in range(3)), [])
        columns.append(jnp.concatenate(rows, axis=0))
    return jnp.concatenate(columns, axis=1)


def tile_of(x):
    return slice(32 * x, 32 * x + 32)


def correlate(ref, z, targets):
    rows = jnp.concatenate([near((ref,), z, x) for x in range(PLANES)], axis=1)
    return lax.dot_general(
        rows,
        jnp.concatenate(targets, axis=1),
        (((1,), (1,)), ((), ())),
        preferred_element_type=F32,
    )


def layers(
    width,
    own_ref,
    first_ref,
    second_ref,
    odd_ref,
    weight_ref,
    joint_ref,
    column_ref,
    out_ref,
    p_vol,
    p_hid,
    p_tan,
    p_jv,
    slopes,
    packed,
):
    odd = odd_ref[0] > 0

    @pl.when(odd)
    def _():
        p_vol[0:3] = first_ref[...]
        p_vol[7:10] = second_ref[...]

    @pl.when(jnp.logical_not(odd))
    def _():
        p_vol[0:3] = second_ref[...]
        p_vol[7:10] = first_ref[...]

    p_vol[3:7] = own_ref[...]

    def inside(column):
        at = column_ref[0] + column
        return (at >= 0) & (at < width)

    for z in range(0, 8, 2):
        for x in range(PLANES):
            product = jnp.dot(weight_ref[0:192, :], near((p_vol,), z, x), preferred_element_type=F32)
            for at in range(2):
                part = product[:, 128 * at : 128 * at + 128]
                here = inside(z + at - 2)
                hidden, slope = gelu_pair(fold(part[0:96]))
                tangent = slope * fold(part[96:192])
                p_hid[z + at, tile_of(x)] = jnp.where(here, hidden, 0.0).astype(BF16)
                p_tan[z + at, tile_of(x)] = jnp.where(here, tangent, 0.0).astype(BF16)
                if 2 <= z + at < 6:
                    slopes[z + at - 2, x] = slope

    for z in range(0, 6, 2):
        for x in range(PLANES):
            product = jnp.dot(joint_ref[...], near((p_tan, p_hid), z, x), preferred_element_type=F32)
            for at in range(2):
                jv = fold(product[:, 128 * at : 128 * at + 128])
                jv = jnp.where(inside(z + at - 1), jv, 0.0)
                p_jv[z + at, tile_of(x)] = jv.astype(BF16)

    def spread(tiles):
        both = [
            jnp.concatenate([after(tile), tile, before(tile), jnp.zeros_like(tile)], axis=0)
            for tile in tiles
        ]
        return jnp.concatenate(both, axis=1).astype(BF16)

    sums_first = sums_second = 0.0
    for z in range(0, OWN, 2):
        targets = [
            spread([p_jv[z + at + 1, tile_of(x)].astype(F32) for at in range(2)])
            for x in range(PLANES)
        ]
        sums_second = sums_second + correlate(p_hid, z + 1, targets)
        targets = []
        for x in range(PLANES):
            product = jnp.dot(weight_ref[192:288, :], near((p_jv,), z, x), preferred_element_type=F32)
            tiles = []
            for at in range(2):
                back = slopes[z + at, x] * fold(product[:, 128 * at : 128 * at + 128])
                tiles.append(back.astype(BF16).astype(F32))
            targets.append(spread(tiles))
        sums_first = sums_first + correlate(p_vol, z + 2, targets)

    for g in range(4):
        tiles = [p_jv[1 + i // 2, tile_of(2 * g + i % 2)].astype(F32) for i in range(8)]
        tiles = exchange(tiles, (4, 5, 6))
        for j in range(8):
            out_ref[8 * g + j, 0:32] = tiles[j].astype(BF16)

    rest = pltpu.roll(sums_first, 96, 1)
    packed[0:288] = jnp.where(lanes_of((288, 128)) < 96, sums_second, rest)
    packed[288:432] = jnp.where(
        lanes_of((144, 128)) < 64, rest[0:144], pltpu.roll(rest[144:288], 64, 1)
    )
    packed[432:512] = jnp.zeros((80, 128), F32)
    for member in range(MEMBERS):
        out_ref[member, 32:48] = packed[16 * member : 16 * member + 16].astype(BF16)


def gather_sums(parts_ref, out_ref):
    total = jnp.sum(parts_ref[:, 32:48].astype(F32), axis=0)
    for member in range(8):
        out_ref[member] = total


def combine(parts_ref, out_ref):
    total = jnp.sum(parts_ref[...], axis=0).astype(BF16)
    for member in range(MEMBERS):
        out_ref[member] = total


def finish(scale, packed_ref, d_first_ref, d_second_ref, first_ref, second_ref, rest_ref):
    depth = pl.program_id(0)

    @pl.when(depth == 0)
    def _():
        rest = packed_ref[288:432, :].astype(F32)
        rest_ref[0:144] = rest
        rest_ref[144:288] = pltpu.roll(rest, 64, 1)

    def damped(summed, damping):
        return scale * summed + damping

    for column in range(3):
        block = pl.ds(pl.multiple_of(96 * column + 32 * depth, 32), 32)
        low = packed_ref[block, :].astype(F32)
        far = rest_ref[block, :]
        for row in range(3):
            at = 3 * row + column
            second_ref[at] = damped(low[:, 32 * row : 32 * row + 32], d_second_ref[at])
        first_ref[column] = damped(low[:, 96:128], d_first_ref[column])
        first_ref[3 + column] = damped(far[:, 0:32], d_first_ref[3 + column])
        first_ref[6 + column] = damped(far[:, 32:64], d_first_ref[6 + column])


def filters(w_first_ref, v_first_ref, w_second_ref, v_second_ref, rows_ref, joint_ref):
    def tall(ref):
        return jnp.concatenate(
            [
                jnp.concatenate(
                    [ref[9 * (k % 3) + 3 * row + k // 3].astype(F32) for k in range(9)], axis=0
                )
                for row in range(3)
            ],
            axis=1,
        )

    def turned(refs):
        return jnp.concatenate([tall(ref) for ref in refs], axis=0).T.astype(BF16)

    rows_ref[0:96] = turned([w_first_ref])
    rows_ref[96:192] = turned([v_first_ref])
    joint_ref[...] = turned([w_second_ref, v_second_ref])
    for row in range(3):
        blocks = [
            w_second_ref[26 - (9 * (k % 3) + 3 * row + k // 3)].astype(F32) for k in range(9)
        ]
        rows_ref[192 + 32 * row : 224 + 32 * row] = jnp.concatenate(blocks, axis=1).astype(BF16)


def call(kernel, operands, outputs, scratch, name, limit, flops):
    vmem = pl.BlockSpec(memory_space=pltpu.VMEM)
    smem = pl.BlockSpec(memory_space=pltpu.SMEM)
    return pl.pallas_call(
        kernel,
        out_shape=tuple(jax.ShapeDtypeStruct(shape, dtype) for shape, dtype in outputs),
        in_specs=[smem if x.dtype == jnp.int32 else vmem for x in operands],
        out_specs=(vmem,) * len(outputs),
        scratch_shapes=[pltpu.VMEM(shape, dtype) for shape, dtype in scratch],
        compiler_params=pltpu.CompilerParams(vmem_limit_bytes=limit << 20),
        cost_estimate=pl.CostEstimate(flops=flops, bytes_accessed=1 << 20, transcendentals=0),
        name=name,
    )(*operands)


def body(volume, w_first, w_second, v_first, v_second):
    channels, depth, height, width = volume.shape
    n_gx, n_gy, n_gz = (lax.axis_size(axis) for axis in AXES)
    members = n_gx * n_gy
    count_all = float(depth * n_gx * height * n_gy * width * n_gz)
    factor = math.sqrt(27.0 * channels)
    small = (channels, 128)

    sent = pl.pallas_call(
        pack,
        grid=(channels // 8,),
        out_shape=jax.ShapeDtypeStruct((members,) + small, BF16),
        in_specs=[pl.BlockSpec((8, depth, height, width), lambda i: (i, 0, 0, 0))],
        out_specs=pl.BlockSpec((members, 8, 128), lambda i: (0, i, 0)),
        scratch_shapes=[pltpu.VMEM((256, 128), F32)],
        compiler_params=pltpu.CompilerParams(dimension_semantics=("arbitrary",)),
        name="pack",
    )(volume)
    parts = lax.all_to_all(sent, GROUP, 0, 0)

    z = (lax.axis_index("gy") // 4) * 4 + lax.axis_index("gx")
    x = lax.axis_index("gy") & 3
    place = jnp.where(x == 0, 31 - z, 3 * z + jnp.where((z & 1) == 0, x - 1, 3 - x))
    odd = (place & 1).reshape(1)
    column = (OWN * (lax.axis_index("gz") * members + place)).reshape(1)
    blocks = [w.reshape(27, channels, channels) for w in (w_first, v_first, w_second, v_second)]
    weights = call(
        filters, blocks, [((288, 288), BF16), ((96, 576), BF16)], [], "filters", 8, 2 * 10**8
    )
    damping = tuple(
        factor * 0.1 * v.astype(F32).reshape(27, channels, channels) for v in (v_first, v_second)
    )
    parts, odd, column, weights, damping = lax.optimization_barrier(
        (parts, odd, column, weights, damping)
    )

    halo = ((OWN - 1, 256, 128), BF16)
    own, first, second = call(
        arrange, (parts, odd), [((OWN, 256, 128), BF16), halo, halo], [], "arrange", 8, 10**8
    )

    def swapped(start):
        def device(at):
            return LINE[at % members] * n_gz + at // members

        pairs = [(device(i), device(i + 1)) for i in range(start, members * n_gz - 1, 2)]
        return pairs + [(b, a) for a, b in pairs]

    first = lax.ppermute(first, AXES, swapped(0))
    second = lax.ppermute(second, AXES, swapped(1))

    (leaving,) = call(
        lambda *refs: layers(width * n_gz, *refs),
        (own, first, second, odd, *weights, column),
        [((members, 48, 128), BF16)],
        [
            ((10, 256, 128), BF16),
            ((8, 256, 128), BF16),
            ((8, 256, 128), BF16),
            ((6, 256, 128), BF16),
            ((OWN, PLANES) + small, F32),
            ((512, 128), F32),
        ],
        "layers",
        24,
        8 * 10**9,
    )

    parts = lax.all_to_all(leaving, GROUP, 0, 0)
    (sums,) = call(gather_sums, (parts,), [((n_gz, 16, 128), F32)], [], "gather_sums", 8, 10**8)
    sums = lax.all_to_all(sums, "gz", 0, 0)
    (every,) = call(combine, (sums,), [((members, 16, 128), BF16)], [], "combine", 8, 10**8)
    every = lax.all_to_all(every, GROUP, 0, 0).reshape(512, 128)
    (out,) = call(
        unpack,
        (parts,),
        [(volume.shape, BF16)],
        [((1024, 128), F32)],
        "unpack",
        8,
        10**9,
    )
    third = pl.BlockSpec((9, channels, channels), lambda i: (i, 0, 0))
    gv_first, gv_second = pl.pallas_call(
        lambda *refs: finish(factor / count_all, *refs),
        grid=(3,),
        out_shape=(jax.ShapeDtypeStruct((27, channels, channels), F32),) * 2,
        in_specs=[pl.BlockSpec((512, 128), lambda i: (0, 0)), third, third],
        out_specs=(third, third),
        scratch_shapes=[pltpu.VMEM((288, 128), F32)],
        compiler_params=pltpu.CompilerParams(
            dimension_semantics=("arbitrary",), vmem_limit_bytes=8 << 20
        ),
        name="finish",
    )(every, *damping)
    return (out, gv_first.reshape(v_first.shape), gv_second.reshape(v_first.shape))


def solution(mesh):
    in_specs = (P(None, "gx", "gy", "gz"), P(), P(), P(), P())
    out_specs = (P(None, "gx", "gy", "gz"), P(), P())
    return jax.shard_map(body, mesh=mesh, in_specs=in_specs, out_specs=out_specs, check_vma=False)
```

```python
import math

import jax
import jax.numpy as jnp
from jax import lax
from jax.experimental import pallas as pl
from jax.experimental.pallas import tpu as pltpu
from jax.sharding import PartitionSpec as P

F32 = jnp.float32
BF16 = jnp.bfloat16
AXES = ("gx", "gy", "gz")
GROUP = ("gx", "gy")
PLANES = 8
OWN = 4
MEMBERS = 32


CHIPS = (
    (
        0, 1, 11, 10, 13, 3, 2, 12, 22, 23, 20, 21, 31, 32, 33, 30,
        40, 43, 42, 41, 51, 50, 53, 52, 62, 61, 71, 72, 73, 63, 60, 70,
    ),
    (
        70, 71, 1, 2, 72, 62, 63, 53, 43, 33, 23, 13, 12, 11, 21, 22,
        32, 42, 52, 51, 61, 60, 50, 40, 41, 31, 30, 20, 10, 0, 3, 73,
    ),
)
LINES = tuple(tuple(c // 10 % 4 * 8 + c // 40 * 4 + c % 10 for c in chips) for chips in CHIPS)


def member_at(place):
    return jnp.where((lax.axis_index("gz") & 1) == 0, LINES[0][place], LINES[1][place])


def own_place():
    member = lax.axis_index("gx") * 8 + lax.axis_index("gy")
    place = jnp.int32(0)
    for at in range(MEMBERS):
        place = jnp.where(member == member_at(at), at, place)
    return place


def lanes_of(shape):
    return lax.broadcasted_iota(jnp.int32, shape, len(shape) - 1)


def exchange(tiles, bits):
    tiles = list(tiles)
    lane = lanes_of(tiles[0].shape)
    for place, bit in enumerate(bits):
        step = 1 << bit
        clear = (lane & step) == 0
        for low in range(len(tiles)):
            if low & (1 << place):
                continue
            high = low | (1 << place)
            a, b = tiles[low], tiles[high]
            tiles[low] = jnp.where(clear, a, pltpu.roll(b, step, 1))
            tiles[high] = jnp.where(clear, pltpu.roll(a, 128 - step, 1), b)
    return tiles


def permutation(inverse):
    source = lax.broadcasted_iota(jnp.int32, (128, 128), 0)
    target = lax.broadcasted_iota(jnp.int32, (128, 128), 1)
    if inverse:
        source, target = target, source
    hit = source == 4 * (target & 31) + (target >> 5)
    return jnp.where(hit, 1.0, 0.0).astype(BF16)


def pack(cells_ref, out_ref, sorted_ref):
    sorted_ref[...] = jnp.dot(
        cells_ref[...].reshape(1024, 128), permutation(False), preferred_element_type=F32
    )
    for part in range(4):
        tiles = [sorted_ref[pl.ds(256 * part + i, 8, stride=32)] for i in range(32)]
        tiles = exchange(tiles, (0, 1, 2, 3, 4))
        for i in range(MEMBERS):
            out_ref[member_at(i), 8 * part : 8 * part + 8] = tiles[i].astype(BF16)


def arrange(parts_ref, own_ref, first_ref, second_ref):
    for g in range(4):
        tiles = exchange([parts_ref[8 * g + j].astype(F32) for j in range(8)], (4, 5, 6))
        for i in range(8):
            plane = 2 * g + i % 2
            own_ref[i // 2, 32 * plane : 32 * plane + 32] = tiles[i].astype(BF16)
    odd = (own_place() & 1) == 1

    @pl.when(odd)
    def _():
        first_ref[...] = own_ref[0:3]
        second_ref[...] = own_ref[1:4]

    @pl.when(jnp.logical_not(odd))
    def _():
        first_ref[...] = own_ref[1:4]
        second_ref[...] = own_ref[0:3]


def unpack(parts_ref, out_ref, mixed_ref):
    for part in range(2):
        at = slice(16 * part, 16 * part + 16)
        tiles = [parts_ref[member_at(i), at].astype(F32) for i in range(MEMBERS)]
        tiles = exchange(tiles, (0, 1, 2, 3, 4))
        for i in range(32):
            mixed_ref[pl.ds(512 * part + i, 16, stride=32)] = tiles[i]
    moved = jnp.dot(mixed_ref[...].astype(BF16), permutation(True), preferred_element_type=F32)
    out_ref[...] = moved.astype(BF16).reshape(32, 2, 16, 128)


def gelu_pair(pre):
    inner = 0.7978845608 * (pre + 0.044715 * pre * pre * pre)
    hyper = jnp.tanh(inner)
    hidden = 0.5 * pre * (1.0 + hyper)
    slope = 0.5 * (1.0 + hyper) + 0.5 * pre * (1.0 - hyper * hyper) * 0.7978845608 * (
        1.0 + 0.134145 * pre * pre
    )
    return hidden, slope


def before(value):
    return jnp.where(lanes_of(value.shape) > 0, pltpu.roll(value, 1, 1), 0.0)


def after(value):
    return jnp.where(lanes_of(value.shape) < 127, pltpu.roll(value, 127, 1), 0.0)


def fold(product):
    return before(product[0:32]) + product[32:64] + after(product[64:96])


def near(refs, z, x):
    def block(ref, at):
        rows = ref[at, max(32 * x - 32, 0) : min(32 * x + 64, 256)]
        blank = jnp.zeros((32, 128), BF16)
        if x == 0:
            return [blank, rows]
        if x == PLANES - 1:
            return [rows, blank]
        return [rows]

    columns = []
    for at in range(2):
        rows = sum((block(ref, z + at + offset) for ref in refs for offset in range(3)), [])
        columns.append(jnp.concatenate(rows, axis=0))
    return jnp.concatenate(columns, axis=1)


def tile_of(x):
    return slice(32 * x, 32 * x + 32)


def correlate(ref, z, targets):
    rows = jnp.concatenate([near((ref,), z, x) for x in range(PLANES)], axis=1)
    return lax.dot_general(
        rows,
        jnp.concatenate(targets, axis=1),
        (((1,), (1,)), ((), ())),
        preferred_element_type=F32,
    )


def layers(
    width,
    own_ref,
    first_ref,
    second_ref,
    weight_ref,
    joint_ref,
    out_ref,
    p_vol,
    p_hid,
    p_tan,
    p_jv,
    slopes,
    packed,
):
    place = own_place()
    column = OWN * (lax.axis_index("gz") * MEMBERS + place)
    odd = (place & 1) == 1

    @pl.when(odd)
    def _():
        p_vol[0:3] = first_ref[...]
        p_vol[7:10] = second_ref[...]

    @pl.when(jnp.logical_not(odd))
    def _():
        p_vol[0:3] = second_ref[...]
        p_vol[7:10] = first_ref[...]

    p_vol[3:7] = own_ref[...]

    def inside(offset):
        return (column + offset >= 0) & (column + offset < width)

    for z in range(0, 8, 2):
        for x in range(PLANES):
            product = jnp.dot(weight_ref[0:192, :], near((p_vol,), z, x), preferred_element_type=F32)
            for at in range(2):
                part = product[:, 128 * at : 128 * at + 128]
                here = inside(z + at - 2)
                hidden, slope = gelu_pair(fold(part[0:96]))
                tangent = slope * fold(part[96:192])
                p_hid[z + at, tile_of(x)] = jnp.where(here, hidden, 0.0).astype(BF16)
                p_tan[z + at, tile_of(x)] = jnp.where(here, tangent, 0.0).astype(BF16)
                if 2 <= z + at < 6:
                    slopes[z + at - 2, x] = slope

    for z in range(0, 6, 2):
        for x in range(PLANES):
            product = jnp.dot(joint_ref[...], near((p_tan, p_hid), z, x), preferred_element_type=F32)
            for at in range(2):
                jv = fold(product[:, 128 * at : 128 * at + 128])
                jv = jnp.where(inside(z + at - 1), jv, 0.0)
                p_jv[z + at, tile_of(x)] = jv.astype(BF16)

    def spread(tiles):
        both = [
            jnp.concatenate([after(tile), tile, before(tile), jnp.zeros_like(tile)], axis=0)
            for tile in tiles
        ]
        return jnp.concatenate(both, axis=1).astype(BF16)

    sums_first = sums_second = 0.0
    for z in range(0, OWN, 2):
        targets = [
            spread([p_jv[z + at + 1, tile_of(x)].astype(F32) for at in range(2)])
            for x in range(PLANES)
        ]
        sums_second = sums_second + correlate(p_hid, z + 1, targets)
        targets = []
        for x in range(PLANES):
            product = jnp.dot(weight_ref[192:288, :], near((p_jv,), z, x), preferred_element_type=F32)
            tiles = []
            for at in range(2):
                back = slopes[z + at, x] * fold(product[:, 128 * at : 128 * at + 128])
                tiles.append(back.astype(BF16).astype(F32))
            targets.append(spread(tiles))
        sums_first = sums_first + correlate(p_vol, z + 2, targets)

    for g in range(4):
        tiles = [p_jv[1 + i // 2, tile_of(2 * g + i % 2)].astype(F32) for i in range(8)]
        tiles = exchange(tiles, (4, 5, 6))
        for j in range(8):
            out_ref[8 * g + j, 0:32] = tiles[j].astype(BF16)

    rest = pltpu.roll(sums_first, 96, 1)
    packed[0:288] = jnp.where(lanes_of((288, 128)) < 96, sums_second, rest)
    packed[288:432] = jnp.where(
        lanes_of((144, 128)) < 64, rest[0:144], pltpu.roll(rest[144:288], 64, 1)
    )
    packed[432:512] = jnp.zeros((80, 128), F32)
    for member in range(MEMBERS):
        out_ref[member, 32:48] = packed[16 * member : 16 * member + 16].astype(BF16)


def gather_sums(parts_ref, out_ref):
    total = jnp.sum(parts_ref[:, 32:48].astype(F32), axis=0)
    for member in range(8):
        out_ref[member] = total


def combine(parts_ref, out_ref):
    total = jnp.sum(parts_ref[...], axis=0).astype(BF16)
    for member in range(MEMBERS):
        out_ref[member] = total


def finish(scale, packed_ref, d_first_ref, d_second_ref, first_ref, second_ref, rest_ref):
    depth = pl.program_id(0)

    @pl.when(depth == 0)
    def _():
        rest = packed_ref[288:432, :].astype(F32)
        rest_ref[0:144] = rest
        rest_ref[144:288] = pltpu.roll(rest, 64, 1)

    def damped(summed, damping):
        return scale * summed + damping

    for column in range(3):
        block = pl.ds(pl.multiple_of(96 * column + 32 * depth, 32), 32)
        low = packed_ref[block, :].astype(F32)
        far = rest_ref[block, :]
        for row in range(3):
            at = 3 * row + column
            second_ref[at] = damped(low[:, 32 * row : 32 * row + 32], d_second_ref[at])
        first_ref[column] = damped(low[:, 96:128], d_first_ref[column])
        first_ref[3 + column] = damped(far[:, 0:32], d_first_ref[3 + column])
        first_ref[6 + column] = damped(far[:, 32:64], d_first_ref[6 + column])


def filters(w_first_ref, v_first_ref, w_second_ref, v_second_ref, rows_ref, joint_ref):
    def tall(ref):
        return jnp.concatenate(
            [
                jnp.concatenate(
                    [ref[9 * (k % 3) + 3 * row + k // 3].astype(F32) for k in range(9)], axis=0
                )
                for row in range(3)
            ],
            axis=1,
        )

    def turned(refs):
        return jnp.concatenate([tall(ref) for ref in refs], axis=0).T.astype(BF16)

    rows_ref[0:96] = turned([w_first_ref])
    rows_ref[96:192] = turned([v_first_ref])
    joint_ref[...] = turned([w_second_ref, v_second_ref])
    for row in range(3):
        blocks = [
            w_second_ref[26 - (9 * (k % 3) + 3 * row + k // 3)].astype(F32) for k in range(9)
        ]
        rows_ref[192 + 32 * row : 224 + 32 * row] = jnp.concatenate(blocks, axis=1).astype(BF16)


def call(kernel, operands, outputs, scratch, name, limit, flops):
    vmem = pl.BlockSpec(memory_space=pltpu.VMEM)
    return pl.pallas_call(
        kernel,
        out_shape=tuple(jax.ShapeDtypeStruct(shape, dtype) for shape, dtype in outputs),
        in_specs=[vmem] * len(operands),
        out_specs=(vmem,) * len(outputs),
        scratch_shapes=[pltpu.VMEM(shape, dtype) for shape, dtype in scratch],
        compiler_params=pltpu.CompilerParams(vmem_limit_bytes=limit << 20),
        cost_estimate=pl.CostEstimate(flops=flops, bytes_accessed=1 << 20, transcendentals=0),
        name=name,
    )(*operands)


def body(volume, w_first, w_second, v_first, v_second):
    channels, depth, height, width = volume.shape
    n_gx, n_gy, n_gz = (lax.axis_size(axis) for axis in AXES)
    members = n_gx * n_gy
    count_all = float(depth * n_gx * height * n_gy * width * n_gz)
    factor = math.sqrt(27.0 * channels)
    small = (channels, 128)

    (sent,) = call(
        pack, (volume,), [((members,) + small, BF16)], [((1024, 128), F32)], "pack", 8, 10**8
    )
    parts = lax.all_to_all(sent, GROUP, 0, 0)

    blocks = [w.reshape(27, channels, channels) for w in (w_first, v_first, w_second, v_second)]
    weights = call(
        filters, blocks, [((288, 288), BF16), ((96, 576), BF16)], [], "filters", 8, 2 * 10**8
    )
    damping = tuple(
        factor * 0.1 * v.astype(F32).reshape(27, channels, channels) for v in (v_first, v_second)
    )
    parts, weights, damping = lax.optimization_barrier((parts, weights, damping))

    halo = ((OWN - 1, 256, 128), BF16)
    own, first, second = call(
        arrange, (parts,), [((OWN, 256, 128), BF16), halo, halo], [], "arrange", 8, 10**8
    )

    def swapped(start):
        def device(at):
            gz, place = divmod(at, members)
            return LINES[gz % 2][place] * n_gz + gz

        pairs = [(device(i), device(i + 1)) for i in range(start, members * n_gz - 1, 2)]
        return pairs + [(b, a) for a, b in pairs]

    first = lax.ppermute(first, AXES, swapped(0))
    second = lax.ppermute(second, AXES, swapped(1))

    (leaving,) = call(
        lambda *refs: layers(width * n_gz, *refs),
        (own, first, second, *weights),
        [((members, 48, 128), BF16)],
        [
            ((10, 256, 128), BF16),
            ((8, 256, 128), BF16),
            ((8, 256, 128), BF16),
            ((6, 256, 128), BF16),
            ((OWN, PLANES) + small, F32),
            ((512, 128), F32),
        ],
        "layers",
        24,
        8 * 10**9,
    )

    parts = lax.all_to_all(leaving, GROUP, 0, 0)
    (sums,) = call(gather_sums, (parts,), [((n_gz, 16, 128), F32)], [], "gather_sums", 8, 10**8)
    sums = lax.all_to_all(sums, "gz", 0, 0)
    (every,) = call(combine, (sums,), [((members, 16, 128), BF16)], [], "combine", 8, 10**8)
    every = lax.all_to_all(every, GROUP, 0, 0).reshape(512, 128)
    (out,) = call(
        unpack,
        (parts,),
        [(volume.shape, BF16)],
        [((1024, 128), F32)],
        "unpack",
        8,
        10**9,
    )
    third = pl.BlockSpec((9, channels, channels), lambda i: (i, 0, 0))
    gv_first, gv_second = pl.pallas_call(
        lambda *refs: finish(factor / count_all, *refs),
        grid=(3,),
        out_shape=(jax.ShapeDtypeStruct((27, channels, channels), F32),) * 2,
        in_specs=[pl.BlockSpec((512, 128), lambda i: (0, 0)), third, third],
        out_specs=(third, third),
        scratch_shapes=[pltpu.VMEM((288, 128), F32)],
        compiler_params=pltpu.CompilerParams(
            dimension_semantics=("arbitrary",), vmem_limit_bytes=8 << 20
        ),
        name="finish",
    )(every, *damping)
    return (out, gv_first.reshape(v_first.shape), gv_second.reshape(v_first.shape))


def solution(mesh):
    in_specs = (P(None, "gx", "gy", "gz"), P(), P(), P(), P())
    out_specs = (P(None, "gx", "gy", "gz"), P(), P())
    return jax.shard_map(body, mesh=mesh, in_specs=in_specs, out_specs=out_specs, check_vma=False)
```

```python
import math

import jax
import jax.numpy as jnp
from jax import lax
from jax.experimental import pallas as pl
from jax.experimental.pallas import tpu as pltpu
from jax.sharding import PartitionSpec as P

F32 = jnp.float32
BF16 = jnp.bfloat16
AXES = ("gx", "gy", "gz")
GROUP = ("gx", "gy")
PLANES = 8
OWN = 4
MEMBERS = 32


def snake():
    def member(z, x):
        return z % 4 * 8 + z // 4 * 4 + x

    line = []
    for z in range(8):
        line += [member(z, x) for x in ((1, 2, 3) if z % 2 == 0 else (3, 2, 1))]
    return tuple(line + [member(z, 0) for z in reversed(range(8))])


LINES = (snake(), snake()[:1] + snake()[:0:-1])


def member_at(place):
    return jnp.where((lax.axis_index("gz") & 1) == 0, LINES[0][place], LINES[1][place])


def own_place():
    member = lax.axis_index("gx") * 8 + lax.axis_index("gy")
    place = jnp.int32(0)
    for at in range(MEMBERS):
        place = jnp.where(member == member_at(at), at, place)
    return place


def lanes_of(shape):
    return lax.broadcasted_iota(jnp.int32, shape, len(shape) - 1)


def exchange(tiles, bits):
    tiles = list(tiles)
    lane = lanes_of(tiles[0].shape)
    for place, bit in enumerate(bits):
        step = 1 << bit
        clear = (lane & step) == 0
        for low in range(len(tiles)):
            if low & (1 << place):
                continue
            high = low | (1 << place)
            a, b = tiles[low], tiles[high]
            tiles[low] = jnp.where(clear, a, pltpu.roll(b, step, 1))
            tiles[high] = jnp.where(clear, pltpu.roll(a, 128 - step, 1), b)
    return tiles


def permutation(inverse):
    source = lax.broadcasted_iota(jnp.int32, (128, 128), 0)
    target = lax.broadcasted_iota(jnp.int32, (128, 128), 1)
    if inverse:
        source, target = target, source
    hit = source == 4 * (target & 31) + (target >> 5)
    return jnp.where(hit, 1.0, 0.0).astype(BF16)


def pack(cells_ref, out_ref, sorted_ref):
    sorted_ref[...] = jnp.dot(
        cells_ref[...].reshape(1024, 128), permutation(False), preferred_element_type=F32
    )
    for part in range(4):
        tiles = [sorted_ref[pl.ds(256 * part + i, 8, stride=32)] for i in range(32)]
        tiles = exchange(tiles, (0, 1, 2, 3, 4))
        for i in range(MEMBERS):
            out_ref[member_at(i), 8 * part : 8 * part + 8] = tiles[i].astype(BF16)


def arrange(parts_ref, own_ref, first_ref, second_ref):
    for g in range(4):
        tiles = exchange([parts_ref[8 * g + j].astype(F32) for j in range(8)], (4, 5, 6))
        for i in range(8):
            plane = 2 * g + i % 2
            own_ref[i // 2, 32 * plane : 32 * plane + 32] = tiles[i].astype(BF16)
    odd = (own_place() & 1) == 1

    @pl.when(odd)
    def _():
        first_ref[...] = own_ref[0:3]
        second_ref[...] = own_ref[1:4]

    @pl.when(jnp.logical_not(odd))
    def _():
        first_ref[...] = own_ref[1:4]
        second_ref[...] = own_ref[0:3]


def unpack(parts_ref, out_ref, mixed_ref):
    for part in range(2):
        at = slice(16 * part, 16 * part + 16)
        tiles = [parts_ref[member_at(i), at].astype(F32) for i in range(MEMBERS)]
        tiles = exchange(tiles, (0, 1, 2, 3, 4))
        for i in range(32):
            mixed_ref[pl.ds(512 * part + i, 16, stride=32)] = tiles[i]
    moved = jnp.dot(mixed_ref[...].astype(BF16), permutation(True), preferred_element_type=F32)
    out_ref[...] = moved.astype(BF16).reshape(32, 2, 16, 128)


def gelu_pair(pre):
    inner = 0.7978845608 * (pre + 0.044715 * pre * pre * pre)
    hyper = jnp.tanh(inner)
    hidden = 0.5 * pre * (1.0 + hyper)
    slope = 0.5 * (1.0 + hyper) + 0.5 * pre * (1.0 - hyper * hyper) * 0.7978845608 * (
        1.0 + 0.134145 * pre * pre
    )
    return hidden, slope


def before(value):
    return jnp.where(lanes_of(value.shape) > 0, pltpu.roll(value, 1, 1), 0.0)


def after(value):
    return jnp.where(lanes_of(value.shape) < 127, pltpu.roll(value, 127, 1), 0.0)


def fold(product):
    return before(product[0:32]) + product[32:64] + after(product[64:96])


def near(refs, z, x):
    def block(ref, at):
        rows = ref[at, max(32 * x - 32, 0) : min(32 * x + 64, 256)]
        blank = jnp.zeros((32, 128), BF16)
        if x == 0:
            return [blank, rows]
        if x == PLANES - 1:
            return [rows, blank]
        return [rows]

    columns = []
    for at in range(2):
        rows = sum((block(ref, z + at + offset) for ref in refs for offset in range(3)), [])
        columns.append(jnp.concatenate(rows, axis=0))
    return jnp.concatenate(columns, axis=1)


def tile_of(x):
    return slice(32 * x, 32 * x + 32)


def correlate(ref, z, targets):
    rows = jnp.concatenate([near((ref,), z, x) for x in range(PLANES)], axis=1)
    return lax.dot_general(
        rows,
        jnp.concatenate(targets, axis=1),
        (((1,), (1,)), ((), ())),
        preferred_element_type=F32,
    )


def layers(
    width,
    own_ref,
    first_ref,
    second_ref,
    weight_ref,
    joint_ref,
    out_ref,
    p_vol,
    p_hid,
    p_tan,
    p_jv,
    slopes,
    packed,
):
    place = own_place()
    column = OWN * (lax.axis_index("gz") * MEMBERS + place)
    odd = (place & 1) == 1

    @pl.when(odd)
    def _():
        p_vol[0:3] = first_ref[...]
        p_vol[7:10] = second_ref[...]

    @pl.when(jnp.logical_not(odd))
    def _():
        p_vol[0:3] = second_ref[...]
        p_vol[7:10] = first_ref[...]

    p_vol[3:7] = own_ref[...]

    def inside(offset):
        return (column + offset >= 0) & (column + offset < width)

    for z in range(0, 8, 2):
        for x in range(PLANES):
            product = jnp.dot(weight_ref[0:192, :], near((p_vol,), z, x), preferred_element_type=F32)
            for at in range(2):
                part = product[:, 128 * at : 128 * at + 128]
                here = inside(z + at - 2)
                hidden, slope = gelu_pair(fold(part[0:96]))
                tangent = slope * fold(part[96:192])
                p_hid[z + at, tile_of(x)] = jnp.where(here, hidden, 0.0).astype(BF16)
                p_tan[z + at, tile_of(x)] = jnp.where(here, tangent, 0.0).astype(BF16)
                if 2 <= z + at < 6:
                    slopes[z + at - 2, x] = slope

    for z in range(0, 6, 2):
        for x in range(PLANES):
            product = jnp.dot(joint_ref[...], near((p_tan, p_hid), z, x), preferred_element_type=F32)
            for at in range(2):
                jv = fold(product[:, 128 * at : 128 * at + 128])
                jv = jnp.where(inside(z + at - 1), jv, 0.0)
                p_jv[z + at, tile_of(x)] = jv.astype(BF16)

    def spread(tiles):
        both = [
            jnp.concatenate([after(tile), tile, before(tile), jnp.zeros_like(tile)], axis=0)
            for tile in tiles
        ]
        return jnp.concatenate(both, axis=1).astype(BF16)

    sums_first = sums_second = 0.0
    for z in range(0, OWN, 2):
        targets = [
            spread([p_jv[z + at + 1, tile_of(x)].astype(F32) for at in range(2)])
            for x in range(PLANES)
        ]
        sums_second = sums_second + correlate(p_hid, z + 1, targets)
        targets = []
        for x in range(PLANES):
            product = jnp.dot(weight_ref[192:288, :], near((p_jv,), z, x), preferred_element_type=F32)
            tiles = []
            for at in range(2):
                back = slopes[z + at, x] * fold(product[:, 128 * at : 128 * at + 128])
                tiles.append(back.astype(BF16).astype(F32))
            targets.append(spread(tiles))
        sums_first = sums_first + correlate(p_vol, z + 2, targets)

    for g in range(4):
        tiles = [p_jv[1 + i // 2, tile_of(2 * g + i % 2)].astype(F32) for i in range(8)]
        tiles = exchange(tiles, (4, 5, 6))
        for j in range(8):
            out_ref[8 * g + j, 0:32] = tiles[j].astype(BF16)

    rest = pltpu.roll(sums_first, 96, 1)
    packed[0:288] = jnp.where(lanes_of((288, 128)) < 96, sums_second, rest)
    packed[288:432] = jnp.where(
        lanes_of((144, 128)) < 64, rest[0:144], pltpu.roll(rest[144:288], 64, 1)
    )
    packed[432:512] = jnp.zeros((80, 128), F32)
    for member in range(MEMBERS):
        out_ref[member, 32:48] = packed[16 * member : 16 * member + 16].astype(BF16)


def gather_sums(parts_ref, out_ref):
    total = jnp.sum(parts_ref[:, 32:48].astype(F32), axis=0)
    for member in range(8):
        out_ref[member] = total


def combine(parts_ref, out_ref):
    total = jnp.sum(parts_ref[...], axis=0).astype(BF16)
    for member in range(MEMBERS):
        out_ref[member] = total


def finish(scale, packed_ref, d_first_ref, d_second_ref, first_ref, second_ref, rest_ref):
    depth = pl.program_id(0)

    @pl.when(depth == 0)
    def _():
        rest = packed_ref[288:432, :].astype(F32)
        rest_ref[0:144] = rest
        rest_ref[144:288] = pltpu.roll(rest, 64, 1)

    def damped(summed, damping):
        return scale * summed + damping

    for column in range(3):
        block = pl.ds(pl.multiple_of(96 * column + 32 * depth, 32), 32)
        low = packed_ref[block, :].astype(F32)
        far = rest_ref[block, :]
        for row in range(3):
            at = 3 * row + column
            second_ref[at] = damped(low[:, 32 * row : 32 * row + 32], d_second_ref[at])
        first_ref[column] = damped(low[:, 96:128], d_first_ref[column])
        first_ref[3 + column] = damped(far[:, 0:32], d_first_ref[3 + column])
        first_ref[6 + column] = damped(far[:, 32:64], d_first_ref[6 + column])


def filters(w_first_ref, v_first_ref, w_second_ref, v_second_ref, rows_ref, joint_ref):
    def tall(ref):
        return jnp.concatenate(
            [
                jnp.concatenate(
                    [ref[9 * (k % 3) + 3 * row + k // 3].astype(F32) for k in range(9)], axis=0
                )
                for row in range(3)
            ],
            axis=1,
        )

    def turned(refs):
        return jnp.concatenate([tall(ref) for ref in refs], axis=0).T.astype(BF16)

    rows_ref[0:96] = turned([w_first_ref])
    rows_ref[96:192] = turned([v_first_ref])
    joint_ref[...] = turned([w_second_ref, v_second_ref])
    for row in range(3):
        blocks = [
            w_second_ref[26 - (9 * (k % 3) + 3 * row + k // 3)].astype(F32) for k in range(9)
        ]
        rows_ref[192 + 32 * row : 224 + 32 * row] = jnp.concatenate(blocks, axis=1).astype(BF16)


def call(kernel, operands, outputs, scratch, name, limit, flops):
    vmem = pl.BlockSpec(memory_space=pltpu.VMEM)
    return pl.pallas_call(
        kernel,
        out_shape=tuple(jax.ShapeDtypeStruct(shape, dtype) for shape, dtype in outputs),
        in_specs=[vmem] * len(operands),
        out_specs=(vmem,) * len(outputs),
        scratch_shapes=[pltpu.VMEM(shape, dtype) for shape, dtype in scratch],
        compiler_params=pltpu.CompilerParams(vmem_limit_bytes=limit << 20),
        cost_estimate=pl.CostEstimate(flops=flops, bytes_accessed=1 << 20, transcendentals=0),
        name=name,
    )(*operands)


def body(volume, w_first, w_second, v_first, v_second):
    channels, depth, height, width = volume.shape
    n_gx, n_gy, n_gz = (lax.axis_size(axis) for axis in AXES)
    members = n_gx * n_gy
    count_all = float(depth * n_gx * height * n_gy * width * n_gz)
    factor = math.sqrt(27.0 * channels)
    small = (channels, 128)

    (sent,) = call(
        pack, (volume,), [((members,) + small, BF16)], [((1024, 128), F32)], "pack", 8, 10**8
    )
    parts = lax.all_to_all(sent, GROUP, 0, 0)

    parts, w_first, w_second, v_first, v_second = lax.optimization_barrier(
        (parts, w_first, w_second, v_first, v_second)
    )
    blocks = [w.reshape(27, channels, channels) for w in (w_first, v_first, w_second, v_second)]
    weights = call(
        filters, blocks, [((288, 288), BF16), ((96, 576), BF16)], [], "filters", 8, 2 * 10**8
    )
    damping = tuple(
        factor * 0.1 * v.astype(F32).reshape(27, channels, channels) for v in (v_first, v_second)
    )

    halo = ((OWN - 1, 256, 128), BF16)
    own, first, second = call(
        arrange, (parts,), [((OWN, 256, 128), BF16), halo, halo], [], "arrange", 8, 10**8
    )

    def swapped(start):
        def device(at):
            gz, place = divmod(at, members)
            return LINES[gz % 2][place] * n_gz + gz

        pairs = [(device(i), device(i + 1)) for i in range(start, members * n_gz - 1, 2)]
        return pairs + [(b, a) for a, b in pairs]

    first = lax.ppermute(first, AXES, swapped(0))
    second = lax.ppermute(second, AXES, swapped(1))

    (leaving,) = call(
        lambda *refs: layers(width * n_gz, *refs),
        (own, first, second, *weights),
        [((members, 48, 128), BF16)],
        [
            ((10, 256, 128), BF16),
            ((8, 256, 128), BF16),
            ((8, 256, 128), BF16),
            ((6, 256, 128), BF16),
            ((OWN, PLANES) + small, F32),
            ((512, 128), F32),
        ],
        "layers",
        24,
        8 * 10**9,
    )

    parts = lax.all_to_all(leaving, GROUP, 0, 0)
    (sums,) = call(gather_sums, (parts,), [((n_gz, 16, 128), F32)], [], "gather_sums", 8, 10**8)
    sums = lax.all_to_all(sums, "gz", 0, 0)
    (every,) = call(combine, (sums,), [((members, 16, 128), BF16)], [], "combine", 8, 10**8)
    every = lax.all_to_all(every, GROUP, 0, 0).reshape(512, 128)
    (out,) = call(
        unpack,
        (parts,),
        [(volume.shape, BF16)],
        [((1024, 128), F32)],
        "unpack",
        8,
        10**9,
    )
    third = pl.BlockSpec((9, channels, channels), lambda i: (i, 0, 0))
    gv_first, gv_second = pl.pallas_call(
        lambda *refs: finish(factor / count_all, *refs),
        grid=(3,),
        out_shape=(jax.ShapeDtypeStruct((27, channels, channels), F32),) * 2,
        in_specs=[pl.BlockSpec((512, 128), lambda i: (0, 0)), third, third],
        out_specs=(third, third),
        scratch_shapes=[pltpu.VMEM((288, 128), F32)],
        compiler_params=pltpu.CompilerParams(
            dimension_semantics=("arbitrary",), vmem_limit_bytes=8 << 20
        ),
        name="finish",
    )(every, *damping)
    return (out, gv_first.reshape(v_first.shape), gv_second.reshape(v_first.shape))


def solution(mesh):
    in_specs = (P(None, "gx", "gy", "gz"), P(), P(), P(), P())
    out_specs = (P(None, "gx", "gy", "gz"), P(), P())
    return jax.shard_map(body, mesh=mesh, in_specs=in_specs, out_specs=out_specs, check_vma=False)
```

```python
import math

import jax
import jax.numpy as jnp
from jax import lax
from jax.experimental import pallas as pl
from jax.experimental.pallas import tpu as pltpu
from jax.sharding import PartitionSpec as P

F32 = jnp.float32
BF16 = jnp.bfloat16
AXES = ("gx", "gy", "gz")
GROUP = ("gx", "gy")
PLANES = 8
OWN = 4
MEMBERS = 32


def snake():
    def member(z, x):
        return z % 4 * 8 + z // 4 * 4 + x

    line = []
    for z in range(8):
        line += [member(z, x) for x in ((1, 2, 3) if z % 2 == 0 else (3, 2, 1))]
    return tuple(line + [member(z, 0) for z in reversed(range(8))])


LINES = (snake(), snake()[:1] + snake()[:0:-1])


def member_at(place):
    return jnp.where((lax.axis_index("gz") & 1) == 0, LINES[0][place], LINES[1][place])


def own_place():
    member = lax.axis_index("gx") * 8 + lax.axis_index("gy")
    place = jnp.int32(0)
    for at in range(MEMBERS):
        place = jnp.where(member == member_at(at), at, place)
    return place


def lanes_of(shape):
    return lax.broadcasted_iota(jnp.int32, shape, len(shape) - 1)


def exchange(tiles, bits):
    tiles = list(tiles)
    lane = lanes_of(tiles[0].shape)
    for place, bit in enumerate(bits):
        step = 1 << bit
        clear = (lane & step) == 0
        for low in range(len(tiles)):
            if low & (1 << place):
                continue
            high = low | (1 << place)
            a, b = tiles[low], tiles[high]
            tiles[low] = jnp.where(clear, a, pltpu.roll(b, step, 1))
            tiles[high] = jnp.where(clear, pltpu.roll(a, 128 - step, 1), b)
    return tiles


def permutation(inverse):
    source = lax.broadcasted_iota(jnp.int32, (128, 128), 0)
    target = lax.broadcasted_iota(jnp.int32, (128, 128), 1)
    if inverse:
        source, target = target, source
    hit = source == 4 * (target & 31) + (target >> 5)
    return jnp.where(hit, 1.0, 0.0).astype(BF16)


def pack(cells_ref, out_ref, cells, sorted_ref, arrived):
    def fetch(part):
        at = pl.ds(8 * part, 8)
        return pltpu.make_async_copy(cells_ref.at[at], cells.at[at], arrived.at[part])

    for part in range(4):
        fetch(part).start()
    order = permutation(False)
    for part in range(4):
        fetch(part).wait()
        sorted_ref[...] = jnp.dot(
            cells[8 * part : 8 * part + 8].reshape(256, 128), order, preferred_element_type=F32
        )
        tiles = exchange([sorted_ref[pl.ds(i, 8, stride=32)] for i in range(32)], (0, 1, 2, 3, 4))
        for i in range(MEMBERS):
            out_ref[member_at(i), 8 * part : 8 * part + 8] = tiles[i].astype(BF16)


def arrange(parts_ref, own_ref, first_ref, second_ref):
    for g in range(4):
        tiles = exchange([parts_ref[8 * g + j].astype(F32) for j in range(8)], (4, 5, 6))
        for i in range(8):
            plane = 2 * g + i % 2
            own_ref[i // 2, 32 * plane : 32 * plane + 32] = tiles[i].astype(BF16)
    odd = (own_place() & 1) == 1

    @pl.when(odd)
    def _():
        first_ref[...] = own_ref[0:3]
        second_ref[...] = own_ref[1:4]

    @pl.when(jnp.logical_not(odd))
    def _():
        first_ref[...] = own_ref[1:4]
        second_ref[...] = own_ref[0:3]


def gelu_pair(pre):
    inner = 0.7978845608 * (pre + 0.044715 * pre * pre * pre)
    hyper = jnp.tanh(inner)
    hidden = 0.5 * pre * (1.0 + hyper)
    slope = 0.5 * (1.0 + hyper) + 0.5 * pre * (1.0 - hyper * hyper) * 0.7978845608 * (
        1.0 + 0.134145 * pre * pre
    )
    return hidden, slope


def before(value):
    return jnp.where(lanes_of(value.shape) > 0, pltpu.roll(value, 1, 1), 0.0)


def after(value):
    return jnp.where(lanes_of(value.shape) < 127, pltpu.roll(value, 127, 1), 0.0)


def fold(product):
    return before(product[0:32]) + product[32:64] + after(product[64:96])


def near(refs, z, x):
    def block(ref, at):
        rows = ref[at, max(32 * x - 32, 0) : min(32 * x + 64, 256)]
        blank = jnp.zeros((32, 128), BF16)
        if x == 0:
            return [blank, rows]
        if x == PLANES - 1:
            return [rows, blank]
        return [rows]

    columns = []
    for at in range(2):
        rows = sum((block(ref, z + at + offset) for ref in refs for offset in range(3)), [])
        columns.append(jnp.concatenate(rows, axis=0))
    return jnp.concatenate(columns, axis=1)


def tile_of(x):
    return slice(32 * x, 32 * x + 32)


def correlate(ref, z, targets):
    rows = jnp.concatenate([near((ref,), z, x) for x in range(PLANES)], axis=1)
    return lax.dot_general(
        rows,
        jnp.concatenate(targets, axis=1),
        (((1,), (1,)), ((), ())),
        preferred_element_type=F32,
    )


def layers(
    width,
    own_ref,
    first_ref,
    second_ref,
    weight_ref,
    joint_ref,
    out_ref,
    p_vol,
    p_hid,
    p_tan,
    p_jv,
    slopes,
    packed,
):
    place = own_place()
    column = OWN * (lax.axis_index("gz") * MEMBERS + place)
    odd = (place & 1) == 1

    @pl.when(odd)
    def _():
        p_vol[0:3] = first_ref[...]
        p_vol[7:10] = second_ref[...]

    @pl.when(jnp.logical_not(odd))
    def _():
        p_vol[0:3] = second_ref[...]
        p_vol[7:10] = first_ref[...]

    p_vol[3:7] = own_ref[...]

    def inside(offset):
        return (column + offset >= 0) & (column + offset < width)

    for z in range(0, 8, 2):
        for x in range(PLANES):
            product = jnp.dot(weight_ref[0:192, :], near((p_vol,), z, x), preferred_element_type=F32)
            for at in range(2):
                part = product[:, 128 * at : 128 * at + 128]
                here = inside(z + at - 2)
                hidden, slope = gelu_pair(fold(part[0:96]))
                tangent = slope * fold(part[96:192])
                p_hid[z + at, tile_of(x)] = jnp.where(here, hidden, 0.0).astype(BF16)
                p_tan[z + at, tile_of(x)] = jnp.where(here, tangent, 0.0).astype(BF16)
                if 2 <= z + at < 6:
                    slopes[z + at - 2, x] = slope

    for z in range(0, 6, 2):
        for x in range(PLANES):
            product = jnp.dot(joint_ref[...], near((p_tan, p_hid), z, x), preferred_element_type=F32)
            for at in range(2):
                jv = fold(product[:, 128 * at : 128 * at + 128])
                jv = jnp.where(inside(z + at - 1), jv, 0.0)
                p_jv[z + at, tile_of(x)] = jv.astype(BF16)

    def spread(tiles):
        both = [
            jnp.concatenate([after(tile), tile, before(tile), jnp.zeros_like(tile)], axis=0)
            for tile in tiles
        ]
        return jnp.concatenate(both, axis=1).astype(BF16)

    sums_first = sums_second = 0.0
    for z in range(0, OWN, 2):
        targets = [
            spread([p_jv[z + at + 1, tile_of(x)].astype(F32) for at in range(2)])
            for x in range(PLANES)
        ]
        sums_second = sums_second + correlate(p_hid, z + 1, targets)
        targets = []
        for x in range(PLANES):
            product = jnp.dot(weight_ref[192:288, :], near((p_jv,), z, x), preferred_element_type=F32)
            tiles = []
            for at in range(2):
                back = slopes[z + at, x] * fold(product[:, 128 * at : 128 * at + 128])
                tiles.append(back.astype(BF16).astype(F32))
            targets.append(spread(tiles))
        sums_first = sums_first + correlate(p_vol, z + 2, targets)

    for g in range(4):
        tiles = [p_jv[1 + i // 2, tile_of(2 * g + i % 2)].astype(F32) for i in range(8)]
        tiles = exchange(tiles, (4, 5, 6))
        for j in range(8):
            out_ref[8 * g + j, 0:32] = tiles[j].astype(BF16)

    rest = pltpu.roll(sums_first, 96, 1)
    packed[0:288] = jnp.where(lanes_of((288, 128)) < 96, sums_second, rest)
    packed[288:432] = jnp.where(
        lanes_of((144, 128)) < 64, rest[0:144], pltpu.roll(rest[144:288], 64, 1)
    )
    packed[432:512] = jnp.zeros((80, 128), F32)
    for member in range(MEMBERS):
        out_ref[member, 32:48] = packed[16 * member : 16 * member + 16].astype(BF16)


def gather_sums(parts_ref, out_ref):
    total = jnp.sum(parts_ref[:, 32:48].astype(F32), axis=0)
    for member in range(8):
        out_ref[member] = total


def combine(parts_ref, out_ref):
    total = jnp.sum(parts_ref[...], axis=0).astype(BF16)
    for member in range(MEMBERS):
        out_ref[member] = total


def finish(
    scale,
    packed_ref,
    d_first_ref,
    d_second_ref,
    parts_ref,
    first_ref,
    second_ref,
    jv_ref,
    first,
    second,
    jv,
    mixed_ref,
    left,
):
    leaving = []

    def leave(source, target, at):
        leaving.append(pltpu.make_async_copy(source.at[at], target.at[at], left.at[len(leaving)]))
        leaving[-1].start()

    rest = packed_ref[288:432, :].astype(F32)
    rest = jnp.concatenate([rest, pltpu.roll(rest, 64, 1)], axis=0)
    for depth in range(3):
        for column in range(3):
            block = slice(96 * column + 32 * depth, 96 * column + 32 * depth + 32)
            low = packed_ref[block, :].astype(F32)
            far = rest[block]
            for row in range(3):
                at = 9 * depth + 3 * row + column
                second[at] = scale * low[:, 32 * row : 32 * row + 32] + d_second_ref[at]
            for row, summed in enumerate((low[:, 96:128], far[:, 0:32], far[:, 32:64])):
                at = 9 * depth + 3 * row + column
                first[at] = scale * summed + d_first_ref[at]
        leave(first, first_ref, pl.ds(9 * depth, 9))
        leave(second, second_ref, pl.ds(9 * depth, 9))

    order = permutation(True)
    for part in range(2):
        at = slice(16 * part, 16 * part + 16)
        tiles = [parts_ref[member_at(i), at].astype(F32) for i in range(MEMBERS)]
        tiles = exchange(tiles, (0, 1, 2, 3, 4))
        for i in range(32):
            mixed_ref[pl.ds(i, 16, stride=32)] = tiles[i]
        moved = jnp.dot(mixed_ref[...].astype(BF16), order, preferred_element_type=F32)
        jv[at] = moved.astype(BF16).reshape(16, 2, 16, 128)
        leave(jv, jv_ref, pl.ds(16 * part, 16))
    for copy in leaving:
        copy.wait()


def filters(w_first_ref, v_first_ref, w_second_ref, v_second_ref, rows_ref, joint_ref):
    def tall(ref):
        return jnp.concatenate(
            [
                jnp.concatenate(
                    [ref[9 * (k % 3) + 3 * row + k // 3].astype(F32) for k in range(9)], axis=0
                )
                for row in range(3)
            ],
            axis=1,
        )

    def turned(refs):
        return jnp.concatenate([tall(ref) for ref in refs], axis=0).T.astype(BF16)

    rows_ref[0:96] = turned([w_first_ref])
    rows_ref[96:192] = turned([v_first_ref])
    joint_ref[...] = turned([w_second_ref, v_second_ref])
    for row in range(3):
        blocks = [
            w_second_ref[26 - (9 * (k % 3) + 3 * row + k // 3)].astype(F32) for k in range(9)
        ]
        rows_ref[192 + 32 * row : 224 + 32 * row] = jnp.concatenate(blocks, axis=1).astype(BF16)


def call(kernel, operands, outputs, scratch, name, limit, flops):
    vmem = pl.BlockSpec(memory_space=pltpu.VMEM)
    return pl.pallas_call(
        kernel,
        out_shape=tuple(jax.ShapeDtypeStruct(shape, dtype) for shape, dtype in outputs),
        in_specs=[vmem] * len(operands),
        out_specs=(vmem,) * len(outputs),
        scratch_shapes=[pltpu.VMEM(shape, dtype) for shape, dtype in scratch],
        compiler_params=pltpu.CompilerParams(vmem_limit_bytes=limit << 20),
        cost_estimate=pl.CostEstimate(flops=flops, bytes_accessed=1 << 20, transcendentals=0),
        name=name,
    )(*operands)


def body(volume, w_first, w_second, v_first, v_second):
    channels, depth, height, width = volume.shape
    n_gx, n_gy, n_gz = (lax.axis_size(axis) for axis in AXES)
    members = n_gx * n_gy
    count_all = float(depth * n_gx * height * n_gy * width * n_gz)
    factor = math.sqrt(27.0 * channels)
    small = (channels, 128)

    sent = pl.pallas_call(
        pack,
        out_shape=jax.ShapeDtypeStruct((members,) + small, BF16),
        in_specs=[pl.BlockSpec(memory_space=pltpu.HBM)],
        out_specs=pl.BlockSpec(memory_space=pltpu.VMEM),
        scratch_shapes=[
            pltpu.VMEM(volume.shape, BF16),
            pltpu.VMEM((256, 128), F32),
            pltpu.SemaphoreType.DMA((4,)),
        ],
        compiler_params=pltpu.CompilerParams(vmem_limit_bytes=8 << 20),
        cost_estimate=pl.CostEstimate(flops=10**8, bytes_accessed=1, transcendentals=0),
        name="pack",
    )(pltpu.with_memory_space_constraint(volume, pltpu.HBM))
    parts = lax.all_to_all(sent, GROUP, 0, 0)

    parts, w_first, w_second, v_first, v_second = lax.optimization_barrier(
        (parts, w_first, w_second, v_first, v_second)
    )
    blocks = [w.reshape(27, channels, channels) for w in (w_first, v_first, w_second, v_second)]
    weights = call(
        filters, blocks, [((288, 288), BF16), ((96, 576), BF16)], [], "filters", 8, 2 * 10**8
    )
    damping = tuple(
        factor * 0.1 * v.astype(F32).reshape(27, channels, channels) for v in (v_first, v_second)
    )

    halo = ((OWN - 1, 256, 128), BF16)
    own, first, second = call(
        arrange, (parts,), [((OWN, 256, 128), BF16), halo, halo], [], "arrange", 8, 10**8
    )

    def swapped(start):
        def device(at):
            gz, place = divmod(at, members)
            return LINES[gz % 2][place] * n_gz + gz

        pairs = [(device(i), device(i + 1)) for i in range(start, members * n_gz - 1, 2)]
        return pairs + [(b, a) for a, b in pairs]

    first = lax.ppermute(first, AXES, swapped(0))
    second = lax.ppermute(second, AXES, swapped(1))
    first, second, damping = lax.optimization_barrier((first, second, damping))

    (leaving,) = call(
        lambda *refs: layers(width * n_gz, *refs),
        (own, first, second, *weights),
        [((members, 48, 128), BF16)],
        [
            ((10, 256, 128), BF16),
            ((8, 256, 128), BF16),
            ((8, 256, 128), BF16),
            ((6, 256, 128), BF16),
            ((OWN, PLANES) + small, F32),
            ((512, 128), F32),
        ],
        "layers",
        24,
        8 * 10**9,
    )

    parts = lax.all_to_all(leaving, GROUP, 0, 0)
    (sums,) = call(gather_sums, (parts,), [((n_gz, 16, 128), F32)], [], "gather_sums", 8, 10**8)
    sums = lax.all_to_all(sums, "gz", 0, 0)
    (every,) = call(combine, (sums,), [((members, 16, 128), BF16)], [], "combine", 8, 10**8)
    every = lax.all_to_all(every, GROUP, 0, 0).reshape(512, 128)
    hbm = pl.BlockSpec(memory_space=pltpu.HBM)
    filter_shape = (27, channels, channels)
    gv_first, gv_second, out = pl.pallas_call(
        lambda *refs: finish(factor / count_all, *refs),
        out_shape=(
            jax.ShapeDtypeStruct(filter_shape, F32),
            jax.ShapeDtypeStruct(filter_shape, F32),
            jax.ShapeDtypeStruct(volume.shape, BF16),
        ),
        in_specs=[pl.BlockSpec(memory_space=pltpu.VMEM)] * 4,
        out_specs=(hbm,) * 3,
        scratch_shapes=[
            pltpu.VMEM(filter_shape, F32),
            pltpu.VMEM(filter_shape, F32),
            pltpu.VMEM(volume.shape, BF16),
            pltpu.VMEM((512, 128), F32),
            pltpu.SemaphoreType.DMA((8,)),
        ],
        compiler_params=pltpu.CompilerParams(vmem_limit_bytes=8 << 20),
        cost_estimate=pl.CostEstimate(flops=10**9, bytes_accessed=1 << 20, transcendentals=0),
        name="finish",
    )(every, *damping, parts)
    return (out, gv_first.reshape(v_first.shape), gv_second.reshape(v_first.shape))


def solution(mesh):
    in_specs = (P(None, "gx", "gy", "gz"), P(), P(), P(), P())
    out_specs = (P(None, "gx", "gy", "gz"), P(), P())
    return jax.shard_map(body, mesh=mesh, in_specs=in_specs, out_specs=out_specs, check_vma=False)
```

```python
import math

import jax
import jax.numpy as jnp
from jax import lax
from jax.experimental import pallas as pl
from jax.experimental.pallas import tpu as pltpu
from jax.sharding import PartitionSpec as P

F32 = jnp.float32
BF16 = jnp.bfloat16
AXES = ("gx", "gy", "gz")
GROUP = ("gx", "gy")
PLANES = 8
OWN = 4
MEMBERS = 32


def snake():
    def member(z, x):
        return z % 4 * 8 + z // 4 * 4 + x

    line = []
    for z in range(8):
        line += [member(z, x) for x in ((1, 2, 3) if z % 2 == 0 else (3, 2, 1))]
    return tuple(line + [member(z, 0) for z in reversed(range(8))])


LINES = (snake(), snake()[:1] + snake()[:0:-1])


def member_at(place):
    return jnp.where((lax.axis_index("gz") & 1) == 0, LINES[0][place], LINES[1][place])


def own_place():
    member = lax.axis_index("gx") * 8 + lax.axis_index("gy")
    place = jnp.int32(0)
    for at in range(MEMBERS):
        place = jnp.where(member == member_at(at), at, place)
    return place


def lanes_of(shape):
    return lax.broadcasted_iota(jnp.int32, shape, len(shape) - 1)


def exchange(tiles, bits):
    tiles = list(tiles)
    lane = lanes_of(tiles[0].shape)
    for place, bit in enumerate(bits):
        step = 1 << bit
        clear = (lane & step) == 0
        for low in range(len(tiles)):
            if low & (1 << place):
                continue
            high = low | (1 << place)
            a, b = tiles[low], tiles[high]
            tiles[low] = jnp.where(clear, a, pltpu.roll(b, step, 1))
            tiles[high] = jnp.where(clear, pltpu.roll(a, 128 - step, 1), b)
    return tiles


def permutation(inverse):
    source = lax.broadcasted_iota(jnp.int32, (128, 128), 0)
    target = lax.broadcasted_iota(jnp.int32, (128, 128), 1)
    if inverse:
        source, target = target, source
    hit = source == 4 * (target & 31) + (target >> 5)
    return jnp.where(hit, 1.0, 0.0).astype(BF16)


def pack(cells_ref, out_ref, sorted_ref):
    sorted_ref[...] = jnp.dot(
        cells_ref[...].reshape(1024, 128), permutation(False), preferred_element_type=F32
    )
    for part in range(4):
        tiles = [sorted_ref[pl.ds(256 * part + i, 8, stride=32)] for i in range(32)]
        tiles = exchange(tiles, (0, 1, 2, 3, 4))
        for i in range(MEMBERS):
            out_ref[member_at(i), 8 * part : 8 * part + 8] = tiles[i].astype(BF16)


def arrange(parts_ref, own_ref, first_ref, second_ref):
    for g in range(4):
        tiles = exchange([parts_ref[8 * g + j].astype(F32) for j in range(8)], (4, 5, 6))
        for i in range(8):
            plane = 2 * g + i % 2
            own_ref[i // 2, 32 * plane : 32 * plane + 32] = tiles[i].astype(BF16)
    odd = (own_place() & 1) == 1

    @pl.when(odd)
    def _():
        first_ref[...] = own_ref[0:3]
        second_ref[...] = own_ref[1:4]

    @pl.when(jnp.logical_not(odd))
    def _():
        first_ref[...] = own_ref[1:4]
        second_ref[...] = own_ref[0:3]


def gelu_pair(pre):
    inner = 0.7978845608 * (pre + 0.044715 * pre * pre * pre)
    hyper = jnp.tanh(inner)
    hidden = 0.5 * pre * (1.0 + hyper)
    slope = 0.5 * (1.0 + hyper) + 0.5 * pre * (1.0 - hyper * hyper) * 0.7978845608 * (
        1.0 + 0.134145 * pre * pre
    )
    return hidden, slope


def before(value):
    return jnp.where(lanes_of(value.shape) > 0, pltpu.roll(value, 1, 1), 0.0)


def after(value):
    return jnp.where(lanes_of(value.shape) < 127, pltpu.roll(value, 127, 1), 0.0)


def fold(product):
    return before(product[0:32]) + product[32:64] + after(product[64:96])


def near(refs, z, x):
    def block(ref, at):
        rows = ref[at, max(32 * x - 32, 0) : min(32 * x + 64, 256)]
        blank = jnp.zeros((32, 128), BF16)
        if x == 0:
            return [blank, rows]
        if x == PLANES - 1:
            return [rows, blank]
        return [rows]

    columns = []
    for at in range(2):
        rows = sum((block(ref, z + at + offset) for ref in refs for offset in range(3)), [])
        columns.append(jnp.concatenate(rows, axis=0))
    return jnp.concatenate(columns, axis=1)


def tile_of(x):
    return slice(32 * x, 32 * x + 32)


def correlate(ref, z, targets):
    rows = jnp.concatenate([near((ref,), z, x) for x in range(PLANES)], axis=1)
    return lax.dot_general(
        rows,
        jnp.concatenate(targets, axis=1),
        (((1,), (1,)), ((), ())),
        preferred_element_type=F32,
    )


def layers(
    width,
    own_ref,
    first_ref,
    second_ref,
    weight_ref,
    joint_ref,
    out_ref,
    p_vol,
    p_hid,
    p_tan,
    p_jv,
    slopes,
    packed,
):
    place = own_place()
    column = OWN * (lax.axis_index("gz") * MEMBERS + place)
    odd = (place & 1) == 1

    @pl.when(odd)
    def _():
        p_vol[0:3] = first_ref[...]
        p_vol[7:10] = second_ref[...]

    @pl.when(jnp.logical_not(odd))
    def _():
        p_vol[0:3] = second_ref[...]
        p_vol[7:10] = first_ref[...]

    p_vol[3:7] = own_ref[...]

    def inside(offset):
        return (column + offset >= 0) & (column + offset < width)

    for z in range(0, 8, 2):
        for x in range(PLANES):
            product = jnp.dot(weight_ref[0:192, :], near((p_vol,), z, x), preferred_element_type=F32)
            for at in range(2):
                part = product[:, 128 * at : 128 * at + 128]
                here = inside(z + at - 2)
                hidden, slope = gelu_pair(fold(part[0:96]))
                tangent = slope * fold(part[96:192])
                p_hid[z + at, tile_of(x)] = jnp.where(here, hidden, 0.0).astype(BF16)
                p_tan[z + at, tile_of(x)] = jnp.where(here, tangent, 0.0).astype(BF16)
                if 2 <= z + at < 6:
                    slopes[z + at - 2, x] = slope

    for z in range(0, 6, 2):
        for x in range(PLANES):
            product = jnp.dot(joint_ref[...], near((p_tan, p_hid), z, x), preferred_element_type=F32)
            for at in range(2):
                jv = fold(product[:, 128 * at : 128 * at + 128])
                jv = jnp.where(inside(z + at - 1), jv, 0.0)
                p_jv[z + at, tile_of(x)] = jv.astype(BF16)

    def spread(tiles):
        both = [
            jnp.concatenate([after(tile), tile, before(tile), jnp.zeros_like(tile)], axis=0)
            for tile in tiles
        ]
        return jnp.concatenate(both, axis=1).astype(BF16)

    sums_first = sums_second = 0.0
    for z in range(0, OWN, 2):
        targets = [
            spread([p_jv[z + at + 1, tile_of(x)].astype(F32) for at in range(2)])
            for x in range(PLANES)
        ]
        sums_second = sums_second + correlate(p_hid, z + 1, targets)
        targets = []
        for x in range(PLANES):
            product = jnp.dot(weight_ref[192:288, :], near((p_jv,), z, x), preferred_element_type=F32)
            tiles = []
            for at in range(2):
                back = slopes[z + at, x] * fold(product[:, 128 * at : 128 * at + 128])
                tiles.append(back.astype(BF16).astype(F32))
            targets.append(spread(tiles))
        sums_first = sums_first + correlate(p_vol, z + 2, targets)

    for g in range(4):
        tiles = [p_jv[1 + i // 2, tile_of(2 * g + i % 2)].astype(F32) for i in range(8)]
        tiles = exchange(tiles, (4, 5, 6))
        for j in range(8):
            out_ref[8 * g + j, 0:32] = tiles[j].astype(BF16)

    rest = pltpu.roll(sums_first, 96, 1)
    packed[0:288] = jnp.where(lanes_of((288, 128)) < 96, sums_second, rest)
    packed[288:432] = jnp.where(
        lanes_of((144, 128)) < 64, rest[0:144], pltpu.roll(rest[144:288], 64, 1)
    )
    packed[432:512] = jnp.zeros((80, 128), F32)
    for member in range(MEMBERS):
        out_ref[member, 32:48] = packed[16 * member : 16 * member + 16].astype(BF16)


def gather_sums(parts_ref, out_ref):
    total = jnp.sum(parts_ref[:, 32:48].astype(F32), axis=0)
    for member in range(8):
        out_ref[member] = total


def combine(parts_ref, out_ref):
    total = jnp.sum(parts_ref[...], axis=0).astype(BF16)
    for member in range(MEMBERS):
        out_ref[member] = total


def finish(
    scale,
    packed_ref,
    d_first_ref,
    d_second_ref,
    parts_ref,
    first_ref,
    second_ref,
    jv_ref,
    first,
    second,
    mixed_ref,
    left,
):
    leaving = []

    def leave(source, target, at):
        leaving.append(pltpu.make_async_copy(source.at[at], target.at[at], left.at[len(leaving)]))
        leaving[-1].start()

    rest = packed_ref[288:432, :].astype(F32)
    rest = jnp.concatenate([rest, pltpu.roll(rest, 64, 1)], axis=0)
    for depth in range(3):
        for column in range(3):
            block = slice(96 * column + 32 * depth, 96 * column + 32 * depth + 32)
            low = packed_ref[block, :].astype(F32)
            far = rest[block]
            for row in range(3):
                at = 9 * depth + 3 * row + column
                second[at] = scale * low[:, 32 * row : 32 * row + 32] + d_second_ref[at]
            for row, summed in enumerate((low[:, 96:128], far[:, 0:32], far[:, 32:64])):
                at = 9 * depth + 3 * row + column
                first[at] = scale * summed + d_first_ref[at]
        leave(first, first_ref, pl.ds(9 * depth, 9))
        leave(second, second_ref, pl.ds(9 * depth, 9))

    order = permutation(True)
    for part in range(2):
        at = slice(16 * part, 16 * part + 16)
        tiles = [parts_ref[member_at(i), at].astype(F32) for i in range(MEMBERS)]
        tiles = exchange(tiles, (0, 1, 2, 3, 4))
        for i in range(32):
            mixed_ref[pl.ds(i, 16, stride=32)] = tiles[i]
        moved = jnp.dot(mixed_ref[...].astype(BF16), order, preferred_element_type=F32)
        jv_ref[at] = moved.astype(BF16).reshape(16, 2, 16, 128)
    for copy in leaving:
        copy.wait()


def filters(w_first_ref, v_first_ref, w_second_ref, v_second_ref, rows_ref, joint_ref):
    def tall(ref):
        return jnp.concatenate(
            [
                jnp.concatenate(
                    [ref[9 * (k % 3) + 3 * row + k // 3].astype(F32) for k in range(9)], axis=0
                )
                for row in range(3)
            ],
            axis=1,
        )

    def turned(refs):
        return jnp.concatenate([tall(ref) for ref in refs], axis=0).T.astype(BF16)

    rows_ref[0:96] = turned([w_first_ref])
    rows_ref[96:192] = turned([v_first_ref])
    joint_ref[...] = turned([w_second_ref, v_second_ref])
    for row in range(3):
        blocks = [
            w_second_ref[26 - (9 * (k % 3) + 3 * row + k // 3)].astype(F32) for k in range(9)
        ]
        rows_ref[192 + 32 * row : 224 + 32 * row] = jnp.concatenate(blocks, axis=1).astype(BF16)


def call(kernel, operands, outputs, scratch, name, limit, flops):
    vmem = pl.BlockSpec(memory_space=pltpu.VMEM)
    return pl.pallas_call(
        kernel,
        out_shape=tuple(jax.ShapeDtypeStruct(shape, dtype) for shape, dtype in outputs),
        in_specs=[vmem] * len(operands),
        out_specs=(vmem,) * len(outputs),
        scratch_shapes=[pltpu.VMEM(shape, dtype) for shape, dtype in scratch],
        compiler_params=pltpu.CompilerParams(vmem_limit_bytes=limit << 20),
        cost_estimate=pl.CostEstimate(flops=flops, bytes_accessed=1 << 20, transcendentals=0),
        name=name,
    )(*operands)


def body(volume, w_first, w_second, v_first, v_second):
    channels, depth, height, width = volume.shape
    n_gx, n_gy, n_gz = (lax.axis_size(axis) for axis in AXES)
    members = n_gx * n_gy
    count_all = float(depth * n_gx * height * n_gy * width * n_gz)
    factor = math.sqrt(27.0 * channels)
    small = (channels, 128)

    (sent,) = call(
        pack, (volume,), [((members,) + small, BF16)], [((1024, 128), F32)], "pack", 8, 10**8
    )
    parts = lax.all_to_all(sent, GROUP, 0, 0)

    parts, w_first, w_second, v_first, v_second = lax.optimization_barrier(
        (parts, w_first, w_second, v_first, v_second)
    )
    blocks = [w.reshape(27, channels, channels) for w in (w_first, v_first, w_second, v_second)]
    weights = call(
        filters, blocks, [((288, 288), BF16), ((96, 576), BF16)], [], "filters", 8, 2 * 10**8
    )
    damping = tuple(
        factor * 0.1 * v.astype(F32).reshape(27, channels, channels) for v in (v_first, v_second)
    )

    halo = ((OWN - 1, 256, 128), BF16)
    own, first, second = call(
        arrange, (parts,), [((OWN, 256, 128), BF16), halo, halo], [], "arrange", 8, 10**8
    )

    def swapped(start):
        def device(at):
            gz, place = divmod(at, members)
            return LINES[gz % 2][place] * n_gz + gz

        pairs = [(device(i), device(i + 1)) for i in range(start, members * n_gz - 1, 2)]
        return pairs + [(b, a) for a, b in pairs]

    first = lax.ppermute(first, AXES, swapped(0))
    second = lax.ppermute(second, AXES, swapped(1))
    first, second, damping = lax.optimization_barrier((first, second, damping))

    (leaving,) = call(
        lambda *refs: layers(width * n_gz, *refs),
        (own, first, second, *weights),
        [((members, 48, 128), BF16)],
        [
            ((10, 256, 128), BF16),
            ((8, 256, 128), BF16),
            ((8, 256, 128), BF16),
            ((6, 256, 128), BF16),
            ((OWN, PLANES) + small, F32),
            ((512, 128), F32),
        ],
        "layers",
        24,
        8 * 10**9,
    )

    parts = lax.all_to_all(leaving, GROUP, 0, 0)
    (sums,) = call(gather_sums, (parts,), [((n_gz, 16, 128), F32)], [], "gather_sums", 8, 10**8)
    sums = lax.all_to_all(sums, "gz", 0, 0)
    (every,) = call(combine, (sums,), [((members, 16, 128), BF16)], [], "combine", 8, 10**8)
    every = lax.all_to_all(every, GROUP, 0, 0).reshape(512, 128)
    hbm = pl.BlockSpec(memory_space=pltpu.HBM)
    filter_shape = (27, channels, channels)
    gv_first, gv_second, out = pl.pallas_call(
        lambda *refs: finish(factor / count_all, *refs),
        out_shape=(
            jax.ShapeDtypeStruct(filter_shape, F32),
            jax.ShapeDtypeStruct(filter_shape, F32),
            jax.ShapeDtypeStruct(volume.shape, BF16),
        ),
        in_specs=[pl.BlockSpec(memory_space=pltpu.VMEM)] * 4,
        out_specs=(hbm, hbm, pl.BlockSpec(memory_space=pltpu.VMEM)),
        scratch_shapes=[
            pltpu.VMEM(filter_shape, F32),
            pltpu.VMEM(filter_shape, F32),
            pltpu.VMEM((512, 128), F32),
            pltpu.SemaphoreType.DMA((6,)),
        ],
        compiler_params=pltpu.CompilerParams(vmem_limit_bytes=8 << 20),
        cost_estimate=pl.CostEstimate(flops=10**9, bytes_accessed=1 << 20, transcendentals=0),
        name="finish",
    )(every, *damping, parts)
    return (out, gv_first.reshape(v_first.shape), gv_second.reshape(v_first.shape))


def solution(mesh):
    in_specs = (P(None, "gx", "gy", "gz"), P(), P(), P(), P())
    out_specs = (P(None, "gx", "gy", "gz"), P(), P())
    return jax.shard_map(body, mesh=mesh, in_specs=in_specs, out_specs=out_specs, check_vma=False)
```

```python
import math

import jax
import jax.numpy as jnp
from jax import lax
from jax.experimental import pallas as pl
from jax.experimental.pallas import tpu as pltpu
from jax.sharding import PartitionSpec as P

F32 = jnp.float32
BF16 = jnp.bfloat16
AXES = ("gx", "gy", "gz")
GROUP = ("gx", "gy")
PLANES = 8
OWN = 4
MEMBERS = 32


def snake():
    def member(z, x):
        return z % 4 * 8 + z // 4 * 4 + x

    line = []
    for z in range(8):
        line += [member(z, x) for x in ((1, 2, 3) if z % 2 == 0 else (3, 2, 1))]
    return tuple(line + [member(z, 0) for z in reversed(range(8))])


LINES = (snake(), snake()[:1] + snake()[:0:-1])


def member_at(place):
    return jnp.where((lax.axis_index("gz") & 1) == 0, LINES[0][place], LINES[1][place])


def own_place():
    member = lax.axis_index("gx") * 8 + lax.axis_index("gy")
    place = jnp.int32(0)
    for at in range(MEMBERS):
        place = jnp.where(member == member_at(at), at, place)
    return place


def lanes_of(shape):
    return lax.broadcasted_iota(jnp.int32, shape, len(shape) - 1)


def exchange(tiles, bits):
    tiles = list(tiles)
    lane = lanes_of(tiles[0].shape)
    for place, bit in enumerate(bits):
        step = 1 << bit
        clear = (lane & step) == 0
        for low in range(len(tiles)):
            if low & (1 << place):
                continue
            high = low | (1 << place)
            a, b = tiles[low], tiles[high]
            tiles[low] = jnp.where(clear, a, pltpu.roll(b, step, 1))
            tiles[high] = jnp.where(clear, pltpu.roll(a, 128 - step, 1), b)
    return tiles


def permutation(inverse):
    source = lax.broadcasted_iota(jnp.int32, (128, 128), 0)
    target = lax.broadcasted_iota(jnp.int32, (128, 128), 1)
    if inverse:
        source, target = target, source
    hit = source == 4 * (target & 31) + (target >> 5)
    return jnp.where(hit, 1.0, 0.0).astype(BF16)


def pack(cells_ref, out_ref, sorted_ref):
    sorted_ref[...] = jnp.dot(
        cells_ref[...].reshape(1024, 128), permutation(False), preferred_element_type=F32
    )
    for part in range(4):
        tiles = [sorted_ref[pl.ds(256 * part + i, 8, stride=32)] for i in range(32)]
        tiles = exchange(tiles, (0, 1, 2, 3, 4))
        for i in range(MEMBERS):
            out_ref[member_at(i), 8 * part : 8 * part + 8] = tiles[i].astype(BF16)


def arrange(parts_ref, own_ref, first_ref, second_ref):
    for g in range(4):
        tiles = exchange([parts_ref[8 * g + j].astype(F32) for j in range(8)], (4, 5, 6))
        for i in range(8):
            plane = 2 * g + i % 2
            own_ref[i // 2, 32 * plane : 32 * plane + 32] = tiles[i].astype(BF16)
    odd = (own_place() & 1) == 1

    @pl.when(odd)
    def _():
        first_ref[...] = own_ref[0:3]
        second_ref[...] = own_ref[1:4]

    @pl.when(jnp.logical_not(odd))
    def _():
        first_ref[...] = own_ref[1:4]
        second_ref[...] = own_ref[0:3]


def unpack(parts_ref, out_ref, mixed_ref):
    for part in range(2):
        at = slice(16 * part, 16 * part + 16)
        tiles = [parts_ref[member_at(i), at].astype(F32) for i in range(MEMBERS)]
        tiles = exchange(tiles, (0, 1, 2, 3, 4))
        for i in range(32):
            mixed_ref[pl.ds(512 * part + i, 16, stride=32)] = tiles[i]
    moved = jnp.dot(mixed_ref[...].astype(BF16), permutation(True), preferred_element_type=F32)
    out_ref[...] = moved.astype(BF16).reshape(32, 2, 16, 128)


def gelu_pair(pre):
    inner = 0.7978845608 * (pre + 0.044715 * pre * pre * pre)
    hyper = jnp.tanh(inner)
    hidden = 0.5 * pre * (1.0 + hyper)
    slope = 0.5 * (1.0 + hyper) + 0.5 * pre * (1.0 - hyper * hyper) * 0.7978845608 * (
        1.0 + 0.134145 * pre * pre
    )
    return hidden, slope


def before(value):
    return jnp.where(lanes_of(value.shape) > 0, pltpu.roll(value, 1, 1), 0.0)


def after(value):
    return jnp.where(lanes_of(value.shape) < 127, pltpu.roll(value, 127, 1), 0.0)


def fold(product):
    return before(product[0:32]) + product[32:64] + after(product[64:96])


def near(groups, z, x, whole=False):
    def block(column):
        ref, at = column
        rows = ref[at, max(32 * x - 32, 0) : min(32 * x + 64, 256)]
        blank = jnp.zeros((32, 128), BF16)
        if whole and x == 0:
            return [blank, rows]
        if whole and x == PLANES - 1:
            return [rows, blank]
        return [rows]

    columns = []
    for at in range(2):
        rows = sum((block(group[z + at + offset]) for group in groups for offset in range(3)), [])
        columns.append(jnp.concatenate(rows, axis=0))
    return jnp.concatenate(columns, axis=1)


def tile_of(x):
    return slice(32 * x, 32 * x + 32)


def correlate(group, z, targets):
    rows = jnp.concatenate([near((group,), z, x, True) for x in range(PLANES)], axis=1)
    return lax.dot_general(
        rows,
        jnp.concatenate(targets, axis=1),
        (((1,), (1,)), ((), ())),
        preferred_element_type=F32,
    )


def layers(
    width,
    own_ref,
    first_ref,
    second_ref,
    weight_ref,
    joint_ref,
    edge_ref,
    edge_joint_ref,
    out_ref,
    p_halo,
    p_hid,
    p_tan,
    p_jv,
    slopes,
    packed,
):
    place = own_place()
    column = OWN * (lax.axis_index("gz") * MEMBERS + place)
    odd = (place & 1) == 1

    def inside(offset):
        return (column + offset >= 0) & (column + offset < width)

    for at in range(3):
        p_halo[at] = jnp.where(odd, first_ref[at], second_ref[at])
        p_halo[3 + at] = jnp.where(odd, second_ref[at], first_ref[at])
    volume = [(p_halo, at) for at in range(3)]
    volume += [(own_ref, at) for at in range(OWN)]
    volume += [(p_halo, 3 + at) for at in range(3)]
    hidden_columns = [(p_hid, at) for at in range(8)]
    tangent_columns = [(p_tan, at) for at in range(8)]
    jv_columns = [(p_jv, at) for at in range(6)]

    def weights(ref, edge, rows, x):
        if x == 0:
            return edge[0, rows]
        if x == PLANES - 1:
            return edge[1, rows]
        return ref[rows]

    for z in range(0, 8, 2):
        for x in range(PLANES):
            product = jnp.dot(
                weights(weight_ref, edge_ref, slice(0, 192), x),
                near((volume,), z, x),
                preferred_element_type=F32,
            )
            for at in range(2):
                part = product[:, 128 * at : 128 * at + 128]
                here = inside(z + at - 2)
                hidden, slope = gelu_pair(fold(part[0:96]))
                tangent = slope * fold(part[96:192])
                p_hid[z + at, tile_of(x)] = jnp.where(here, hidden, 0.0).astype(BF16)
                p_tan[z + at, tile_of(x)] = jnp.where(here, tangent, 0.0).astype(BF16)
                if 2 <= z + at < 6:
                    slopes[z + at - 2, x] = slope

    for z in range(0, 6, 2):
        for x in range(PLANES):
            product = jnp.dot(
                weights(joint_ref, edge_joint_ref, slice(0, 96), x),
                near((tangent_columns, hidden_columns), z, x),
                preferred_element_type=F32,
            )
            for at in range(2):
                jv = fold(product[:, 128 * at : 128 * at + 128])
                jv = jnp.where(inside(z + at - 1), jv, 0.0)
                p_jv[z + at, tile_of(x)] = jv.astype(BF16)

    for g in range(4):
        tiles = [p_jv[1 + i // 2, tile_of(2 * g + i % 2)].astype(F32) for i in range(8)]
        tiles = exchange(tiles, (4, 5, 6))
        for j in range(8):
            out_ref[8 * g + j, 0:32] = tiles[j].astype(BF16)

    def spread(tiles):
        both = [
            jnp.concatenate([after(tile), tile, before(tile), jnp.zeros_like(tile)], axis=0)
            for tile in tiles
        ]
        return jnp.concatenate(both, axis=1).astype(BF16)

    sums_first = sums_second = 0.0
    for z in range(0, OWN, 2):
        targets = [
            spread([p_jv[z + at + 1, tile_of(x)].astype(F32) for at in range(2)])
            for x in range(PLANES)
        ]
        sums_second = sums_second + correlate(hidden_columns, z + 1, targets)
        targets = []
        for x in range(PLANES):
            product = jnp.dot(
                weights(weight_ref, edge_ref, slice(192, 288), x),
                near((jv_columns,), z, x),
                preferred_element_type=F32,
            )
            tiles = []
            for at in range(2):
                back = slopes[z + at, x] * fold(product[:, 128 * at : 128 * at + 128])
                tiles.append(back.astype(BF16).astype(F32))
            targets.append(spread(tiles))
        sums_first = sums_first + correlate(volume, z + 2, targets)

    rest = pltpu.roll(sums_first, 96, 1)
    packed[0:288] = jnp.where(lanes_of((288, 128)) < 96, sums_second, rest)
    packed[288:432] = jnp.where(
        lanes_of((144, 128)) < 64, rest[0:144], pltpu.roll(rest[144:288], 64, 1)
    )
    packed[432:512] = jnp.zeros((80, 128), F32)
    for member in range(MEMBERS):
        out_ref[member, 32:48] = packed[16 * member : 16 * member + 16].astype(BF16)


def gather_sums(parts_ref, out_ref):
    total = jnp.sum(parts_ref[:, 32:48].astype(F32), axis=0)
    for member in range(8):
        out_ref[member] = total


def combine(parts_ref, out_ref):
    total = jnp.sum(parts_ref[...], axis=0).astype(BF16)
    for member in range(MEMBERS):
        out_ref[member] = total


def finish(scale, packed_ref, d_first_ref, d_second_ref, first_ref, second_ref, rest_ref):
    depth = pl.program_id(0)

    @pl.when(depth == 0)
    def _():
        rest = packed_ref[288:432, :].astype(F32)
        rest_ref[0:144] = rest
        rest_ref[144:288] = pltpu.roll(rest, 64, 1)

    def damped(summed, damping):
        return scale * summed + damping

    for column in range(3):
        block = pl.ds(pl.multiple_of(96 * column + 32 * depth, 32), 32)
        low = packed_ref[block, :].astype(F32)
        far = rest_ref[block, :]
        for row in range(3):
            at = 3 * row + column
            second_ref[at] = damped(low[:, 32 * row : 32 * row + 32], d_second_ref[at])
        first_ref[column] = damped(low[:, 96:128], d_first_ref[column])
        first_ref[3 + column] = damped(far[:, 0:32], d_first_ref[3 + column])
        first_ref[6 + column] = damped(far[:, 32:64], d_first_ref[6 + column])


def filters(
    w_first_ref, v_first_ref, w_second_ref, v_second_ref, rows_ref, joint_ref, edge_ref, edge_joint_ref
):
    def turned(refs, depths):
        blocks = [(x, z) for z in range(3) for x in depths]
        tall = [
            jnp.concatenate(
                [
                    jnp.concatenate([ref[9 * x + 3 * row + z].astype(F32) for x, z in blocks], axis=0)
                    for row in range(3)
                ],
                axis=1,
            )
            for ref in refs
        ]
        return jnp.concatenate(tall, axis=0).T.astype(BF16)

    def flipped(row, depths):
        blocks = [
            w_second_ref[26 - (9 * x + 3 * row + z)].astype(F32) for z in range(3) for x in depths
        ]
        return jnp.concatenate(blocks, axis=1).astype(BF16)

    for depths, rows, joint in (
        ((0, 1, 2), rows_ref, joint_ref),
        ((1, 2), edge_ref.at[0], edge_joint_ref.at[0]),
        ((0, 1), edge_ref.at[1], edge_joint_ref.at[1]),
    ):
        rows[0:96] = turned([w_first_ref], depths)
        rows[96:192] = turned([v_first_ref], depths)
        joint[...] = turned([w_second_ref, v_second_ref], depths)
        for row in range(3):
            rows[192 + 32 * row : 224 + 32 * row] = flipped(row, depths)


def call(kernel, operands, outputs, scratch, name, limit, flops):
    vmem = pl.BlockSpec(memory_space=pltpu.VMEM)
    return pl.pallas_call(
        kernel,
        out_shape=tuple(jax.ShapeDtypeStruct(shape, dtype) for shape, dtype in outputs),
        in_specs=[vmem] * len(operands),
        out_specs=(vmem,) * len(outputs),
        scratch_shapes=[pltpu.VMEM(shape, dtype) for shape, dtype in scratch],
        compiler_params=pltpu.CompilerParams(vmem_limit_bytes=limit << 20),
        cost_estimate=pl.CostEstimate(flops=flops, bytes_accessed=1 << 20, transcendentals=0),
        name=name,
    )(*operands)


def body(volume, w_first, w_second, v_first, v_second):
    channels, depth, height, width = volume.shape
    n_gx, n_gy, n_gz = (lax.axis_size(axis) for axis in AXES)
    members = n_gx * n_gy
    count_all = float(depth * n_gx * height * n_gy * width * n_gz)
    factor = math.sqrt(27.0 * channels)
    small = (channels, 128)

    (sent,) = call(
        pack, (volume,), [((members,) + small, BF16)], [((1024, 128), F32)], "pack", 8, 10**8
    )
    parts = lax.all_to_all(sent, GROUP, 0, 0)

    parts, w_first, w_second, v_first, v_second = lax.optimization_barrier(
        (parts, w_first, w_second, v_first, v_second)
    )
    blocks = [w.reshape(27, channels, channels) for w in (w_first, v_first, w_second, v_second)]
    weights = call(
        filters,
        blocks,
        [((288, 288), BF16), ((96, 576), BF16), ((2, 288, 192), BF16), ((2, 96, 384), BF16)],
        [],
        "filters",
        8,
        2 * 10**8,
    )
    damping = tuple(
        factor * 0.1 * v.astype(F32).reshape(27, channels, channels) for v in (v_first, v_second)
    )

    halo = ((OWN - 1, 256, 128), BF16)
    own, first, second = call(
        arrange, (parts,), [((OWN, 256, 128), BF16), halo, halo], [], "arrange", 8, 10**8
    )

    def swapped(start):
        def device(at):
            gz, place = divmod(at, members)
            return LINES[gz % 2][place] * n_gz + gz

        pairs = [(device(i), device(i + 1)) for i in range(start, members * n_gz - 1, 2)]
        return pairs + [(b, a) for a, b in pairs]

    first = lax.ppermute(first, AXES, swapped(0))
    second = lax.ppermute(second, AXES, swapped(1))

    (leaving,) = call(
        lambda *refs: layers(width * n_gz, *refs),
        (own, first, second, *weights),
        [((members, 48, 128), BF16)],
        [
            ((6, 256, 128), BF16),
            ((8, 256, 128), BF16),
            ((8, 256, 128), BF16),
            ((6, 256, 128), BF16),
            ((OWN, PLANES) + small, F32),
            ((512, 128), F32),
        ],
        "layers",
        24,
        8 * 10**9,
    )

    parts = lax.all_to_all(leaving, GROUP, 0, 0)
    (sums,) = call(gather_sums, (parts,), [((n_gz, 16, 128), F32)], [], "gather_sums", 8, 10**8)
    sums = lax.all_to_all(sums, "gz", 0, 0)
    (every,) = call(combine, (sums,), [((members, 16, 128), BF16)], [], "combine", 8, 10**8)
    every = lax.all_to_all(every, GROUP, 0, 0).reshape(512, 128)
    (out,) = call(
        unpack,
        (parts,),
        [(volume.shape, BF16)],
        [((1024, 128), F32)],
        "unpack",
        8,
        10**9,
    )
    third = pl.BlockSpec((9, channels, channels), lambda i: (i, 0, 0))
    gv_first, gv_second = pl.pallas_call(
        lambda *refs: finish(factor / count_all, *refs),
        grid=(3,),
        out_shape=(jax.ShapeDtypeStruct((27, channels, channels), F32),) * 2,
        in_specs=[pl.BlockSpec((512, 128), lambda i: (0, 0)), third, third],
        out_specs=(third, third),
        scratch_shapes=[pltpu.VMEM((288, 128), F32)],
        compiler_params=pltpu.CompilerParams(
            dimension_semantics=("arbitrary",), vmem_limit_bytes=8 << 20
        ),
        name="finish",
    )(every, *damping)
    return (out, gv_first.reshape(v_first.shape), gv_second.reshape(v_first.shape))


def solution(mesh):
    in_specs = (P(None, "gx", "gy", "gz"), P(), P(), P(), P())
    out_specs = (P(None, "gx", "gy", "gz"), P(), P())
    return jax.shard_map(body, mesh=mesh, in_specs=in_specs, out_specs=out_specs, check_vma=False)
```

```python
import math

import jax
import jax.numpy as jnp
from jax import lax
from jax.experimental import pallas as pl
from jax.experimental.pallas import tpu as pltpu
from jax.sharding import PartitionSpec as P

F32 = jnp.float32
BF16 = jnp.bfloat16
AXES = ("gx", "gy", "gz")
GROUP = ("gx", "gy")
PLANES = 8
OWN = 4
MEMBERS = 32


def snake():
    def member(z, x):
        return z % 4 * 8 + z // 4 * 4 + x

    line = []
    for z in range(8):
        line += [member(z, x) for x in ((1, 2, 3) if z % 2 == 0 else (3, 2, 1))]
    return tuple(line + [member(z, 0) for z in reversed(range(8))])


LINES = (snake(), snake()[:1] + snake()[:0:-1])


def member_at(place):
    return jnp.where((lax.axis_index("gz") & 1) == 0, LINES[0][place], LINES[1][place])


def own_place():
    member = lax.axis_index("gx") * 8 + lax.axis_index("gy")
    place = jnp.int32(0)
    for at in range(MEMBERS):
        place = jnp.where(member == member_at(at), at, place)
    return place


def lanes_of(shape):
    return lax.broadcasted_iota(jnp.int32, shape, len(shape) - 1)


def exchange(tiles, bits):
    tiles = list(tiles)
    lane = lanes_of(tiles[0].shape)
    for place, bit in enumerate(bits):
        step = 1 << bit
        clear = (lane & step) == 0
        for low in range(len(tiles)):
            if low & (1 << place):
                continue
            high = low | (1 << place)
            a, b = tiles[low], tiles[high]
            tiles[low] = jnp.where(clear, a, pltpu.roll(b, step, 1))
            tiles[high] = jnp.where(clear, pltpu.roll(a, 128 - step, 1), b)
    return tiles


def permutation(inverse):
    source = lax.broadcasted_iota(jnp.int32, (128, 128), 0)
    target = lax.broadcasted_iota(jnp.int32, (128, 128), 1)
    if inverse:
        source, target = target, source
    hit = source == 4 * (target & 31) + (target >> 5)
    return jnp.where(hit, 1.0, 0.0).astype(BF16)


def pack(cells_ref, out_ref, sorted_ref):
    sorted_ref[...] = jnp.dot(
        cells_ref[...].reshape(1024, 128), permutation(False), preferred_element_type=F32
    )
    for part in range(4):
        tiles = [sorted_ref[pl.ds(256 * part + i, 8, stride=32)] for i in range(32)]
        tiles = exchange(tiles, (0, 1, 2, 3, 4))
        for i in range(MEMBERS):
            out_ref[member_at(i), 8 * part : 8 * part + 8] = tiles[i].astype(BF16)


def arrange(parts_ref, own_ref, first_ref, second_ref):
    for g in range(4):
        tiles = exchange([parts_ref[8 * g + j].astype(F32) for j in range(8)], (4, 5, 6))
        for i in range(8):
            plane = 2 * g + i % 2
            own_ref[i // 2, 32 * plane : 32 * plane + 32] = tiles[i].astype(BF16)
    odd = (own_place() & 1) == 1

    @pl.when(odd)
    def _():
        first_ref[...] = own_ref[0:3]
        second_ref[...] = own_ref[1:4]

    @pl.when(jnp.logical_not(odd))
    def _():
        first_ref[...] = own_ref[1:4]
        second_ref[...] = own_ref[0:3]


def unpack(parts_ref, out_ref, mixed_ref):
    for part in range(2):
        at = slice(16 * part, 16 * part + 16)
        tiles = [parts_ref[member_at(i), at].astype(F32) for i in range(MEMBERS)]
        tiles = exchange(tiles, (0, 1, 2, 3, 4))
        for i in range(32):
            mixed_ref[pl.ds(512 * part + i, 16, stride=32)] = tiles[i]
    moved = jnp.dot(mixed_ref[...].astype(BF16), permutation(True), preferred_element_type=F32)
    out_ref[...] = moved.astype(BF16).reshape(32, 2, 16, 128)


def gelu_pair(pre):
    inner = 0.7978845608 * (pre + 0.044715 * pre * pre * pre)
    hyper = jnp.tanh(inner)
    hidden = 0.5 * pre * (1.0 + hyper)
    slope = 0.5 * (1.0 + hyper) + 0.5 * pre * (1.0 - hyper * hyper) * 0.7978845608 * (
        1.0 + 0.134145 * pre * pre
    )
    return hidden, slope


def before(value):
    return jnp.where(lanes_of(value.shape) > 0, pltpu.roll(value, 1, 1), 0.0)


def after(value):
    return jnp.where(lanes_of(value.shape) < 127, pltpu.roll(value, 127, 1), 0.0)


def fold(product):
    return before(product[0:32]) + product[32:64] + after(product[64:96])


def near(groups, z, x, whole=False):
    def block(column):
        ref, at = column
        rows = ref[at, max(32 * x - 32, 0) : min(32 * x + 64, 256)]
        blank = jnp.zeros((32, 128), BF16)
        if whole and x == 0:
            return [blank, rows]
        if whole and x == PLANES - 1:
            return [rows, blank]
        return [rows]

    columns = []
    for at in range(2):
        rows = sum((block(group[z + at + offset]) for group in groups for offset in range(3)), [])
        columns.append(jnp.concatenate(rows, axis=0))
    return jnp.concatenate(columns, axis=1)


def tile_of(x):
    return slice(32 * x, 32 * x + 32)


def correlate(group, z, targets):
    rows = jnp.concatenate([near((group,), z, x, True) for x in range(PLANES)], axis=1)
    return lax.dot_general(
        rows,
        jnp.concatenate(targets, axis=1),
        (((1,), (1,)), ((), ())),
        preferred_element_type=F32,
    )


def layers(
    width,
    own_ref,
    first_ref,
    second_ref,
    weight_ref,
    joint_ref,
    edge_ref,
    edge_joint_ref,
    out_ref,
    p_halo,
    p_hid,
    p_tan,
    p_jv,
    slopes,
    packed,
):
    place = own_place()
    column = OWN * (lax.axis_index("gz") * MEMBERS + place)
    odd = (place & 1) == 1

    def inside(offset):
        return (column + offset >= 0) & (column + offset < width)

    for at in range(3):
        p_halo[at] = jnp.where(odd, first_ref[at], second_ref[at])
        p_halo[3 + at] = jnp.where(odd, second_ref[at], first_ref[at])
    volume = [(p_halo, at) for at in range(3)]
    volume += [(own_ref, at) for at in range(OWN)]
    volume += [(p_halo, 3 + at) for at in range(3)]
    hidden_columns = [(p_hid, at) for at in range(8)]
    tangent_columns = [(p_tan, at) for at in range(8)]
    jv_columns = [(p_jv, at) for at in range(6)]

    def weights(ref, edge, rows, x):
        if x == 0:
            return edge[0, rows]
        if x == PLANES - 1:
            return edge[1, rows]
        return ref[rows]

    for z in range(0, 8, 2):
        for x in range(PLANES):
            product = jnp.dot(
                weights(weight_ref, edge_ref, slice(0, 192), x),
                near((volume,), z, x),
                preferred_element_type=F32,
            )
            for at in range(2):
                part = product[:, 128 * at : 128 * at + 128]
                here = inside(z + at - 2)
                hidden, slope = gelu_pair(fold(part[0:96]))
                tangent = slope * fold(part[96:192])
                p_hid[z + at, tile_of(x)] = jnp.where(here, hidden, 0.0).astype(BF16)
                p_tan[z + at, tile_of(x)] = jnp.where(here, tangent, 0.0).astype(BF16)
                if 2 <= z + at < 6:
                    slopes[z + at - 2, x] = slope

    for z in range(0, 6, 2):
        for x in range(PLANES):
            product = jnp.dot(
                weights(joint_ref, edge_joint_ref, slice(0, 96), x),
                near((tangent_columns, hidden_columns), z, x),
                preferred_element_type=F32,
            )
            for at in range(2):
                jv = fold(product[:, 128 * at : 128 * at + 128])
                jv = jnp.where(inside(z + at - 1), jv, 0.0)
                p_jv[z + at, tile_of(x)] = jv.astype(BF16)

    for g in range(4):
        tiles = [p_jv[1 + i // 2, tile_of(2 * g + i % 2)].astype(F32) for i in range(8)]
        tiles = exchange(tiles, (4, 5, 6))
        for j in range(8):
            out_ref[8 * g + j, 0:32] = tiles[j].astype(BF16)

    def spread(tiles):
        both = [
            jnp.concatenate([after(tile), tile, before(tile), jnp.zeros_like(tile)], axis=0)
            for tile in tiles
        ]
        return jnp.concatenate(both, axis=1).astype(BF16)

    sums_first = sums_second = 0.0
    for z in range(0, OWN, 2):
        targets = [
            spread([p_jv[z + at + 1, tile_of(x)].astype(F32) for at in range(2)])
            for x in range(PLANES)
        ]
        sums_second = sums_second + correlate(hidden_columns, z + 1, targets)
        targets = []
        for x in range(PLANES):
            product = jnp.dot(
                weights(weight_ref, edge_ref, slice(192, 288), x),
                near((jv_columns,), z, x),
                preferred_element_type=F32,
            )
            tiles = []
            for at in range(2):
                back = slopes[z + at, x] * fold(product[:, 128 * at : 128 * at + 128])
                tiles.append(back.astype(BF16).astype(F32))
            targets.append(spread(tiles))
        sums_first = sums_first + correlate(volume, z + 2, targets)

    rest = pltpu.roll(sums_first, 96, 1)
    packed[0:288] = jnp.where(lanes_of((288, 128)) < 96, sums_second, rest)
    packed[288:432] = jnp.where(
        lanes_of((144, 128)) < 64, rest[0:144], pltpu.roll(rest[144:288], 64, 1)
    )
    packed[432:512] = jnp.zeros((80, 128), F32)
    for member in range(MEMBERS):
        out_ref[member, 32:48] = packed[16 * member : 16 * member + 16].astype(BF16)


def gather_sums(parts_ref, out_ref):
    total = jnp.sum(parts_ref[:, 32:48].astype(F32), axis=0)
    for member in range(8):
        out_ref[member] = total


def combine(parts_ref, out_ref):
    total = jnp.sum(parts_ref[...], axis=0).astype(BF16)
    for member in range(MEMBERS):
        out_ref[member] = total


def finish(scale, packed_ref, d_first_ref, d_second_ref, first_ref, second_ref, rest_ref):
    depth = pl.program_id(0)

    @pl.when(depth == 0)
    def _():
        rest = packed_ref[288:432, :].astype(F32)
        rest_ref[0:144] = rest
        rest_ref[144:288] = pltpu.roll(rest, 64, 1)

    def damped(summed, damping):
        return scale * summed + damping

    for column in range(3):
        block = pl.ds(pl.multiple_of(96 * column + 32 * depth, 32), 32)
        low = packed_ref[block, :].astype(F32)
        far = rest_ref[block, :]
        for row in range(3):
            at = 3 * row + column
            second_ref[at] = damped(low[:, 32 * row : 32 * row + 32], d_second_ref[at])
        first_ref[column] = damped(low[:, 96:128], d_first_ref[column])
        first_ref[3 + column] = damped(far[:, 0:32], d_first_ref[3 + column])
        first_ref[6 + column] = damped(far[:, 32:64], d_first_ref[6 + column])


def filters(
    w_first_ref, v_first_ref, w_second_ref, v_second_ref, rows_ref, joint_ref, edge_ref, edge_joint_ref
):
    def turned(refs, depths):
        blocks = [(x, z) for z in range(3) for x in depths]
        tall = [
            jnp.concatenate(
                [
                    jnp.concatenate([ref[9 * x + 3 * row + z].astype(F32) for x, z in blocks], axis=0)
                    for row in range(3)
                ],
                axis=1,
            )
            for ref in refs
        ]
        return jnp.concatenate(tall, axis=0).T.astype(BF16)

    def flipped(row, depths):
        blocks = [
            w_second_ref[26 - (9 * x + 3 * row + z)].astype(F32) for z in range(3) for x in depths
        ]
        return jnp.concatenate(blocks, axis=1).astype(BF16)

    for depths, rows, joint in (
        ((0, 1, 2), rows_ref, joint_ref),
        ((1, 2), edge_ref.at[0], edge_joint_ref.at[0]),
        ((0, 1), edge_ref.at[1], edge_joint_ref.at[1]),
    ):
        rows[0:96] = turned([w_first_ref], depths)
        rows[96:192] = turned([v_first_ref], depths)
        joint[...] = turned([w_second_ref, v_second_ref], depths)
        for row in range(3):
            rows[192 + 32 * row : 224 + 32 * row] = flipped(row, depths)


def call(kernel, operands, outputs, scratch, name, limit, flops):
    vmem = pl.BlockSpec(memory_space=pltpu.VMEM)
    return pl.pallas_call(
        kernel,
        out_shape=tuple(jax.ShapeDtypeStruct(shape, dtype) for shape, dtype in outputs),
        in_specs=[vmem] * len(operands),
        out_specs=(vmem,) * len(outputs),
        scratch_shapes=[pltpu.VMEM(shape, dtype) for shape, dtype in scratch],
        compiler_params=pltpu.CompilerParams(vmem_limit_bytes=limit << 20),
        cost_estimate=pl.CostEstimate(flops=flops, bytes_accessed=1 << 20, transcendentals=0),
        name=name,
    )(*operands)


def body(volume, w_first, w_second, v_first, v_second):
    channels, depth, height, width = volume.shape
    n_gx, n_gy, n_gz = (lax.axis_size(axis) for axis in AXES)
    members = n_gx * n_gy
    count_all = float(depth * n_gx * height * n_gy * width * n_gz)
    factor = math.sqrt(27.0 * channels)
    small = (channels, 128)

    (sent,) = call(
        pack, (volume,), [((members,) + small, BF16)], [((1024, 128), F32)], "pack", 8, 10**8
    )
    parts = lax.all_to_all(sent, GROUP, 0, 0)

    parts, w_first, w_second, v_first, v_second = lax.optimization_barrier(
        (parts, w_first, w_second, v_first, v_second)
    )
    blocks = [w.reshape(27, channels, channels) for w in (w_first, v_first, w_second, v_second)]
    weights = call(
        filters,
        blocks,
        [((288, 288), BF16), ((96, 576), BF16), ((2, 288, 192), BF16), ((2, 96, 384), BF16)],
        [],
        "filters",
        8,
        2 * 10**8,
    )
    damping = tuple(
        factor * 0.1 * v.astype(F32).reshape(27, channels, channels) for v in (v_first, v_second)
    )

    halo = ((OWN - 1, 256, 128), BF16)
    own, first, second = call(
        arrange, (parts,), [((OWN, 256, 128), BF16), halo, halo], [], "arrange", 8, 10**8
    )

    def swapped(start):
        def device(at):
            gz, place = divmod(at, members)
            return LINES[gz % 2][place] * n_gz + gz

        pairs = [(device(i), device(i + 1)) for i in range(start, members * n_gz - 1, 2)]
        return pairs + [(b, a) for a, b in pairs]

    first = lax.ppermute(first, AXES, swapped(0))
    second = lax.ppermute(second, AXES, swapped(1))
    first, second, damping = lax.optimization_barrier((first, second, damping))

    (leaving,) = call(
        lambda *refs: layers(width * n_gz, *refs),
        (own, first, second, *weights),
        [((members, 48, 128), BF16)],
        [
            ((6, 256, 128), BF16),
            ((8, 256, 128), BF16),
            ((8, 256, 128), BF16),
            ((6, 256, 128), BF16),
            ((OWN, PLANES) + small, F32),
            ((512, 128), F32),
        ],
        "layers",
        24,
        8 * 10**9,
    )

    parts = lax.all_to_all(leaving, GROUP, 0, 0)
    (sums,) = call(gather_sums, (parts,), [((n_gz, 16, 128), F32)], [], "gather_sums", 8, 10**8)
    sums = lax.all_to_all(sums, "gz", 0, 0)
    (out,) = call(
        unpack,
        (parts,),
        [(volume.shape, BF16)],
        [((1024, 128), F32)],
        "unpack",
        8,
        10**9,
    )
    sums, out = lax.optimization_barrier((sums, out))
    (every,) = call(combine, (sums,), [((members, 16, 128), BF16)], [], "combine", 8, 10**8)
    every = lax.all_to_all(every, GROUP, 0, 0).reshape(512, 128)
    third = pl.BlockSpec((9, channels, channels), lambda i: (i, 0, 0))
    gv_first, gv_second = pl.pallas_call(
        lambda *refs: finish(factor / count_all, *refs),
        grid=(3,),
        out_shape=(jax.ShapeDtypeStruct((27, channels, channels), F32),) * 2,
        in_specs=[pl.BlockSpec((512, 128), lambda i: (0, 0)), third, third],
        out_specs=(third, third),
        scratch_shapes=[pltpu.VMEM((288, 128), F32)],
        compiler_params=pltpu.CompilerParams(
            dimension_semantics=("arbitrary",), vmem_limit_bytes=8 << 20
        ),
        name="finish",
    )(every, *damping)
    return (out, gv_first.reshape(v_first.shape), gv_second.reshape(v_first.shape))


def solution(mesh):
    in_specs = (P(None, "gx", "gy", "gz"), P(), P(), P(), P())
    out_specs = (P(None, "gx", "gy", "gz"), P(), P())
    return jax.shard_map(body, mesh=mesh, in_specs=in_specs, out_specs=out_specs, check_vma=False)
```

```python
import math

import jax
import jax.numpy as jnp
from jax import lax
from jax.experimental import pallas as pl
from jax.experimental.pallas import tpu as pltpu
from jax.sharding import PartitionSpec as P

F32 = jnp.float32
BF16 = jnp.bfloat16
AXES = ("gx", "gy", "gz")
GROUP = ("gx", "gy")
PLANES = 8
OWN = 4
MEMBERS = 32


def snake():
    def member(z, x):
        return z % 4 * 8 + z // 4 * 4 + x

    line = []
    for z in range(8):
        line += [member(z, x) for x in ((1, 2, 3) if z % 2 == 0 else (3, 2, 1))]
    return tuple(line + [member(z, 0) for z in reversed(range(8))])


LINES = (snake(), snake()[:1] + snake()[:0:-1])


def member_at(place):
    return jnp.where((lax.axis_index("gz") & 1) == 0, LINES[0][place], LINES[1][place])


def own_place():
    member = lax.axis_index("gx") * 8 + lax.axis_index("gy")
    place = jnp.int32(0)
    for at in range(MEMBERS):
        place = jnp.where(member == member_at(at), at, place)
    return place


def lanes_of(shape):
    return lax.broadcasted_iota(jnp.int32, shape, len(shape) - 1)


def exchange(tiles, bits):
    tiles = list(tiles)
    lane = lanes_of(tiles[0].shape)
    for place, bit in enumerate(bits):
        step = 1 << bit
        clear = (lane & step) == 0
        for low in range(len(tiles)):
            if low & (1 << place):
                continue
            high = low | (1 << place)
            a, b = tiles[low], tiles[high]
            tiles[low] = jnp.where(clear, a, pltpu.roll(b, step, 1))
            tiles[high] = jnp.where(clear, pltpu.roll(a, 128 - step, 1), b)
    return tiles


def permutation(inverse):
    source = lax.broadcasted_iota(jnp.int32, (128, 128), 0)
    target = lax.broadcasted_iota(jnp.int32, (128, 128), 1)
    if inverse:
        source, target = target, source
    hit = source == 4 * (target & 31) + (target >> 5)
    return jnp.where(hit, 1.0, 0.0).astype(BF16)


def pack(cells_ref, out_ref, sorted_ref):
    sorted_ref[...] = jnp.dot(
        cells_ref[...].reshape(1024, 128), permutation(False), preferred_element_type=F32
    )
    for part in range(4):
        tiles = [sorted_ref[pl.ds(256 * part + i, 8, stride=32)] for i in range(32)]
        tiles = exchange(tiles, (0, 1, 2, 3, 4))
        for i in range(MEMBERS):
            out_ref[member_at(i), 8 * part : 8 * part + 8] = tiles[i].astype(BF16)


def arrange(parts_ref, own_ref, first_ref, second_ref):
    for g in range(4):
        tiles = exchange([parts_ref[8 * g + j].astype(F32) for j in range(8)], (4, 5, 6))
        for i in range(8):
            plane = 2 * g + i % 2
            own_ref[i // 2, 32 * plane : 32 * plane + 32] = tiles[i].astype(BF16)
    odd = (own_place() & 1) == 1

    @pl.when(odd)
    def _():
        first_ref[...] = own_ref[0:3]
        second_ref[...] = own_ref[1:4]

    @pl.when(jnp.logical_not(odd))
    def _():
        first_ref[...] = own_ref[1:4]
        second_ref[...] = own_ref[0:3]


def unpack(parts_ref, out_ref, mixed_ref):
    for part in range(2):
        at = slice(16 * part, 16 * part + 16)
        tiles = [parts_ref[member_at(i), at].astype(F32) for i in range(MEMBERS)]
        tiles = exchange(tiles, (0, 1, 2, 3, 4))
        for i in range(32):
            mixed_ref[pl.ds(512 * part + i, 16, stride=32)] = tiles[i]
    moved = jnp.dot(mixed_ref[...].astype(BF16), permutation(True), preferred_element_type=F32)
    out_ref[...] = moved.astype(BF16).reshape(32, 2, 16, 128)


def gelu_pair(pre):
    inner = 0.7978845608 * (pre + 0.044715 * pre * pre * pre)
    hyper = jnp.tanh(inner)
    hidden = 0.5 * pre * (1.0 + hyper)
    slope = 0.5 * (1.0 + hyper) + 0.5 * pre * (1.0 - hyper * hyper) * 0.7978845608 * (
        1.0 + 0.134145 * pre * pre
    )
    return hidden, slope


def before(value):
    return jnp.where(lanes_of(value.shape) > 0, pltpu.roll(value, 1, 1), 0.0)


def after(value):
    return jnp.where(lanes_of(value.shape) < 127, pltpu.roll(value, 127, 1), 0.0)


def fold(product):
    return before(product[0:32]) + product[32:64] + after(product[64:96])


def near(groups, pair, x, whole=False):
    def block(column):
        ref, at = column
        rows = ref[at, max(32 * x - 32, 0) : min(32 * x + 64, 256)]
        blank = jnp.zeros((32, 128), BF16)
        if whole and x == 0:
            return [blank, rows]
        if whole and x == PLANES - 1:
            return [rows, blank]
        return [rows]

    columns = []
    for z in pair:
        rows = sum((block(group[z + offset]) for group in groups for offset in range(3)), [])
        columns.append(jnp.concatenate(rows, axis=0))
    return jnp.concatenate(columns, axis=1)


def tile_of(x):
    return slice(32 * x, 32 * x + 32)


def correlate(group, z, targets):
    rows = jnp.concatenate([near((group,), (z, z + 1), x, True) for x in range(PLANES)], axis=1)
    return lax.dot_general(
        rows,
        jnp.concatenate(targets, axis=1),
        (((1,), (1,)), ((), ())),
        preferred_element_type=F32,
    )


def weights(ref, edge, rows, x):
    if x == 0:
        return edge[0, rows]
    if x == PLANES - 1:
        return edge[1, rows]
    return ref[rows]


def first_layer(weight_ref, edge_ref, volume, pair, x):
    product = jnp.dot(
        weights(weight_ref, edge_ref, slice(0, 192), x),
        near((volume,), pair, x),
        preferred_element_type=F32,
    )
    for at in range(2):
        part = product[:, 128 * at : 128 * at + 128]
        hidden, slope = gelu_pair(fold(part[0:96]))
        yield hidden, slope * fold(part[96:192]), slope


def inner(own_ref, weight_ref, edge_ref, hidden_ref, tangent_ref, slope_ref):
    volume = [(own_ref, at) for at in range(OWN)]
    for x in range(PLANES):
        for at, (hidden, tangent, slope) in enumerate(
            first_layer(weight_ref, edge_ref, volume, (0, 1), x)
        ):
            hidden_ref[at, tile_of(x)] = hidden.astype(BF16)
            tangent_ref[at, tile_of(x)] = tangent.astype(BF16)
            slope_ref[at, x] = slope


def layers(
    width,
    own_ref,
    first_ref,
    second_ref,
    weight_ref,
    joint_ref,
    edge_ref,
    edge_joint_ref,
    hidden_ref,
    tangent_ref,
    slope_ref,
    out_ref,
    p_halo,
    p_hid,
    p_tan,
    p_jv,
    slopes,
    packed,
):
    place = own_place()
    column = OWN * (lax.axis_index("gz") * MEMBERS + place)
    odd = (place & 1) == 1

    def inside(offset):
        return (column + offset >= 0) & (column + offset < width)

    for at in range(3):
        p_halo[at] = jnp.where(odd, first_ref[at], second_ref[at])
        p_halo[3 + at] = jnp.where(odd, second_ref[at], first_ref[at])
    volume = [(p_halo, at) for at in range(3)]
    volume += [(own_ref, at) for at in range(OWN)]
    volume += [(p_halo, 3 + at) for at in range(3)]
    hidden_columns = [(p_hid, at) for at in range(8)]
    tangent_columns = [(p_tan, at) for at in range(8)]
    for at in range(2):
        hidden_columns[3 + at] = (hidden_ref, at)
        tangent_columns[3 + at] = (tangent_ref, at)
    jv_columns = [(p_jv, at) for at in range(6)]

    for pair in ((1, 2), (5, 6), (0, 7)):
        for x in range(PLANES):
            for z, (hidden, tangent, slope) in zip(
                pair, first_layer(weight_ref, edge_ref, volume, pair, x)
            ):
                here = inside(z - 2)
                p_hid[z, tile_of(x)] = jnp.where(here, hidden, 0.0).astype(BF16)
                p_tan[z, tile_of(x)] = jnp.where(here, tangent, 0.0).astype(BF16)
                if z in (2, 5):
                    slopes[z - 2, x] = slope

    for z in range(0, 6, 2):
        for x in range(PLANES):
            product = jnp.dot(
                weights(joint_ref, edge_joint_ref, slice(0, 96), x),
                near((tangent_columns, hidden_columns), (z, z + 1), x),
                preferred_element_type=F32,
            )
            for at in range(2):
                jv = fold(product[:, 128 * at : 128 * at + 128])
                jv = jnp.where(inside(z + at - 1), jv, 0.0)
                p_jv[z + at, tile_of(x)] = jv.astype(BF16)

    for g in range(4):
        tiles = [p_jv[1 + i // 2, tile_of(2 * g + i % 2)].astype(F32) for i in range(8)]
        tiles = exchange(tiles, (4, 5, 6))
        for j in range(8):
            out_ref[8 * g + j, 0:32] = tiles[j].astype(BF16)

    def spread(tiles):
        both = [
            jnp.concatenate([after(tile), tile, before(tile), jnp.zeros_like(tile)], axis=0)
            for tile in tiles
        ]
        return jnp.concatenate(both, axis=1).astype(BF16)

    sums_first = sums_second = 0.0
    for z in range(0, OWN, 2):
        targets = [
            spread([p_jv[z + at + 1, tile_of(x)].astype(F32) for at in range(2)])
            for x in range(PLANES)
        ]
        sums_second = sums_second + correlate(hidden_columns, z + 1, targets)
        targets = []
        for x in range(PLANES):
            product = jnp.dot(
                weights(weight_ref, edge_ref, slice(192, 288), x),
                near((jv_columns,), (z, z + 1), x),
                preferred_element_type=F32,
            )
            tiles = []
            for at in range(2):
                slope = slope_ref[z + at - 1, x] if z + at in (1, 2) else slopes[z + at, x]
                back = slope * fold(product[:, 128 * at : 128 * at + 128])
                tiles.append(back.astype(BF16).astype(F32))
            targets.append(spread(tiles))
        sums_first = sums_first + correlate(volume, z + 2, targets)

    rest = pltpu.roll(sums_first, 96, 1)
    packed[0:288] = jnp.where(lanes_of((288, 128)) < 96, sums_second, rest)
    packed[288:432] = jnp.where(
        lanes_of((144, 128)) < 64, rest[0:144], pltpu.roll(rest[144:288], 64, 1)
    )
    packed[432:512] = jnp.zeros((80, 128), F32)
    for member in range(MEMBERS):
        out_ref[member, 32:48] = packed[16 * member : 16 * member + 16].astype(BF16)


def gather_sums(parts_ref, out_ref):
    total = jnp.sum(parts_ref[:, 32:48].astype(F32), axis=0)
    for member in range(8):
        out_ref[member] = total


def combine(parts_ref, out_ref):
    total = jnp.sum(parts_ref[...], axis=0).astype(BF16)
    for member in range(MEMBERS):
        out_ref[member] = total


def finish(scale, packed_ref, d_first_ref, d_second_ref, first_ref, second_ref, rest_ref):
    depth = pl.program_id(0)

    @pl.when(depth == 0)
    def _():
        rest = packed_ref[288:432, :].astype(F32)
        rest_ref[0:144] = rest
        rest_ref[144:288] = pltpu.roll(rest, 64, 1)

    def damped(summed, damping):
        return scale * summed + damping

    for column in range(3):
        block = pl.ds(pl.multiple_of(96 * column + 32 * depth, 32), 32)
        low = packed_ref[block, :].astype(F32)
        far = rest_ref[block, :]
        for row in range(3):
            at = 3 * row + column
            second_ref[at] = damped(low[:, 32 * row : 32 * row + 32], d_second_ref[at])
        first_ref[column] = damped(low[:, 96:128], d_first_ref[column])
        first_ref[3 + column] = damped(far[:, 0:32], d_first_ref[3 + column])
        first_ref[6 + column] = damped(far[:, 32:64], d_first_ref[6 + column])


def filters(
    w_first_ref, v_first_ref, w_second_ref, v_second_ref, rows_ref, joint_ref, edge_ref, edge_joint_ref
):
    def turned(refs, depths):
        blocks = [(x, z) for z in range(3) for x in depths]
        tall = [
            jnp.concatenate(
                [
                    jnp.concatenate([ref[9 * x + 3 * row + z].astype(F32) for x, z in blocks], axis=0)
                    for row in range(3)
                ],
                axis=1,
            )
            for ref in refs
        ]
        return jnp.concatenate(tall, axis=0).T.astype(BF16)

    def flipped(row, depths):
        blocks = [
            w_second_ref[26 - (9 * x + 3 * row + z)].astype(F32) for z in range(3) for x in depths
        ]
        return jnp.concatenate(blocks, axis=1).astype(BF16)

    for depths, rows, joint in (
        ((0, 1, 2), rows_ref, joint_ref),
        ((1, 2), edge_ref.at[0], edge_joint_ref.at[0]),
        ((0, 1), edge_ref.at[1], edge_joint_ref.at[1]),
    ):
        rows[0:96] = turned([w_first_ref], depths)
        rows[96:192] = turned([v_first_ref], depths)
        joint[...] = turned([w_second_ref, v_second_ref], depths)
        for row in range(3):
            rows[192 + 32 * row : 224 + 32 * row] = flipped(row, depths)


def call(kernel, operands, outputs, scratch, name, limit, flops):
    vmem = pl.BlockSpec(memory_space=pltpu.VMEM)
    return pl.pallas_call(
        kernel,
        out_shape=tuple(jax.ShapeDtypeStruct(shape, dtype) for shape, dtype in outputs),
        in_specs=[vmem] * len(operands),
        out_specs=(vmem,) * len(outputs),
        scratch_shapes=[pltpu.VMEM(shape, dtype) for shape, dtype in scratch],
        compiler_params=pltpu.CompilerParams(vmem_limit_bytes=limit << 20),
        cost_estimate=pl.CostEstimate(flops=flops, bytes_accessed=1 << 20, transcendentals=0),
        name=name,
    )(*operands)


def body(volume, w_first, w_second, v_first, v_second):
    channels, depth, height, width = volume.shape
    n_gx, n_gy, n_gz = (lax.axis_size(axis) for axis in AXES)
    members = n_gx * n_gy
    count_all = float(depth * n_gx * height * n_gy * width * n_gz)
    factor = math.sqrt(27.0 * channels)
    small = (channels, 128)

    (sent,) = call(
        pack, (volume,), [((members,) + small, BF16)], [((1024, 128), F32)], "pack", 8, 10**8
    )
    parts = lax.all_to_all(sent, GROUP, 0, 0)

    parts, w_first, w_second, v_first, v_second = lax.optimization_barrier(
        (parts, w_first, w_second, v_first, v_second)
    )
    blocks = [w.reshape(27, channels, channels) for w in (w_first, v_first, w_second, v_second)]
    weights = call(
        filters,
        blocks,
        [((288, 288), BF16), ((96, 576), BF16), ((2, 288, 192), BF16), ((2, 96, 384), BF16)],
        [],
        "filters",
        8,
        2 * 10**8,
    )
    damping = tuple(
        factor * 0.1 * v.astype(F32).reshape(27, channels, channels) for v in (v_first, v_second)
    )

    halo = ((OWN - 1, 256, 128), BF16)
    own, first, second = call(
        arrange, (parts,), [((OWN, 256, 128), BF16), halo, halo], [], "arrange", 8, 10**8
    )

    def swapped(start):
        def device(at):
            gz, place = divmod(at, members)
            return LINES[gz % 2][place] * n_gz + gz

        pairs = [(device(i), device(i + 1)) for i in range(start, members * n_gz - 1, 2)]
        return pairs + [(b, a) for a, b in pairs]

    middle = ((2, 256, 128), BF16)
    ready = call(
        inner,
        (own, weights[0], weights[2]),
        [middle, middle, ((2, PLANES) + small, F32)],
        [],
        "inner",
        8,
        10**9,
    )
    first = lax.ppermute(first, AXES, swapped(0))
    second = lax.ppermute(second, AXES, swapped(1))

    (leaving,) = call(
        lambda *refs: layers(width * n_gz, *refs),
        (own, first, second, *weights, *ready),
        [((members, 48, 128), BF16)],
        [
            ((6, 256, 128), BF16),
            ((8, 256, 128), BF16),
            ((8, 256, 128), BF16),
            ((6, 256, 128), BF16),
            ((OWN, PLANES) + small, F32),
            ((512, 128), F32),
        ],
        "layers",
        24,
        8 * 10**9,
    )

    parts = lax.all_to_all(leaving, GROUP, 0, 0)
    (sums,) = call(gather_sums, (parts,), [((n_gz, 16, 128), F32)], [], "gather_sums", 8, 10**8)
    sums = lax.all_to_all(sums, "gz", 0, 0)
    (every,) = call(combine, (sums,), [((members, 16, 128), BF16)], [], "combine", 8, 10**8)
    every = lax.all_to_all(every, GROUP, 0, 0).reshape(512, 128)
    (out,) = call(
        unpack,
        (parts,),
        [(volume.shape, BF16)],
        [((1024, 128), F32)],
        "unpack",
        8,
        10**9,
    )
    third = pl.BlockSpec((9, channels, channels), lambda i: (i, 0, 0))
    gv_first, gv_second = pl.pallas_call(
        lambda *refs: finish(factor / count_all, *refs),
        grid=(3,),
        out_shape=(jax.ShapeDtypeStruct((27, channels, channels), F32),) * 2,
        in_specs=[pl.BlockSpec((512, 128), lambda i: (0, 0)), third, third],
        out_specs=(third, third),
        scratch_shapes=[pltpu.VMEM((288, 128), F32)],
        compiler_params=pltpu.CompilerParams(
            dimension_semantics=("arbitrary",), vmem_limit_bytes=8 << 20
        ),
        name="finish",
    )(every, *damping)
    return (out, gv_first.reshape(v_first.shape), gv_second.reshape(v_first.shape))


def solution(mesh):
    in_specs = (P(None, "gx", "gy", "gz"), P(), P(), P(), P())
    out_specs = (P(None, "gx", "gy", "gz"), P(), P())
    return jax.shard_map(body, mesh=mesh, in_specs=in_specs, out_specs=out_specs, check_vma=False)
```
